128 devices in a mesh: dom: 32 (over x, y, core), grp: 4 (over z).
Axes of the slice: x: 4, y: 4, z: 4, core: 2. Of those that a mesh axis runs over, the one named last changes fastest.
Arguments:
- features: bfloat16 [262144, 256], P(('dom', 'grp')), may hold values from -6 to 6
- edge_src: int32 [2097152], P(('dom', 'grp')), may hold values from 0 to 3071, as said below
- edge_dst: int32 [2097152], P(('dom', 'grp')), may hold values from 0 to 2047, as said below
- edge_count: int32 [128], P(('dom', 'grp')), may hold values from 4096 to 16384, as said below
- halo_index: int32 [128, 128, 8], P(('dom', 'grp')), may hold values from 0 to 2047
- request_rows: int32 [128, 128, 16], P(('dom', 'grp')), may hold values from 0 to 2047, as said below
- pair_ends: int32 [262144, 2], P(('dom', 'grp')), may hold values from 0 to 2047
- labels: int32 [262144], P(('dom', 'grp')), may hold values 0 or 1
- pair_weight: float32 [262144], P(('dom', 'grp')), may hold values from 0.25 to 4
- w_self: bfloat16 [256, 256], replicated, may hold values from -0.375 to 0.375
- w_neigh: bfloat16 [256, 256], replicated, may hold values from -0.375 to 0.375
- w_hidden: bfloat16 [512, 256], replicated, may hold values from -0.25 to 0.25
- b_hidden: float32 [256], replicated, may hold values from -3 to 3
- w_out: float32 [256], replicated, may hold values from -0.375 to 0.375
Outputs:
- logits: float32 [262144], P(('dom', 'grp'))
- grad_features: float32 [262144, 256], P(('dom', 'grp'))
- grad_w_self: float32 [256, 256], replicated
- grad_w_neigh: float32 [256, 256], replicated
- grad_w_hidden: float32 [512, 256], replicated
- grad_b_hidden: float32 [256], replicated
- grad_w_out: float32 [256], replicated
The draws below stay inside these ranges and needn't reach their ends.
Inputs may be any that keep to these rules, and one draw needn't show every extreme that they name: `edge_src`: a row of the partition's own table. `edge_dst`: a local node of the partition; slots at or past edge_count are not live and hold arbitrary values. `edge_count`: some partition has exactly 16384 live slots. `halo_index`: local rows of the sending partition; 8 to every partition, itself included. `request_rows`: local rows of the owning partition, distinct and increasing within each list of 16. `pair_ends`: rows of the shard's own received rows.
All inputs are finite; a program needn't handle non-finite values. No bound on the sum of `labels` on one device may be relied on, other than what follows from the above.
Results may differ from the reference program's by a relative error of at most 0.02.
The reference program's roundings to bfloat16 on the way count: a program that leaves them out, or rounds other values in their place, can miss the bound.
Values may be sent and summed in bfloat16 or wider, within the bound.
A program may use at most 192 MiB of HBM per device.

```python
import math
import jax
import jax.numpy as jnp
from jax import lax

D = 256
NODE_DEV = 2048
HALO = 8
REQ = 16
TE_DEV = 2048
PARTITIONS = 128
EDGE_DEV = 16384
NODES = 262144
EDGES = 2097152
TRAIN = 262144
RECEIVED = 2048


def draw_edge_src(key, part):
    key_one, key_two, key_three = jax.random.split(key, 3)
    coin_flip = jax.random.randint(key_one, (EDGES,), 0, 2)
    local_rows = jax.random.randint(key_two, (EDGES,), 0, NODE_DEV)
    remote_rows = NODE_DEV + jax.random.randint(key_three, (EDGES,), 0, HALO * PARTITIONS)
    return jnp.where(coin_flip == 0, local_rows, remote_rows).astype(jnp.int32)


def draw_edge_dst(key, part):
    key_one, key_two = jax.random.split(key, 2)
    first_draw = jax.random.randint(key_one, (EDGES,), 0, NODE_DEV)
    second_draw = jax.random.randint(key_two, (EDGES,), 0, NODE_DEV)
    return (first_draw * second_draw // (NODE_DEV - 1)).astype(jnp.int32)


def draw_edge_count(key, part):
    key_one, key_two = jax.random.split(key, 2)
    divisor = 1 + jax.random.randint(key_one, (PARTITIONS,), 0, 4)
    counts = EDGE_DEV // divisor
    full_one = jax.random.randint(key_two, (), 0, PARTITIONS)
    return jnp.where(jnp.arange(PARTITIONS) == full_one, EDGE_DEV, counts).astype(jnp.int32)


def draw_request_rows(key, part):
    stride = NODE_DEV // REQ
    offsets = jax.random.randint(key, (PARTITIONS, PARTITIONS, REQ), 0, stride)
    return (jnp.arange(REQ, dtype=jnp.int32)[None, None, :] * stride + offsets).astype(jnp.int32)


def set_ends(entries, stream_key, smallest, top_value):
    shape = entries.shape
    spot = [jax.random.randint(jax.random.fold_in(stream_key, axis), (), 0, shape[axis]) for axis in range(len(shape))]
    entries = entries.at[tuple(spot)].set(smallest)
    longest = shape.index(max(shape))
    spot[longest] = (spot[longest] + 1) % shape[longest]
    return entries.at[tuple(spot)].set(top_value)


def levels(key, extent, cuts, smallest, top_value):
    level = 1.0
    for dim, shards_of in cuts:
        heights = jax.random.uniform(jax.random.fold_in(jax.random.fold_in(key, 6), dim), (shards_of,), jnp.float32, smallest / len(cuts), top_value / len(cuts))
        level = level * jnp.repeat(jnp.exp(heights), extent[dim] // shards_of).reshape((-1,) + (1,) * (len(extent) - 1 - dim))
    return level


def noise(own_key, extent, width, most, cuts=(), kind=jnp.bfloat16):
    level = levels(own_key, extent, cuts, -0.22, 0.18) if cuts else 1.0
    entries = jax.random.normal(own_key, extent, jnp.float32) * width * level
    return jnp.minimum(jnp.maximum(entries, -most), most).astype(kind)


def setup_inputs(seed: int = 0) -> dict:
    streams_of = jax.random.split(jax.random.key(seed), 15)
    features = noise(streams_of[0], (NODES, D), 1.0, 6.0, ((0, 128),))
    edge_src = draw_edge_src(jax.random.fold_in(streams_of[14], 71), 0)
    edge_dst = draw_edge_dst(jax.random.fold_in(streams_of[14], 71), 0)
    edge_count = draw_edge_count(jax.random.fold_in(streams_of[14], 71), 0)
    halo_index = set_ends(jax.random.randint(streams_of[4], (PARTITIONS, PARTITIONS, HALO), 0, NODE_DEV), jax.random.fold_in(streams_of[4], 1), 0, NODE_DEV - 1).astype(jnp.int32)
    request_rows = draw_request_rows(jax.random.fold_in(streams_of[14], 71), 0)
    pair_ends = set_ends(jax.random.randint(streams_of[6], (TRAIN, 2), 0, RECEIVED), jax.random.fold_in(streams_of[6], 1), 0, RECEIVED - 1).astype(jnp.int32)
    labels = set_ends((jax.random.randint(streams_of[7], (TRAIN,), 0, 2) < 1).astype(jnp.int32), jax.random.fold_in(streams_of[7], 1), 0, 1)
    pair_weight = jnp.clip(jnp.exp(math.log(4.0) - 2.7725887 * jax.random.uniform(streams_of[8], (TRAIN,), jnp.float32) ** levels(streams_of[8], (TRAIN,), ((0, 128),), -0.2, 0.2)), 0.25, 4.0)
    w_self = noise(streams_of[9], (D, D), D ** -0.5, 0.375)
    w_neigh = noise(streams_of[10], (D, D), D ** -0.5, 0.375)
    w_hidden = noise(streams_of[11], (2 * D, D), (2 * D) ** -0.5, 0.25)
    b_hidden = noise(streams_of[12], (D,), 0.5, 3.0, (), jnp.float32)
    w_out = noise(streams_of[13], (D,), D ** -0.5, 0.375, (), jnp.float32)
    return dict(features=features, edge_src=edge_src, edge_dst=edge_dst, edge_count=edge_count, halo_index=halo_index, request_rows=request_rows, pair_ends=pair_ends, labels=labels, pair_weight=pair_weight, w_self=w_self, w_neigh=w_neigh, w_hidden=w_hidden, b_hidden=b_hidden, w_out=w_out)


def encode_one(own_rows, halo_rows, src_slots, dst_slots, live_count, w_self, w_neigh):
    row_table = jnp.concatenate([own_rows, halo_rows], axis=0)
    slot_ids = jnp.arange(src_slots.shape[0], dtype=jnp.int32)
    alive_slot = slot_ids < live_count
    dst_index = jnp.where(alive_slot, dst_slots, NODE_DEV).astype(jnp.int32)
    gathered = row_table[src_slots].astype(jnp.float32)
    agg_sums = jax.ops.segment_sum(gathered, dst_index, num_segments=NODE_DEV + 1)[:NODE_DEV]
    degree = jax.ops.segment_sum(alive_slot.astype(jnp.float32), dst_index, num_segments=NODE_DEV + 1)[:NODE_DEV]
    aggregate = (agg_sums / jnp.maximum(degree, 1.0)[:, None]).astype(jnp.bfloat16)
    embedding = (jnp.dot(own_rows, w_self, preferred_element_type=jnp.float32)
                 + jnp.dot(aggregate, w_neigh, preferred_element_type=jnp.float32)).astype(jnp.bfloat16)
    return embedding, aggregate, degree


def reference(features, edge_src, edge_dst, edge_count, halo_index, request_rows, pair_ends, labels, pair_weight, w_self, w_neigh, w_hidden, b_hidden, w_out):
    part_count = PARTITIONS
    own_rows = features.reshape(part_count, NODE_DEV, D)
    senders = jnp.arange(part_count, dtype=jnp.int32)[:, None, None]
    sent_rows = own_rows[senders, halo_index]
    arriving = jnp.transpose(sent_rows, (1, 0, 2, 3)).reshape(part_count, part_count * HALO, D)
    src_slots = edge_src.reshape(part_count, EDGE_DEV)
    dst_slots = edge_dst.reshape(part_count, EDGE_DEV)

    def encode_step(packed):
        return encode_one(packed[0], packed[1], packed[2], packed[3], packed[4], w_self, w_neigh)

    embedding, aggregate, degree = lax.map(encode_step, (own_rows, arriving, src_slots, dst_slots, edge_count))

    end_pairs = pair_ends.reshape(part_count, TE_DEV, 2)
    flag_rows = labels.reshape(part_count, TE_DEV).astype(jnp.float32)
    weight_rows = pair_weight.reshape(part_count, TE_DEV)
    owners = jnp.arange(part_count, dtype=jnp.int32)[:, None]

    def decode_step(carry, packed):
        emb_grad, grad_hidden, grad_bias, grad_out = carry
        wanted_rows, pair_end, flag_row, weight_row = packed
        received = embedding[owners, wanted_rows].reshape(part_count * REQ, D)
        pair_input = jnp.concatenate([received[pair_end[:, 0]], received[pair_end[:, 1]]], axis=1)
        pre_act = jnp.dot(pair_input, w_hidden, preferred_element_type=jnp.float32) + b_hidden
        hidden = jnp.maximum(pre_act, 0.0)
        logits = jnp.dot(hidden, w_out, precision=lax.Precision.HIGHEST)
        slope_term = weight_row * (jax.nn.sigmoid(logits) - flag_row)
        grad_out = grad_out + jnp.dot(slope_term, hidden, precision=lax.Precision.HIGHEST)
        delta_act = jnp.where(pre_act > 0, slope_term[:, None] * w_out[None, :], 0.0)
        grad_bias = grad_bias + jnp.sum(delta_act, axis=0)
        delta_b = delta_act.astype(jnp.bfloat16)
        grad_hidden = grad_hidden + jnp.dot(pair_input.T, delta_b, preferred_element_type=jnp.float32)
        pair_grad = jnp.dot(delta_b, w_hidden.T, preferred_element_type=jnp.float32)
        received_grad = (jax.ops.segment_sum(pair_grad[:, :D], pair_end[:, 0], num_segments=part_count * REQ)
                         + jax.ops.segment_sum(pair_grad[:, D:], pair_end[:, 1], num_segments=part_count * REQ))
        received_grad_b = lax.optimization_barrier(received_grad.astype(jnp.bfloat16))
        emb_grad = emb_grad.at[owners, wanted_rows].add(received_grad_b.astype(jnp.float32).reshape(part_count, REQ, D))
        return (emb_grad, grad_hidden, grad_bias, grad_out), logits

    start = (jnp.zeros((part_count, NODE_DEV, D), jnp.float32), jnp.zeros((2 * D, D), jnp.float32),
             jnp.zeros((D,), jnp.float32), jnp.zeros((D,), jnp.float32))
    final, logit_rows = lax.scan(decode_step, start, (request_rows, end_pairs, flag_rows, weight_rows))
    emb_grad, grad_hidden, grad_bias, grad_out = final
    grad_b = emb_grad.astype(jnp.bfloat16)

    def encode_back(packed):
        own_part, agg_part, deg_part, grad_part, src_part, dst_part, count_part = packed
        grad_self = jnp.dot(own_part.T, grad_part, preferred_element_type=jnp.float32)
        grad_neigh = jnp.dot(agg_part.T, grad_part, preferred_element_type=jnp.float32)
        direct = jnp.dot(grad_part, w_self.T, preferred_element_type=jnp.float32)
        agg_grad = jnp.dot(grad_part, w_neigh.T, preferred_element_type=jnp.float32) / jnp.maximum(deg_part, 1.0)[:, None]
        padded = jnp.concatenate([agg_grad, jnp.zeros((1, D), jnp.float32)], axis=0)
        slot_ids = jnp.arange(src_part.shape[0], dtype=jnp.int32)
        dst_index = jnp.where(slot_ids < count_part, dst_part, NODE_DEV).astype(jnp.int32)
        table_grad = jax.ops.segment_sum(padded[dst_index], src_part, num_segments=NODE_DEV + part_count * HALO)
        return (direct + table_grad[:NODE_DEV], table_grad[NODE_DEV:].reshape(part_count, HALO, D), grad_self, grad_neigh)

    local_grad, halo_back, self_terms, neigh_terms = lax.map(
        encode_back, (own_rows, aggregate, degree, grad_b, src_slots, dst_slots, edge_count))
    returned = jnp.transpose(halo_back, (1, 0, 2, 3))
    local_grad = local_grad.at[senders, halo_index].add(returned)
    return (logit_rows.reshape(part_count * TE_DEV), local_grad.reshape(part_count * NODE_DEV, D),
            jnp.sum(self_terms, axis=0), jnp.sum(neigh_terms, axis=0), grad_hidden, grad_bias, grad_out)
```

```python
import jax
import jax.numpy as jnp
from jax import lax
from jax.experimental import pallas as pl
from jax.experimental.pallas import tpu as pltpu
from jax.sharding import PartitionSpec as P

AXES = ("dom", "grp")
GROUP = 32
LANES = 128
TILE = 256


def exchange(x):
    return lax.all_to_all(x, AXES, split_axis=0, concat_axis=0, tiled=True)


def dot32(a, b):
    return jnp.dot(a, b, preferred_element_type=jnp.float32)


def contract_rows(left, right):
    return lax.dot_general(
        left, right, (((0,), (0,)), ((), ())), preferred_element_type=jnp.float32
    )


def adjacency_kernel(half, panels, row_ref, inc_ref, flag_ref, unit_ref, adj_ref, deg_ref, words):
    step = pl.program_id(0)
    blocks = flag_ref.shape[0]

    @pl.when(step == 0)
    def _():
        rows = half * panels

        def zero(i, carry):
            words[pl.ds(pl.multiple_of(i * TILE, TILE), TILE), :] = jnp.zeros(
                (TILE, LANES), jnp.int32
            )
            return carry

        lax.fori_loop(0, rows // TILE, zero, 0)

        def block(b, carry):
            @pl.when(flag_ref[b] == 0)
            def _():
                at = [row_ref[j * blocks + b] for j in range(GROUP)]
                unit = [inc_ref[j * blocks + b] for j in range(GROUP)]
                new = [
                    words[pl.ds(at[j], 1), :] + unit_ref[pl.ds(unit[j], 1), :]
                    for j in range(GROUP)
                ]
                for j in range(GROUP):
                    words[pl.ds(at[j], 1), :] = new[j]

            @pl.when(flag_ref[b] != 0)
            def _():
                for j in range(GROUP):
                    at = row_ref[j * blocks + b]
                    unit = inc_ref[j * blocks + b]
                    words[pl.ds(at, 1), :] = (
                        words[pl.ds(at, 1), :] + unit_ref[pl.ds(unit, 1), :]
                    )

            return carry

        lax.fori_loop(0, blocks, block, 0)

    per_half = half // TILE
    shift = jnp.where(step >= per_half, 16, 0)
    first = lax.rem(step, per_half) * TILE
    total = jnp.zeros((TILE, LANES), jnp.int32)
    for p in range(panels):
        word = words[pl.ds(pl.multiple_of(p * half + first, TILE), TILE), :]
        count = jnp.bitwise_and(jnp.right_shift(word, shift), 0xFFFF)
        total = total + count
        adj_ref[:, p * LANES : (p + 1) * LANES] = count.astype(jnp.float32).astype(jnp.bfloat16)
    degree = jnp.sum(total.astype(jnp.float32), axis=1, keepdims=True)
    deg_ref[...] = jnp.broadcast_to(jnp.maximum(degree, 1.0), (TILE, LANES))


def adjacency(edge_src, edge_dst, live_count, node_rows, table_rows):
    half = node_rows // 2
    panels = table_rows // LANES
    slots = edge_src.shape[0]
    blocks = slots // GROUP
    slot = lax.iota(jnp.int32, slots)
    live = slot < live_count
    hi = edge_dst // half
    row = (edge_src // LANES) * half + (edge_dst - hi * half)
    spare = half * panels + slot // blocks
    row = jnp.where(live, row, spare)
    unit = jnp.where(live, edge_src % LANES + hi * LANES, 2 * LANES)
    key = row.reshape(GROUP, blocks)
    clash = jnp.zeros((GROUP, blocks), jnp.bool_)
    for s in range(1, GROUP // 2 + 1):
        clash = clash | (key == jnp.roll(key, s, axis=0))
    flag = jnp.any(clash, axis=0).astype(jnp.int32)
    lane = lax.broadcasted_iota(jnp.int32, (2 * LANES + 8, LANES), 1)
    which = lax.broadcasted_iota(jnp.int32, (2 * LANES + 8, LANES), 0)
    units = jnp.where(which == lane, 1, 0) + jnp.where(which - LANES == lane, 65536, 0)
    smem = pl.BlockSpec(memory_space=pltpu.SMEM)
    steps = node_rows // TILE
    return pl.pallas_call(
        lambda *refs: adjacency_kernel(half, panels, *refs),
        grid=(steps,),
        out_shape=(
            jax.ShapeDtypeStruct((node_rows, table_rows), jnp.bfloat16),
            jax.ShapeDtypeStruct((node_rows, LANES), jnp.float32),
        ),
        in_specs=[smem, smem, smem, pl.BlockSpec((2 * LANES + 8, LANES), lambda i: (0, 0))],
        out_specs=(
            pl.BlockSpec((TILE, table_rows), lambda i: (i, 0)),
            pl.BlockSpec((TILE, LANES), lambda i: (i, 0)),
        ),
        scratch_shapes=[pltpu.VMEM((half * panels + GROUP, LANES), jnp.int32)],
        compiler_params=pltpu.CompilerParams(vmem_limit_bytes=24 * 2**20),
        cost_estimate=pl.CostEstimate(
            flops=60_000_000, bytes_accessed=16 * 2**20, transcendentals=0
        ),
        name="adjacency",
    )(row, unit, flag, units)


def per_device(
    features,
    edge_src,
    edge_dst,
    edge_count,
    halo_index,
    request_rows,
    pair_ends,
    labels,
    pair_weight,
    w_self,
    w_neigh,
    w_hidden,
    b_hidden,
    w_out,
):
    node_rows, width = features.shape
    peers = lax.axis_size(AXES)
    halo_len = halo_index.shape[2]
    halo_rows = peers * halo_len
    req_len = request_rows.shape[2]
    recv_rows = peers * req_len
    nodes = lax.iota(jnp.int32, node_rows)

    wanted = exchange(request_rows[0]).reshape(recv_rows)
    halo_rows_of = halo_index[0].reshape(halo_rows)
    halo_pick = (halo_rows_of[:, None] == nodes[None, :]).astype(jnp.bfloat16)
    outgoing = dot32(halo_pick, features).astype(jnp.bfloat16)
    arrived = exchange(outgoing.reshape(peers, halo_len, width)).reshape(halo_rows, width)

    adj, floor_deg = adjacency(
        edge_src, edge_dst, edge_count[0], node_rows, node_rows + halo_rows
    )
    floor_deg = floor_deg[:, :1]
    agg_sums = dot32(adj[:, :node_rows], features) + dot32(adj[:, node_rows:], arrived)
    aggregate = (agg_sums / floor_deg).astype(jnp.bfloat16)
    embedding = (dot32(features, w_self) + dot32(aggregate, w_neigh)).astype(jnp.bfloat16)

    want_pick = (wanted[:, None] == nodes[None, :]).astype(jnp.bfloat16)
    served = dot32(want_pick, embedding).astype(jnp.bfloat16)
    received = exchange(served.reshape(peers, req_len, width)).reshape(recv_rows, width)

    slot_ids = lax.iota(jnp.int32, recv_rows)[None, :]
    select_left = (pair_ends[:, 0][:, None] == slot_ids).astype(jnp.bfloat16)
    select_right = (pair_ends[:, 1][:, None] == slot_ids).astype(jnp.bfloat16)
    left_rows = dot32(select_left, received).astype(jnp.bfloat16)
    right_rows = dot32(select_right, received).astype(jnp.bfloat16)
    pre_act = dot32(left_rows, w_hidden[:width]) + dot32(right_rows, w_hidden[width:]) + b_hidden
    hidden = jnp.maximum(pre_act, 0.0)
    logits = jnp.sum(hidden * w_out, axis=1)
    slope = pair_weight * (jax.nn.sigmoid(logits) - labels.astype(jnp.float32))
    grad_out = jnp.sum(slope[:, None] * hidden, axis=0)
    delta = jnp.where(pre_act > 0, slope[:, None] * w_out[None, :], 0.0)
    grad_bias = jnp.sum(delta, axis=0)
    delta_b = delta.astype(jnp.bfloat16)
    pair_grad = lax.dot_general(
        delta_b, w_hidden, (((1,), (1,)), ((), ())), preferred_element_type=jnp.float32
    ).astype(jnp.bfloat16)
    received_grad = contract_rows(select_left, pair_grad[:, :width]) + contract_rows(
        select_right, pair_grad[:, width:]
    )
    grad_hidden = jnp.concatenate(
        [contract_rows(left_rows, delta_b), contract_rows(right_rows, delta_b)], axis=0
    )
    small = jnp.concatenate([grad_bias, grad_out]).reshape(peers, -1)
    small_hi = small.astype(jnp.bfloat16)
    small_lo = (small - small_hi.astype(jnp.float32)).astype(jnp.bfloat16)
    small_len = small.shape[1]
    small_row = jnp.concatenate(
        [small_hi, small_lo, jnp.zeros((peers, width - 2 * small_len), jnp.bfloat16)], axis=1
    ).reshape(peers, 1, width)
    part_hidden = grad_hidden.shape[0] // peers
    back = exchange(
        jnp.concatenate(
            [
                received_grad.astype(jnp.bfloat16).reshape(peers, req_len, width),
                grad_hidden.astype(jnp.bfloat16).reshape(peers, part_hidden, width),
                small_row,
                jnp.zeros((peers, 7 - part_hidden, width), jnp.bfloat16),
            ],
            axis=1,
        )
    )
    back_rows = back[:, :req_len].reshape(recv_rows, width)
    own_hidden = jnp.sum(back[:, req_len : req_len + part_hidden].astype(jnp.float32), axis=0)
    small_sum = jnp.sum(
        back[:, req_len + part_hidden, : 2 * small_len].astype(jnp.float32), axis=0
    )
    own_small = small_sum[:small_len] + small_sum[small_len:]

    want_put = (nodes[:, None] == wanted[None, :]).astype(jnp.bfloat16)
    grad_b = dot32(want_put, back_rows).astype(jnp.bfloat16)
    grad_self = contract_rows(features, grad_b)
    grad_neigh = contract_rows(aggregate, grad_b)
    agg_grad = (
        lax.dot_general(
            grad_b, w_neigh, (((1,), (1,)), ((), ())), preferred_element_type=jnp.float32
        )
        / floor_deg
    ).astype(jnp.bfloat16)
    table_grad = contract_rows(adj, agg_grad)
    part_node = 2 * width // peers
    weight_terms = jnp.concatenate([grad_self, grad_neigh], axis=0).astype(jnp.bfloat16)
    last = exchange(
        jnp.concatenate(
            [
                table_grad[node_rows:].astype(jnp.bfloat16).reshape(peers, halo_len, width),
                weight_terms.reshape(peers, part_node, width),
                jnp.broadcast_to(
                    own_hidden.astype(jnp.bfloat16)[None], (peers, part_hidden, width)
                ),
            ],
            axis=1,
        )
    )
    own_node = jnp.sum(last[:, halo_len : halo_len + part_node].astype(jnp.float32), axis=0)
    small_own = jnp.concatenate([own_small, jnp.zeros((width - small_len,), jnp.float32)])
    finals = jnp.concatenate(
        [own_node, small_own[None], jnp.zeros((7 - part_node, width), jnp.float32)], axis=0
    ).astype(jnp.bfloat16)
    gathered = exchange(jnp.broadcast_to(finals[None], (peers, 8, width)))
    halo_put = (nodes[:, None] == halo_rows_of[None, :]).astype(jnp.bfloat16)
    grad_features = (
        lax.dot_general(
            grad_b, w_self, (((1,), (1,)), ((), ())), preferred_element_type=jnp.float32
        )
        + table_grad[:node_rows]
        + dot32(halo_put, last[:, :halo_len].reshape(halo_rows, width))
    )
    all_hidden = last[:, halo_len + part_node :].reshape(2 * width, width).astype(jnp.float32)
    all_node = gathered[:, :part_node].reshape(2 * width, width).astype(jnp.float32)
    all_small = gathered[:, part_node, :small_len].reshape(2 * width).astype(jnp.float32)
    return (
        logits,
        grad_features,
        all_node[:width],
        all_node[width:],
        all_hidden,
        all_small[:width],
        all_small[width:],
    )


def solution(mesh):
    split = P(AXES)
    in_specs = (
        P(AXES, None),
        split,
        split,
        split,
        P(AXES, None, None),
        P(AXES, None, None),
        P(AXES, None),
        split,
        split,
        P(),
        P(),
        P(),
        P(),
        P(),
    )
    out_specs = (split, P(AXES, None), P(), P(), P(), P(), P())
    return jax.shard_map(
        per_device, mesh=mesh, in_specs=in_specs, out_specs=out_specs, check_vma=False
    )
```

```python
import jax
import jax.numpy as jnp
from jax import lax
from jax.experimental import pallas as pl
from jax.experimental.pallas import tpu as pltpu
from jax.sharding import PartitionSpec as P

AXES = ("dom", "grp")
LANES = 128
STRIDE = 8
GROUP = LANES // STRIDE
TILE = 256
CLASH = 1 << 20
VMEM = pl.BlockSpec(memory_space=pltpu.VMEM)
SMEM = pl.BlockSpec(memory_space=pltpu.SMEM)


def exchange(x):
    return lax.all_to_all(x, AXES, split_axis=0, concat_axis=0, tiled=True)


def dot32(a, b):
    return jnp.dot(a, b, preferred_element_type=jnp.float32)


def dot_nt(a, b):
    return lax.dot_general(a, b, (((1,), (1,)), ((), ())), preferred_element_type=jnp.float32)


def dot_tn(a, b):
    return lax.dot_general(a, b, (((0,), (0,)), ((), ())), preferred_element_type=jnp.float32)


def params(mib):
    return pltpu.CompilerParams(vmem_limit_bytes=mib * 2**20)


def cost(flops, size):
    return pl.CostEstimate(flops=flops, bytes_accessed=size, transcendentals=0)


def tile_of(i):
    return pl.ds(pl.multiple_of(i * TILE, TILE), TILE)


def pick(index, first, count, axis):
    shape = (index.shape[0], count) if axis == 1 else (count, index.shape[1])
    ids = lax.broadcasted_iota(jnp.int32, shape, axis) + first
    return jnp.where(index == ids, 1.0, 0.0).astype(jnp.bfloat16)


def slots_kernel(half, panels, count_ref, src_ref, dst_ref, row_ref, unit_ref):
    chunks = src_ref.shape[0]
    lane = lax.broadcasted_iota(jnp.int32, (chunks, LANES), 1)
    slot = lax.broadcasted_iota(jnp.int32, (chunks, LANES), 0) * LANES + lane
    live = slot < count_ref[0]
    src = src_ref[...]
    dst = dst_ref[...]
    upper = jnp.where(dst >= half, 1, 0)
    row = jnp.right_shift(src, 7) * half + dst - upper * half
    row = jnp.where(live, row, half * panels + jnp.right_shift(lane, 3))
    unit_ref[...] = jnp.where(live, jnp.bitwise_and(src, LANES - 1) + upper * LANES, 2 * LANES)
    clash = jnp.zeros((chunks, LANES), jnp.int32)
    for k in range(1, GROUP // 2 + 1):
        clash = clash + jnp.where(row == pltpu.roll(row, k * STRIDE, 1), 1, 0)
    any_clash = jnp.max(clash.astype(jnp.float32), axis=1, keepdims=True) > 0.0
    row_ref[...] = row + jnp.where(any_clash & (lane == 0), CLASH, 0)


def counts_kernel(half, panels, row_ref, unit_ref, adj_ref, deg_ref, degt_ref, words, units):
    step = pl.program_id(0)
    chunks = unit_ref.shape[0]

    @pl.when(step == 0)
    def _():
        def zero(i, carry):
            words[tile_of(i), :] = jnp.zeros((TILE, LANES), jnp.int32)
            return carry

        lax.fori_loop(0, half * panels // TILE, zero, 0)
        lane = lax.broadcasted_iota(jnp.int32, (LANES, LANES), 1)

        def fill(c):
            wide = jnp.transpose(
                jnp.broadcast_to(unit_ref[pl.ds(c, 1), :], (LANES, LANES))
            )
            return jnp.where(wide == lane, 1, jnp.where(wide == lane + LANES, 65536, 0))

        units[0:LANES, :] = fill(0)

        def chunk(c, carry):
            now = pl.multiple_of(lax.rem(c, 2) * LANES, LANES)
            later = pl.multiple_of(lax.rem(c + 1, 2) * LANES, LANES)
            base = c * LANES
            head = row_ref[base]
            nxt = fill(jnp.minimum(c + 1, chunks - 1))

            @pl.when(head < CLASH)
            def _():
                for s in range(STRIDE):
                    places = [s + STRIDE * t for t in range(GROUP)]
                    at = [row_ref[base + j] for j in places]
                    new = [
                        words[pl.ds(a, 1), :] + units[pl.ds(now + j, 1), :]
                        for a, j in zip(at, places)
                    ]
                    for a, n in zip(at, new):
                        words[pl.ds(a, 1), :] = n

            @pl.when(head >= CLASH)
            def _():
                def one(j, carry):
                    a = jnp.bitwise_and(row_ref[base + j], CLASH - 1)
                    words[pl.ds(a, 1), :] = words[pl.ds(a, 1), :] + units[pl.ds(now + j, 1), :]
                    return carry

                lax.fori_loop(0, LANES, one, 0)

            units[pl.ds(later, LANES), :] = nxt
            return carry

        lax.fori_loop(0, chunks, chunk, 0)

    per_half = half // TILE
    shift = jnp.where(step >= per_half, 16, 0)
    first = lax.rem(step, per_half) * TILE
    total = jnp.zeros((TILE, LANES), jnp.int32)
    for p in range(panels):
        word = words[pl.ds(pl.multiple_of(p * half + first, TILE), TILE), :]
        count = jnp.bitwise_and(jnp.right_shift(word, shift), 0xFFFF)
        total = total + count
        adj_ref[:, p * LANES : (p + 1) * LANES] = count.astype(jnp.float32).astype(jnp.bfloat16)
    degree = jnp.sum(total.astype(jnp.float32), axis=1, keepdims=True)
    wide = jnp.broadcast_to(jnp.maximum(degree, 1.0), (TILE, LANES))
    deg_ref[...] = wide
    degt_ref[...] = jnp.transpose(wide)[:8]


def adjacency(edge_src, edge_dst, edge_count, node_rows, table_rows):
    half = node_rows // 2
    panels = table_rows // LANES
    chunks = edge_src.shape[0] // LANES
    grid_shape = (chunks, LANES)
    row, unit = pl.pallas_call(
        lambda *refs: slots_kernel(half, panels, *refs),
        out_shape=(
            jax.ShapeDtypeStruct(grid_shape, jnp.int32),
            jax.ShapeDtypeStruct(grid_shape, jnp.int32),
        ),
        in_specs=[SMEM, VMEM, VMEM],
        out_specs=(VMEM, VMEM),
        compiler_params=params(8),
        name="slots",
    )(edge_count, edge_src.reshape(grid_shape), edge_dst.reshape(grid_shape))
    return pl.pallas_call(
        lambda *refs: counts_kernel(half, panels, *refs),
        grid=(node_rows // TILE,),
        out_shape=(
            jax.ShapeDtypeStruct((node_rows, table_rows), jnp.bfloat16),
            jax.ShapeDtypeStruct((node_rows, LANES), jnp.float32),
            jax.ShapeDtypeStruct((8, node_rows), jnp.float32),
        ),
        in_specs=[SMEM, pl.BlockSpec(grid_shape, lambda i: (0, 0))],
        out_specs=(
            pl.BlockSpec((TILE, table_rows), lambda i: (i, 0)),
            pl.BlockSpec((TILE, LANES), lambda i: (i, 0)),
            pl.BlockSpec((8, TILE), lambda i: (0, i)),
        ),
        scratch_shapes=[
            pltpu.VMEM((half * panels + GROUP, LANES), jnp.int32),
            pltpu.VMEM((2 * LANES, LANES), jnp.int32),
        ],
        compiler_params=params(24),
        cost_estimate=cost(60_000_000, 16 * 2**20),
        name="counts",
    )(row.reshape(-1), unit)


def encode_kernel(
    adj_ref, feat_ref, arr_ref, deg_ref, ws_ref, wn_ref, want_ref, agg_ref, served_ref, emb
):
    step = pl.program_id(0)
    node_rows = feat_ref.shape[0]
    sums = dot32(adj_ref[:, :node_rows], feat_ref[...]) + dot32(
        adj_ref[:, node_rows:], arr_ref[...]
    )
    mean = (sums / deg_ref[:, :1]).astype(jnp.bfloat16)
    agg_ref[...] = mean
    own = feat_ref[tile_of(step), :]
    emb[tile_of(step), :] = (dot32(own, ws_ref[...]) + dot32(mean, wn_ref[...])).astype(
        jnp.bfloat16
    )

    @pl.when(step == pl.num_programs(0) - 1)
    def _():
        def serve(j, carry):
            hot = pick(want_ref[tile_of(j), :], 0, node_rows, 1)
            served_ref[tile_of(j), :] = dot32(hot, emb[...]).astype(jnp.bfloat16)
            return carry

        lax.fori_loop(0, served_ref.shape[0] // TILE, serve, 0)


def encode(adj, features, arrived, deg, w_self, w_neigh, want_col):
    node_rows, width = features.shape
    table_rows = adj.shape[1]
    recv_rows = want_col.shape[0]
    whole = lambda a: pl.BlockSpec(a.shape, lambda i: (0, 0))
    return pl.pallas_call(
        encode_kernel,
        grid=(node_rows // TILE,),
        out_shape=(
            jax.ShapeDtypeStruct((node_rows, width), jnp.bfloat16),
            jax.ShapeDtypeStruct((recv_rows, width), jnp.bfloat16),
        ),
        in_specs=[
            pl.BlockSpec((TILE, table_rows), lambda i: (i, 0)),
            whole(features),
            whole(arrived),
            pl.BlockSpec((TILE, LANES), lambda i: (i, 0)),
            whole(w_self),
            whole(w_neigh),
            whole(want_col),
        ],
        out_specs=(
            pl.BlockSpec((TILE, width), lambda i: (i, 0)),
            pl.BlockSpec((recv_rows, width), lambda i: (0, 0)),
        ),
        scratch_shapes=[pltpu.VMEM((node_rows, width), jnp.bfloat16)],
        compiler_params=params(24),
        cost_estimate=cost(8_000_000_000, 16 * 2**20),
        name="encode",
    )(adj, features, arrived, deg, w_self, w_neigh, want_col)


def decode_kernel(
    recv_ref,
    endc_ref,
    endr_ref,
    wl_ref,
    wh_ref,
    bias_ref,
    wo_ref,
    logit_ref,
    rgrad_ref,
    ghid_ref,
    gsmall_ref,
    left_s,
    right_s,
    delta_s,
    pgl_s,
    pgr_s,
):
    pairs = endc_ref.shape[0]
    recv_rows, width = recv_ref.shape
    gsmall_ref[...] = jnp.zeros(gsmall_ref.shape, jnp.float32)

    def forward(i, carry):
        at = tile_of(i)
        ends = endc_ref[at, :]
        left = dot32(pick(ends[:, 0:1], 0, recv_rows, 1), recv_ref[...]).astype(jnp.bfloat16)
        right = dot32(pick(ends[:, 1:2], 0, recv_rows, 1), recv_ref[...]).astype(jnp.bfloat16)
        pre = dot32(left, wh_ref[:width, :]) + dot32(right, wh_ref[width:, :]) + bias_ref[...]
        hidden = jnp.maximum(pre, 0.0)
        logit = jnp.sum(hidden * wo_ref[...], axis=1, keepdims=True)
        logit_ref[at, :] = logit
        wl = wl_ref[at, :]
        slope = wl[:, 0:1] * (jax.nn.sigmoid(logit) - wl[:, 1:2])
        delta = jnp.where(pre > 0, slope * wo_ref[...], 0.0)
        gsmall_ref[0:1, :] += jnp.sum(delta, axis=0, keepdims=True)
        gsmall_ref[1:2, :] += jnp.sum(slope * hidden, axis=0, keepdims=True)
        delta_b = delta.astype(jnp.bfloat16)
        left_s[at, :] = left
        right_s[at, :] = right
        delta_s[at, :] = delta_b
        pgl_s[at, :] = dot_nt(delta_b, wh_ref[:width, :]).astype(jnp.bfloat16)
        pgr_s[at, :] = dot_nt(delta_b, wh_ref[width:, :]).astype(jnp.bfloat16)
        return carry

    lax.fori_loop(0, pairs // TILE, forward, 0)

    def backward(i, carry):
        total = dot32(pick(endr_ref[0:1, :], i * TILE, TILE, 0), pgl_s[...]) + dot32(
            pick(endr_ref[1:2, :], i * TILE, TILE, 0), pgr_s[...]
        )
        rgrad_ref[tile_of(i), :] = total.astype(jnp.bfloat16)
        return carry

    lax.fori_loop(0, recv_rows // TILE, backward, 0)
    ghid_ref[:width, :] = dot_tn(left_s[...], delta_s[...]).astype(jnp.bfloat16)
    ghid_ref[width:, :] = dot_tn(right_s[...], delta_s[...]).astype(jnp.bfloat16)


def decode(received, end_cols, end_rows, wl_cols, w_hidden, bias, w_out):
    recv_rows, width = received.shape
    pairs = end_cols.shape[0]
    scratch = pltpu.VMEM((pairs, width), jnp.bfloat16)
    return pl.pallas_call(
        decode_kernel,
        out_shape=(
            jax.ShapeDtypeStruct((pairs, 1), jnp.float32),
            jax.ShapeDtypeStruct((recv_rows, width), jnp.bfloat16),
            jax.ShapeDtypeStruct((2 * width, width), jnp.bfloat16),
            jax.ShapeDtypeStruct((8, width), jnp.float32),
        ),
        in_specs=[VMEM] * 7,
        out_specs=(VMEM,) * 4,
        scratch_shapes=[scratch] * 5,
        compiler_params=params(32),
        cost_estimate=cost(12_000_000_000, 4 * 2**20),
        name="decode",
    )(received, end_cols, end_rows, wl_cols, w_hidden, bias, w_out)


def node_grads_kernel(
    back_ref, want_ref, feat_ref, agg_ref, wn_ref, degt_ref, adj_ref,
    gradb_ref, gt_ref, gw_ref, halo_ref
):
    step = pl.program_id(0)
    node_rows, width = feat_ref.shape

    @pl.when(step == 0)
    def _():
        def put(i, carry):
            hot = pick(want_ref[...], i * TILE, TILE, 0)
            gradb_ref[tile_of(i), :] = dot32(hot, back_ref[...]).astype(jnp.bfloat16)
            return carry

        lax.fori_loop(0, node_rows // TILE, put, 0)
        gw_ref[:width, :] = dot_tn(feat_ref[...], gradb_ref[...]).astype(jnp.bfloat16)
        gw_ref[width:, :] = dot_tn(agg_ref[...], gradb_ref[...]).astype(jnp.bfloat16)
        gt_ref[...] = (dot_nt(wn_ref[...], gradb_ref[...]) / degt_ref[0:1, :]).astype(
            jnp.bfloat16
        )

    halo_ref[...] = jnp.transpose(dot32(gt_ref[...], adj_ref[...])).astype(jnp.bfloat16)


def node_grads(back, want_row, features, aggregate, w_neigh, degt, adj):
    node_rows, width = features.shape
    halo_rows = adj.shape[1] - node_rows
    whole = lambda a: pl.BlockSpec(a.shape, lambda i: (0, 0))
    skip = node_rows // TILE
    fixed = lambda i: (0, 0)
    return pl.pallas_call(
        node_grads_kernel,
        grid=(halo_rows // TILE,),
        out_shape=(
            jax.ShapeDtypeStruct((node_rows, width), jnp.bfloat16),
            jax.ShapeDtypeStruct((width, node_rows), jnp.bfloat16),
            jax.ShapeDtypeStruct((2 * width, width), jnp.bfloat16),
            jax.ShapeDtypeStruct((halo_rows, width), jnp.bfloat16),
        ),
        in_specs=[
            whole(back),
            whole(want_row),
            whole(features),
            whole(aggregate),
            whole(w_neigh),
            whole(degt),
            pl.BlockSpec((node_rows, TILE), lambda i: (0, i + skip)),
        ],
        out_specs=(
            pl.BlockSpec((node_rows, width), fixed),
            pl.BlockSpec((width, node_rows), fixed),
            pl.BlockSpec((2 * width, width), fixed),
            pl.BlockSpec((TILE, width), lambda i: (i, 0)),
        ),
        compiler_params=params(24),
        cost_estimate=cost(6_000_000_000, 8 * 2**20),
        name="node_grads",
    )(back, want_row, features, aggregate, w_neigh, degt, adj)


def own_grads_kernel(gradb_ref, gt_ref, ws_ref, adj_ref, out_ref):
    out_ref[...] = dot_nt(gradb_ref[...], ws_ref[...]) + jnp.transpose(
        dot32(gt_ref[...], adj_ref[...])
    )


def own_grads(grad_b, grad_t, w_self, adj):
    node_rows, width = grad_b.shape
    whole = lambda a: pl.BlockSpec(a.shape, lambda i: (0, 0))
    return pl.pallas_call(
        own_grads_kernel,
        grid=(node_rows // TILE,),
        out_shape=jax.ShapeDtypeStruct((node_rows, width), jnp.float32),
        in_specs=[
            pl.BlockSpec((TILE, width), lambda i: (i, 0)),
            whole(grad_t),
            whole(w_self),
            pl.BlockSpec((node_rows, TILE), lambda i: (0, i)),
        ],
        out_specs=pl.BlockSpec((TILE, width), lambda i: (i, 0)),
        compiler_params=params(24),
        cost_estimate=cost(6_000_000_000, 8 * 2**20),
        name="own_grads",
    )(grad_b, grad_t, w_self, adj)


def per_device(
    features,
    edge_src,
    edge_dst,
    edge_count,
    halo_index,
    request_rows,
    pair_ends,
    labels,
    pair_weight,
    w_self,
    w_neigh,
    w_hidden,
    b_hidden,
    w_out,
):
    node_rows, width = features.shape
    peers = lax.axis_size(AXES)
    halo_len = halo_index.shape[2]
    halo_rows = peers * halo_len
    req_len = request_rows.shape[2]
    recv_rows = peers * req_len
    nodes = lax.iota(jnp.int32, node_rows)

    halo_pad = jnp.pad(halo_index[0], ((0, 0), (0, req_len - halo_len)), constant_values=-1)
    halo_pick = (halo_pad.reshape(-1)[:, None] == nodes[None, :]).astype(jnp.bfloat16)
    asked = jnp.concatenate([request_rows[0] // 64, request_rows[0] % 64], axis=1)
    asked = jnp.pad(
        asked.astype(jnp.float32)[:, None, :],
        ((0, 0), (halo_len, req_len - halo_len - 1), (0, width - 2 * req_len)),
    ).reshape(peers * req_len, width)
    outgoing = (dot32(halo_pick, features) + asked).astype(jnp.bfloat16)
    outgoing = outgoing.reshape(peers, req_len, width)
    first = exchange(outgoing)
    edge_src, edge_dst, _ = lax.optimization_barrier((edge_src, edge_dst, outgoing))

    adj, deg, degt = adjacency(edge_src, edge_dst, edge_count, node_rows, node_rows + halo_rows)
    arrived = first[:, :halo_len].reshape(halo_rows, width)
    codes = first[:, halo_len, : 2 * req_len].astype(jnp.int32)
    wanted = (codes[:, :req_len] * 64 + codes[:, req_len:]).reshape(recv_rows)
    want_col = wanted.reshape(recv_rows, 1)
    want_row = wanted.reshape(1, recv_rows)
    aggregate, served = encode(adj, features, arrived, deg, w_self, w_neigh, want_col)
    received = exchange(served.reshape(peers, req_len, width)).reshape(recv_rows, width)

    wl_cols = jnp.stack([pair_weight, labels.astype(jnp.float32)], axis=1)
    logits, received_grad, grad_hidden, small = decode(
        received, pair_ends, pair_ends.T, wl_cols, w_hidden, b_hidden[None], w_out[None]
    )
    small = small[:2]
    small_hi = small.astype(jnp.bfloat16)
    small_lo = (small - small_hi.astype(jnp.float32)).astype(jnp.bfloat16)
    part = 2 * width // peers
    back = exchange(
        jnp.concatenate(
            [
                received_grad.reshape(peers, req_len, width),
                grad_hidden.reshape(peers, part, width),
                jnp.broadcast_to(small_hi[None], (peers, 2, width)),
                jnp.broadcast_to(small_lo[None], (peers, 2, width)),
            ],
            axis=1,
        )
    )
    back_rows = back[:, :req_len].reshape(recv_rows, width)
    sums = jnp.sum(back[:, req_len:].astype(jnp.float32), axis=0)
    own_hidden = sums[:part].astype(jnp.bfloat16)
    all_small = sums[part : part + 2] + sums[part + 2 : part + 4]

    grad_b, grad_t, weight_terms, halo_grad = node_grads(
        back_rows, want_row, features, aggregate, w_neigh, degt, adj
    )
    last = exchange(
        jnp.concatenate(
            [
                halo_grad.reshape(peers, halo_len, width),
                weight_terms.reshape(peers, part, width),
                jnp.broadcast_to(own_hidden[None], (peers, part, width)),
            ],
            axis=1,
        )
    )
    own = own_grads(grad_b, grad_t, w_self, adj)
    own_node = jnp.sum(last[:, halo_len : halo_len + part].astype(jnp.float32), axis=0)
    finals = own_node.astype(jnp.bfloat16).reshape(1, part * width // LANES, LANES)
    gathered = exchange(jnp.broadcast_to(finals, (peers, part * width // LANES, LANES)))
    halo_put = (nodes[:, None] == halo_index[0].reshape(halo_rows)[None, :]).astype(jnp.bfloat16)
    grad_features = own + dot32(halo_put, last[:, :halo_len].reshape(halo_rows, width))
    all_hidden = last[:, halo_len + part :].reshape(2 * width, width).astype(jnp.float32)
    all_node = gathered.reshape(2 * width, width).astype(jnp.float32)
    return (
        logits.reshape(-1),
        grad_features,
        all_node[:width],
        all_node[width:],
        all_hidden,
        all_small[0],
        all_small[1],
    )


def solution(mesh):
    split = P(AXES)
    in_specs = (
        P(AXES, None),
        split,
        split,
        split,
        P(AXES, None, None),
        P(AXES, None, None),
        P(AXES, None),
        split,
        split,
        P(),
        P(),
        P(),
        P(),
        P(),
    )
    out_specs = (split, P(AXES, None), P(), P(), P(), P(), P())
    return jax.shard_map(
        per_device, mesh=mesh, in_specs=in_specs, out_specs=out_specs, check_vma=False
    )
```

```python
import jax
import jax.numpy as jnp
from jax import lax
from jax.experimental import pallas as pl
from jax.experimental.pallas import tpu as pltpu
from jax.sharding import PartitionSpec as P

AXES = ("dom", "grp")
LANES = 128
GROUP = 8
STRIDE = LANES // GROUP
BATCH = 8
TILE = 256
CLASH = 1 << 20
VMEM = pl.BlockSpec(memory_space=pltpu.VMEM)
SMEM = pl.BlockSpec(memory_space=pltpu.SMEM)


def exchange(x):
    return lax.all_to_all(x, AXES, split_axis=0, concat_axis=0, tiled=True)


def dot32(a, b):
    return jnp.dot(a, b, preferred_element_type=jnp.float32)


def dot_nt(a, b):
    return lax.dot_general(a, b, (((1,), (1,)), ((), ())), preferred_element_type=jnp.float32)


def dot_tn(a, b):
    return lax.dot_general(a, b, (((0,), (0,)), ((), ())), preferred_element_type=jnp.float32)


def params(mib):
    return pltpu.CompilerParams(vmem_limit_bytes=mib * 2**20)


def cost(flops, size):
    return pl.CostEstimate(flops=flops, bytes_accessed=size, transcendentals=0)


def tile_of(i):
    return pl.ds(pl.multiple_of(i * TILE, TILE), TILE)


def pick(index, first, count, axis):
    shape = (index.shape[0], count) if axis == 1 else (count, index.shape[1])
    ids = lax.broadcasted_iota(jnp.int32, shape, axis) + first
    return jnp.where(index == ids, 1.0, 0.0).astype(jnp.bfloat16)


def column(ref, i):
    rows = ref[:, tile_of(i)]
    return jnp.transpose(jnp.broadcast_to(rows, (8, TILE)) if ref.shape[0] == 1 else rows)


def slots_kernel(half, panels, count_ref, src_ref, dst_ref, row_ref, unit_ref):
    chunks = src_ref.shape[0]
    lane = lax.broadcasted_iota(jnp.int32, (chunks, LANES), 1)
    slot = lax.broadcasted_iota(jnp.int32, (chunks, LANES), 0) * LANES + lane
    live = slot < count_ref[0]
    src = src_ref[...]
    dst = dst_ref[...]
    upper = jnp.where(dst >= half, 1, 0)
    row = jnp.right_shift(src, 7) * half + dst - upper * half
    row = jnp.where(live, row, half * panels + lane // STRIDE)
    unit_ref[...] = jnp.where(live, jnp.bitwise_and(src, LANES - 1) + upper * LANES, 2 * LANES)
    clash = jnp.zeros((chunks, LANES), jnp.int32)
    for k in range(1, GROUP // 2 + 1):
        clash = clash + jnp.where(row == pltpu.roll(row, k * STRIDE, 1), 1, 0)
    any_clash = jnp.max(clash.astype(jnp.float32), axis=1, keepdims=True) > 0.0
    row_ref[...] = row + jnp.where(any_clash & (lane == 0), CLASH, 0)


def counts_kernel(half, panels, row_ref, unit_ref, adj_ref, deg_ref, degt_ref, even, odd, units):
    step = pl.program_id(0)
    chunks = unit_ref.shape[0]

    @pl.when(step == 0)
    def _():
        lane = lax.broadcasted_iota(jnp.int32, (LANES, LANES), 1)
        share = half * panels // (chunks // BATCH)

        def prepare(i, carry):
            part = pl.ds(pl.multiple_of(i * share, share), share)
            for k in range(BATCH):
                c = i * BATCH + k
                wide = jnp.transpose(
                    jnp.broadcast_to(unit_ref[pl.ds(c, 1), :], (LANES, LANES))
                )
                units[pl.ds(pl.multiple_of(c * LANES, LANES), LANES), :] = jnp.where(
                    wide == lane, 1, jnp.where(wide == lane + LANES, 65536, 0)
                )
            even[part, :] = jnp.zeros((share, LANES), jnp.int32)
            odd[part, :] = jnp.zeros((share, LANES), jnp.int32)
            return carry

        lax.fori_loop(0, chunks // BATCH, prepare, 0)

        def chunk(c, carry):
            base = pl.multiple_of(c * LANES, LANES)
            places = row_ref.at[pl.ds(base, LANES)]
            head = places[0]

            def load(s):
                words = odd if s % 2 else even
                at = [places[s + STRIDE * t] for t in range(GROUP)]
                new = [
                    words[pl.ds(a, 1), :] + units[pl.ds(base + (s + STRIDE * t), 1), :]
                    for t, a in enumerate(at)
                ]
                return words, at, new

            def store(words, at, new):
                for a, n in zip(at, new):
                    words[pl.ds(a, 1), :] = n

            @pl.when(head < CLASH)
            def _():
                held = load(0)
                for s in range(1, STRIDE):
                    following = load(s)
                    store(*held)
                    held = following
                store(*held)

            @pl.when(head >= CLASH)
            def _():
                for j in range(LANES):
                    words = odd if j % 2 else even
                    a = places[j]
                    if j == 0:
                        a = a - CLASH
                    words[pl.ds(a, 1), :] = words[pl.ds(a, 1), :] + units[pl.ds(base + j, 1), :]

            return carry

        lax.fori_loop(0, chunks, chunk, 0)

    first = step * TILE
    total = jnp.zeros((TILE, LANES), jnp.int32)
    for p in range(panels):
        part = pl.ds(pl.multiple_of(p * half + first, TILE), TILE)
        word = even[part, :] + odd[part, :]
        total = total + word
        cols = slice(p * LANES, (p + 1) * LANES)
        for h, count in enumerate((jnp.bitwise_and(word, 0xFFFF), jnp.right_shift(word, 16))):
            adj_ref[h, :, cols] = count.astype(jnp.float32).astype(jnp.bfloat16)
    for h, count in enumerate((jnp.bitwise_and(total, 0xFFFF), jnp.right_shift(total, 16))):
        degree = jnp.sum(count.astype(jnp.float32), axis=1, keepdims=True)
        wide = jnp.broadcast_to(jnp.maximum(degree, 1.0), (TILE, LANES))
        deg_ref[h] = wide
        degt_ref[h] = jnp.transpose(wide)[:8]


def adjacency(edge_src, edge_dst, edge_count, node_rows, table_rows):
    half = node_rows // 2
    panels = table_rows // LANES
    chunks = edge_src.shape[0] // LANES
    grid_shape = (chunks, LANES)
    row, unit = pl.pallas_call(
        lambda *refs: slots_kernel(half, panels, *refs),
        out_shape=(
            jax.ShapeDtypeStruct(grid_shape, jnp.int32),
            jax.ShapeDtypeStruct(grid_shape, jnp.int32),
        ),
        in_specs=[SMEM, VMEM, VMEM],
        out_specs=(VMEM, VMEM),
        compiler_params=params(60),
        name="slots",
    )(edge_count, edge_src.reshape(grid_shape), edge_dst.reshape(grid_shape))
    adj, deg, degt = pl.pallas_call(
        lambda *refs: counts_kernel(half, panels, *refs),
        grid=(half // TILE,),
        out_shape=(
            jax.ShapeDtypeStruct((2, half, table_rows), jnp.bfloat16),
            jax.ShapeDtypeStruct((2, half, LANES), jnp.float32),
            jax.ShapeDtypeStruct((2, 8, half), jnp.float32),
        ),
        in_specs=[SMEM, pl.BlockSpec(grid_shape, lambda i: (0, 0))],
        out_specs=(
            pl.BlockSpec((2, TILE, table_rows), lambda i: (0, i, 0)),
            pl.BlockSpec((2, TILE, LANES), lambda i: (0, i, 0)),
            pl.BlockSpec((2, 8, TILE), lambda i: (0, 0, i)),
        ),
        scratch_shapes=[
            pltpu.VMEM((half * panels + GROUP, LANES), jnp.int32),
            pltpu.VMEM((half * panels + GROUP, LANES), jnp.int32),
            pltpu.VMEM((edge_src.shape[0], LANES), jnp.int32),
        ],
        compiler_params=params(60),
        cost_estimate=cost(60_000_000, 16 * 2**20),
        name="counts",
    )(row.reshape(-1), unit)
    return adj.reshape(node_rows, table_rows), deg.reshape(node_rows, LANES), degt


def encode_kernel(
    adj_ref, feat_ref, arr_ref, deg_ref, ws_ref, wn_ref, want_ref, agg_ref, served_ref, emb
):
    step = pl.program_id(0)
    node_rows = feat_ref.shape[0]
    sums = dot32(adj_ref[:, :node_rows], feat_ref[...]) + dot32(
        adj_ref[:, node_rows:], arr_ref[...]
    )
    mean = (sums / deg_ref[:, :1]).astype(jnp.bfloat16)
    agg_ref[...] = mean
    own = feat_ref[tile_of(step), :]
    emb[tile_of(step), :] = (dot32(own, ws_ref[...]) + dot32(mean, wn_ref[...])).astype(
        jnp.bfloat16
    )

    @pl.when(step == pl.num_programs(0) - 1)
    def _():
        def serve(j, carry):
            hot = pick(column(want_ref, j)[:, :1], 0, node_rows, 1)
            served_ref[tile_of(j), :] = dot32(hot, emb[...]).astype(jnp.bfloat16)
            return carry

        lax.fori_loop(0, served_ref.shape[0] // TILE, serve, 0, unroll=2)


def encode(adj, features, arrived, deg, w_self, w_neigh, want_row):
    node_rows, width = features.shape
    table_rows = adj.shape[1]
    recv_rows = want_row.shape[1]
    whole = lambda a: pl.BlockSpec(a.shape, lambda i: (0, 0))
    return pl.pallas_call(
        encode_kernel,
        grid=(node_rows // TILE,),
        out_shape=(
            jax.ShapeDtypeStruct((node_rows, width), jnp.bfloat16),
            jax.ShapeDtypeStruct((recv_rows, width), jnp.bfloat16),
        ),
        in_specs=[
            pl.BlockSpec((TILE, table_rows), lambda i: (i, 0)),
            whole(features),
            whole(arrived),
            pl.BlockSpec((TILE, LANES), lambda i: (i, 0)),
            whole(w_self),
            whole(w_neigh),
            whole(want_row),
        ],
        out_specs=(
            pl.BlockSpec((TILE, width), lambda i: (i, 0)),
            pl.BlockSpec((recv_rows, width), lambda i: (0, 0)),
        ),
        scratch_shapes=[pltpu.VMEM((node_rows, width), jnp.bfloat16)],
        compiler_params=params(60),
        cost_estimate=cost(8_000_000_000, 16 * 2**20),
        name="encode",
    )(adj, features, arrived, deg, w_self, w_neigh, want_row)


def decode_kernel(
    recv_ref,
    pair_ref,
    wh_ref,
    bias_ref,
    wo_ref,
    logit_ref,
    rgrad_ref,
    ghid_ref,
    gsmall_ref,
    left_s,
    right_s,
    delta_s,
    pgl_s,
    pgr_s,
):
    pairs = pair_ref.shape[1]
    recv_rows, width = recv_ref.shape
    gsmall_ref[...] = jnp.zeros(gsmall_ref.shape, jnp.float32)

    def forward(i, carry):
        at = tile_of(i)
        cols = column(pair_ref, i)
        ends = cols[:, 0:2].astype(jnp.int32)
        left = dot32(pick(ends[:, 0:1], 0, recv_rows, 1), recv_ref[...]).astype(jnp.bfloat16)
        right = dot32(pick(ends[:, 1:2], 0, recv_rows, 1), recv_ref[...]).astype(jnp.bfloat16)
        pre = dot32(left, wh_ref[:width, :]) + dot32(right, wh_ref[width:, :]) + bias_ref[...]
        hidden = jnp.maximum(pre, 0.0)
        logit = jnp.sum(hidden * wo_ref[...], axis=1, keepdims=True)
        logit_ref[at, :] = logit
        slope = cols[:, 2:3] * (jax.nn.sigmoid(logit) - cols[:, 3:4])
        delta = jnp.where(pre > 0, slope * wo_ref[...], 0.0)
        gsmall_ref[0:1, :] += jnp.sum(delta, axis=0, keepdims=True)
        gsmall_ref[1:2, :] += jnp.sum(slope * hidden, axis=0, keepdims=True)
        delta_b = delta.astype(jnp.bfloat16)
        left_s[at, :] = left
        right_s[at, :] = right
        delta_s[at, :] = delta_b
        pgl_s[at, :] = dot_nt(delta_b, wh_ref[:width, :]).astype(jnp.bfloat16)
        pgr_s[at, :] = dot_nt(delta_b, wh_ref[width:, :]).astype(jnp.bfloat16)
        return carry

    lax.fori_loop(0, pairs // TILE, forward, 0, unroll=2)

    ends = pair_ref[0:2, :].astype(jnp.int32)

    def backward(i, carry):
        total = dot32(pick(ends[0:1, :], i * TILE, TILE, 0), pgl_s[...]) + dot32(
            pick(ends[1:2, :], i * TILE, TILE, 0), pgr_s[...]
        )
        rgrad_ref[tile_of(i), :] = total.astype(jnp.bfloat16)
        return carry

    lax.fori_loop(0, recv_rows // TILE, backward, 0, unroll=2)
    ghid_ref[:width, :] = dot_tn(left_s[...], delta_s[...]).astype(jnp.bfloat16)
    ghid_ref[width:, :] = dot_tn(right_s[...], delta_s[...]).astype(jnp.bfloat16)


def decode(received, pair_rows, w_hidden, bias, w_out):
    recv_rows, width = received.shape
    pairs = pair_rows.shape[1]
    scratch = pltpu.VMEM((pairs, width), jnp.bfloat16)
    return pl.pallas_call(
        decode_kernel,
        out_shape=(
            jax.ShapeDtypeStruct((pairs, 1), jnp.float32),
            jax.ShapeDtypeStruct((recv_rows, width), jnp.bfloat16),
            jax.ShapeDtypeStruct((2 * width, width), jnp.bfloat16),
            jax.ShapeDtypeStruct((8, width), jnp.float32),
        ),
        in_specs=[VMEM] * 5,
        out_specs=(VMEM,) * 4,
        scratch_shapes=[scratch] * 5,
        compiler_params=params(60),
        cost_estimate=cost(12_000_000_000, 4 * 2**20),
        name="decode",
    )(received, pair_rows, w_hidden, bias, w_out)


def node_grads_kernel(
    back_ref, want_ref, feat_ref, agg_ref, wn_ref, degt_ref, adj_ref,
    gradb_ref, gt_ref, gw_ref, halo_ref
):
    step = pl.program_id(0)
    node_rows, width = feat_ref.shape

    @pl.when(step == 0)
    def _():
        def put(i, carry):
            hot = pick(want_ref[...], i * TILE, TILE, 0)
            gradb_ref[tile_of(i), :] = dot32(hot, back_ref[...]).astype(jnp.bfloat16)
            return carry

        lax.fori_loop(0, node_rows // TILE, put, 0, unroll=2)
        gw_ref[:width, :] = dot_tn(feat_ref[...], gradb_ref[...]).astype(jnp.bfloat16)
        gw_ref[width:, :] = dot_tn(agg_ref[...], gradb_ref[...]).astype(jnp.bfloat16)
        gt_ref[...] = (
            dot_nt(wn_ref[...], gradb_ref[...])
            / jnp.concatenate([degt_ref[0, 0:1, :], degt_ref[1, 0:1, :]], axis=1)
        ).astype(jnp.bfloat16)

    halo_ref[...] = jnp.transpose(dot32(gt_ref[...], adj_ref[...])).astype(jnp.bfloat16)


def node_grads(back, want_row, features, aggregate, w_neigh, degt, adj):
    node_rows, width = features.shape
    halo_rows = adj.shape[1] - node_rows
    whole = lambda a: pl.BlockSpec(a.shape, lambda i: (0, 0))
    skip = node_rows // TILE
    fixed = lambda i: (0, 0)
    return pl.pallas_call(
        node_grads_kernel,
        grid=(halo_rows // TILE,),
        out_shape=(
            jax.ShapeDtypeStruct((node_rows, width), jnp.bfloat16),
            jax.ShapeDtypeStruct((width, node_rows), jnp.bfloat16),
            jax.ShapeDtypeStruct((2 * width, width), jnp.bfloat16),
            jax.ShapeDtypeStruct((halo_rows, width), jnp.bfloat16),
        ),
        in_specs=[
            whole(back),
            whole(want_row),
            whole(features),
            whole(aggregate),
            whole(w_neigh),
            pl.BlockSpec(degt.shape, lambda i: (0, 0, 0)),
            pl.BlockSpec((node_rows, TILE), lambda i: (0, i + skip)),
        ],
        out_specs=(
            pl.BlockSpec((node_rows, width), fixed),
            pl.BlockSpec((width, node_rows), fixed),
            pl.BlockSpec((2 * width, width), fixed),
            pl.BlockSpec((TILE, width), lambda i: (i, 0)),
        ),
        compiler_params=params(60),
        cost_estimate=cost(6_000_000_000, 8 * 2**20),
        name="node_grads",
    )(back, want_row, features, aggregate, w_neigh, degt, adj)


def own_grads_kernel(gradb_ref, gt_ref, ws_ref, adj_ref, out_ref):
    out_ref[...] = dot_nt(gradb_ref[...], ws_ref[...]) + jnp.transpose(
        dot32(gt_ref[...], adj_ref[...])
    )


def own_grads(grad_b, grad_t, w_self, adj):
    node_rows, width = grad_b.shape
    whole = lambda a: pl.BlockSpec(a.shape, lambda i: (0, 0))
    return pl.pallas_call(
        own_grads_kernel,
        grid=(node_rows // TILE,),
        out_shape=jax.ShapeDtypeStruct((node_rows, width), jnp.float32),
        in_specs=[
            pl.BlockSpec((TILE, width), lambda i: (i, 0)),
            whole(grad_t),
            whole(w_self),
            pl.BlockSpec((node_rows, TILE), lambda i: (0, i)),
        ],
        out_specs=pl.BlockSpec((TILE, width), lambda i: (i, 0)),
        compiler_params=params(60),
        cost_estimate=cost(6_000_000_000, 8 * 2**20),
        name="own_grads",
    )(grad_b, grad_t, w_self, adj)


def per_device(
    features,
    edge_src,
    edge_dst,
    edge_count,
    halo_index,
    request_rows,
    pair_ends,
    labels,
    pair_weight,
    w_self,
    w_neigh,
    w_hidden,
    b_hidden,
    w_out,
):
    node_rows, width = features.shape
    peers = lax.axis_size(AXES)
    halo_len = halo_index.shape[2]
    halo_rows = peers * halo_len
    req_len = request_rows.shape[2]
    recv_rows = peers * req_len
    nodes = lax.iota(jnp.int32, node_rows)

    halo_pad = jnp.pad(halo_index[0], ((0, 0), (0, req_len - halo_len)), constant_values=-1)
    halo_pick = (halo_pad.reshape(-1)[:, None] == nodes[None, :]).astype(jnp.bfloat16)
    asked = jnp.concatenate([request_rows[0] // 64, request_rows[0] % 64], axis=1)
    asked = jnp.pad(
        asked.astype(jnp.float32)[:, None, :],
        ((0, 0), (halo_len, req_len - halo_len - 1), (0, width - 2 * req_len)),
    ).reshape(peers * req_len, width)
    outgoing = (dot32(halo_pick, features) + asked).astype(jnp.bfloat16)
    outgoing = outgoing.reshape(peers, req_len, width)
    first = exchange(outgoing)
    edge_src, edge_dst, _ = lax.optimization_barrier((edge_src, edge_dst, outgoing))

    adj, deg, degt = adjacency(edge_src, edge_dst, edge_count, node_rows, node_rows + halo_rows)
    arrived = first[:, :halo_len].reshape(halo_rows, width)
    codes = first[:, halo_len, : 2 * req_len].astype(jnp.int32)
    wanted = (codes[:, :req_len] * 64 + codes[:, req_len:]).reshape(recv_rows)
    want_row = wanted.reshape(1, recv_rows)
    aggregate, served = encode(adj, features, arrived, deg, w_self, w_neigh, want_row)
    received = exchange(served.reshape(peers, req_len, width)).reshape(recv_rows, width)

    pair_rows = jnp.concatenate(
        [
            pair_ends.T.astype(jnp.float32),
            pair_weight[None],
            labels.astype(jnp.float32)[None],
            jnp.zeros((4, pair_weight.shape[0]), jnp.float32),
        ],
        axis=0,
    )
    logits, received_grad, grad_hidden, small = decode(
        received, pair_rows, w_hidden, b_hidden[None], w_out[None]
    )
    small = small[:2]
    small_hi = small.astype(jnp.bfloat16)
    small_lo = (small - small_hi.astype(jnp.float32)).astype(jnp.bfloat16)
    part = 2 * width // peers
    back = exchange(
        jnp.concatenate(
            [
                received_grad.reshape(peers, req_len, width),
                grad_hidden.reshape(peers, part, width),
                jnp.broadcast_to(small_hi[None], (peers, 2, width)),
                jnp.broadcast_to(small_lo[None], (peers, 2, width)),
            ],
            axis=1,
        )
    )
    back_rows = back[:, :req_len].reshape(recv_rows, width)
    sums = jnp.sum(back[:, req_len:].astype(jnp.float32), axis=0)
    own_hidden = sums[:part].astype(jnp.bfloat16)
    all_small = sums[part : part + 2] + sums[part + 2 : part + 4]

    grad_b, grad_t, weight_terms, halo_grad = node_grads(
        back_rows, want_row, features, aggregate, w_neigh, degt, adj
    )
    last = exchange(
        jnp.concatenate(
            [
                halo_grad.reshape(peers, halo_len, width),
                weight_terms.reshape(peers, part, width),
                jnp.broadcast_to(own_hidden[None], (peers, part, width)),
            ],
            axis=1,
        )
    )
    own = own_grads(grad_b, grad_t, w_self, adj)
    own_node = jnp.sum(last[:, halo_len : halo_len + part].astype(jnp.float32), axis=0)
    finals = own_node.astype(jnp.bfloat16).reshape(1, part * width // LANES, LANES)
    gathered = exchange(jnp.broadcast_to(finals, (peers, part * width // LANES, LANES)))
    halo_put = (nodes[:, None] == halo_index[0].reshape(halo_rows)[None, :]).astype(jnp.bfloat16)
    grad_features = own + dot32(halo_put, last[:, :halo_len].reshape(halo_rows, width))
    all_hidden = last[:, halo_len + part :].reshape(2 * width, width).astype(jnp.float32)
    all_node = gathered.reshape(2 * width, width).astype(jnp.float32)
    return (
        logits.reshape(-1),
        grad_features,
        all_node[:width],
        all_node[width:],
        all_hidden,
        all_small[0],
        all_small[1],
    )


def solution(mesh):
    split = P(AXES)
    in_specs = (
        P(AXES, None),
        split,
        split,
        split,
        P(AXES, None, None),
        P(AXES, None, None),
        P(AXES, None),
        split,
        split,
        P(),
        P(),
        P(),
        P(),
        P(),
    )
    out_specs = (split, P(AXES, None), P(), P(), P(), P(), P())
    return jax.shard_map(
        per_device, mesh=mesh, in_specs=in_specs, out_specs=out_specs, check_vma=False
    )
```

```python
import jax
import jax.numpy as jnp
from jax import lax
from jax.experimental import pallas as pl
from jax.experimental.pallas import tpu as pltpu
from jax.sharding import PartitionSpec as P

AXES = ("dom", "grp")
LANES = 128
GROUP = 8
STRIDE = LANES // GROUP
BATCH = 8
TILE = 256
WIDE = 512
MESH = pl.DeviceIdType.MESH
CLASH = 1 << 20
VMEM = pl.BlockSpec(memory_space=pltpu.VMEM)
SMEM = pl.BlockSpec(memory_space=pltpu.SMEM)


def exchange(x):
    return lax.all_to_all(x, AXES, split_axis=0, concat_axis=0, tiled=True)


def dot32(a, b):
    return jnp.dot(a, b, preferred_element_type=jnp.float32)


def dot_nt(a, b):
    return lax.dot_general(a, b, (((1,), (1,)), ((), ())), preferred_element_type=jnp.float32)


def dot_tn(a, b):
    return lax.dot_general(a, b, (((0,), (0,)), ((), ())), preferred_element_type=jnp.float32)


def params(mib):
    return pltpu.CompilerParams(vmem_limit_bytes=mib * 2**20)


def cost(flops, size):
    return pl.CostEstimate(flops=flops, bytes_accessed=size, transcendentals=0)


def tile_of(i):
    return pl.ds(pl.multiple_of(i * TILE, TILE), TILE)


def pick(index, first, count, axis):
    shape = (index.shape[0], count) if axis == 1 else (count, index.shape[1])
    ids = lax.broadcasted_iota(jnp.int32, shape, axis) + first
    return jnp.where(index == ids, 1.0, 0.0).astype(jnp.bfloat16)


def column(ref, i):
    rows = ref[:, tile_of(i)]
    return jnp.transpose(jnp.broadcast_to(rows, (8, TILE)) if ref.shape[0] == 1 else rows)


def slots_kernel(half, panels, count_ref, src_ref, dst_ref, row_ref, unit_ref):
    chunks = src_ref.shape[0]
    lane = lax.broadcasted_iota(jnp.int32, (chunks, LANES), 1)
    slot = lax.broadcasted_iota(jnp.int32, (chunks, LANES), 0) * LANES + lane
    live = slot < count_ref[0]
    src = src_ref[...]
    dst = dst_ref[...]
    upper = jnp.where(dst >= half, 1, 0)
    row = jnp.right_shift(src, 7) * half + dst - upper * half
    row = jnp.where(live, row, half * panels + lane // STRIDE)
    unit_ref[...] = jnp.where(live, jnp.bitwise_and(src, LANES - 1) + upper * LANES, 2 * LANES)
    clash = jnp.zeros((chunks, LANES), jnp.int32)
    for k in range(1, GROUP // 2 + 1):
        clash = clash + jnp.where(row == pltpu.roll(row, k * STRIDE, 1), 1, 0)
    any_clash = jnp.max(clash.astype(jnp.float32), axis=1, keepdims=True) > 0.0
    row_ref[...] = row + jnp.where(any_clash & (lane == 0), CLASH, 0)


def counts_kernel(half, panels, row_ref, unit_ref, adj_ref, deg_ref, degt_ref, even, odd, units):
    step = pl.program_id(0)
    chunks = unit_ref.shape[0]

    @pl.when(step == 0)
    def _():
        lane = lax.broadcasted_iota(jnp.int32, (LANES, LANES), 1)
        share = half * panels // (chunks // BATCH)

        def prepare(i, carry):
            part = pl.ds(pl.multiple_of(i * share, share), share)
            for k in range(BATCH):
                c = i * BATCH + k
                wide = jnp.transpose(
                    jnp.broadcast_to(unit_ref[pl.ds(c, 1), :], (LANES, LANES))
                )
                units[pl.ds(pl.multiple_of(c * LANES, LANES), LANES), :] = jnp.where(
                    wide == lane, 1, jnp.where(wide == lane + LANES, 65536, 0)
                )
            even[part, :] = jnp.zeros((share, LANES), jnp.int32)
            odd[part, :] = jnp.zeros((share, LANES), jnp.int32)
            return carry

        lax.fori_loop(0, chunks // BATCH, prepare, 0)

        def chunk(c, carry):
            base = pl.multiple_of(c * LANES, LANES)
            places = row_ref.at[pl.ds(base, LANES)]
            head = places[0]

            def load(s):
                words = odd if s % 2 else even
                at = [places[s + STRIDE * t] for t in range(GROUP)]
                new = [
                    words[pl.ds(a, 1), :] + units[pl.ds(base + (s + STRIDE * t), 1), :]
                    for t, a in enumerate(at)
                ]
                return words, at, new

            def store(words, at, new):
                for a, n in zip(at, new):
                    words[pl.ds(a, 1), :] = n

            @pl.when(head < CLASH)
            def _():
                held = load(0)
                for s in range(1, STRIDE):
                    following = load(s)
                    store(*held)
                    held = following
                store(*held)

            @pl.when(head >= CLASH)
            def _():
                for j in range(LANES):
                    words = odd if j % 2 else even
                    a = places[j]
                    if j == 0:
                        a = a - CLASH
                    words[pl.ds(a, 1), :] = words[pl.ds(a, 1), :] + units[pl.ds(base + j, 1), :]

            return carry

        lax.fori_loop(0, chunks, chunk, 0)

    first = step * TILE
    total = jnp.zeros((TILE, LANES), jnp.int32)
    for p in range(panels):
        part = pl.ds(pl.multiple_of(p * half + first, TILE), TILE)
        word = even[part, :] + odd[part, :]
        total = total + word
        cols = slice(p * LANES, (p + 1) * LANES)
        for h, count in enumerate((jnp.bitwise_and(word, 0xFFFF), jnp.right_shift(word, 16))):
            adj_ref[h, :, cols] = count.astype(jnp.float32).astype(jnp.bfloat16)
    for h, count in enumerate((jnp.bitwise_and(total, 0xFFFF), jnp.right_shift(total, 16))):
        degree = jnp.sum(count.astype(jnp.float32), axis=1, keepdims=True)
        wide = jnp.broadcast_to(jnp.maximum(degree, 1.0), (TILE, LANES))
        deg_ref[h] = wide
        degt_ref[h] = jnp.transpose(wide)[:8]


def adjacency(edge_src, edge_dst, edge_count, node_rows, table_rows):
    half = node_rows // 2
    panels = table_rows // LANES
    chunks = edge_src.shape[0] // LANES
    grid_shape = (chunks, LANES)
    row, unit = pl.pallas_call(
        lambda *refs: slots_kernel(half, panels, *refs),
        out_shape=(
            jax.ShapeDtypeStruct(grid_shape, jnp.int32),
            jax.ShapeDtypeStruct(grid_shape, jnp.int32),
        ),
        in_specs=[SMEM, VMEM, VMEM],
        out_specs=(VMEM, VMEM),
        compiler_params=params(60),
        name="slots",
    )(edge_count, edge_src.reshape(grid_shape), edge_dst.reshape(grid_shape))
    adj, deg, degt = pl.pallas_call(
        lambda *refs: counts_kernel(half, panels, *refs),
        grid=(half // TILE,),
        out_shape=(
            jax.ShapeDtypeStruct((2, half, table_rows), jnp.bfloat16),
            jax.ShapeDtypeStruct((2, half, LANES), jnp.float32),
            jax.ShapeDtypeStruct((2, 8, half), jnp.float32),
        ),
        in_specs=[SMEM, pl.BlockSpec(grid_shape, lambda i: (0, 0))],
        out_specs=(
            pl.BlockSpec((2, TILE, table_rows), lambda i: (0, i, 0)),
            pl.BlockSpec((2, TILE, LANES), lambda i: (0, i, 0)),
            pl.BlockSpec((2, 8, TILE), lambda i: (0, 0, i)),
        ),
        scratch_shapes=[
            pltpu.VMEM((half * panels + GROUP, LANES), jnp.int32),
            pltpu.VMEM((half * panels + GROUP, LANES), jnp.int32),
            pltpu.VMEM((edge_src.shape[0], LANES), jnp.int32),
        ],
        compiler_params=params(60),
        cost_estimate=cost(60_000_000, 16 * 2**20),
        name="counts",
    )(row.reshape(-1), unit)
    return adj.reshape(node_rows, table_rows), deg.reshape(node_rows, LANES), degt


def step_kernel(
    adj_ref,
    feat_ref,
    arr_ref,
    deg_ref,
    degt_ref,
    want_ref,
    pair_ref,
    halo_ref,
    ws_ref,
    wn_ref,
    wh_ref,
    bias_ref,
    wo_ref,
    logit_ref,
    gfeat_ref,
    wts_ref,
    sums_ref,
    adj_s,
    emb_s,
    agg_s,
    served_s,
    recv_s,
    left_s,
    right_s,
    delta_s,
    pgl_s,
    pgr_s,
    rgrad_s,
    back_s,
    gradb_s,
    gt_s,
    gw_s,
    small_s,
    last_s,
    lrecv_s,
    share_s,
    srecv_s,
    adj_sem,
    send_sem,
    recv_sem,
):
    node_rows, width = feat_ref.shape
    recv_rows = want_ref.shape[1]
    pairs = pair_ref.shape[1]
    peers, block = last_s.shape[:2]
    grp = lax.axis_size("grp")
    me = lax.axis_index("dom") * grp + lax.axis_index("grp")
    burst = WIDE // block
    bursts = peers // burst
    tiles = node_rows // TILE
    barrier = pltpu.get_barrier_semaphore()

    def device(p):
        return (p // grp, lax.rem(p, grp))

    def load_adj(i):
        return pltpu.make_async_copy(
            adj_ref.at[tile_of(i), :], adj_s.at[tile_of(i), :], adj_sem.at[i]
        )

    def fetch(i, carry):
        load_adj(i).start()
        return carry

    lax.fori_loop(0, tiles, fetch, 0)

    def greet(i, carry):
        pl.semaphore_signal(
            barrier, inc=1, device_id=device(lax.rem(me + i, peers)), device_id_type=MESH
        )
        return carry

    lax.fori_loop(1, peers, greet, 0)

    def rows_of(p):
        return pl.ds(pl.multiple_of(p * block, block), block)

    def burst_at(k):
        return lax.rem(me // burst + k, bursts)

    def ship(k, source, target, which):
        def one(i, carry):
            p = burst_at(k) * burst + lax.rem(lax.rem(me, burst) + i, burst)

            @pl.when(p != me)
            def _():
                pltpu.make_async_remote_copy(
                    src_ref=source(p),
                    dst_ref=target,
                    send_sem=send_sem.at[which],
                    recv_sem=recv_sem.at[which],
                    device_id=device(p),
                    device_id_type=MESH,
                ).start()

            return carry

        lax.fori_loop(0, burst, one, 0)

    def settle(part, which):
        pltpu.make_async_copy(part, part, send_sem.at[which]).wait()
        pltpu.make_async_copy(part, part, recv_sem.at[which]).wait()

    def wide_at(k):
        return pl.ds(pl.multiple_of(burst_at(k) * WIDE, WIDE), WIDE)

    def produce(fill, source, target, which):
        fill(0)

        def middle(k, carry):
            fill(k)
            ship(k - 1, source, target, which)
            return carry

        lax.fori_loop(1, bursts, middle, 0)

    def encode(i, carry):
        load_adj(i).wait()
        at = tile_of(i)
        sums = dot32(adj_s[at, :node_rows], feat_ref[...]) + dot32(
            adj_s[at, node_rows:], arr_ref[...]
        )
        mean = (sums / deg_ref[at, :1]).astype(jnp.bfloat16)
        agg_s[at, :] = mean
        emb_s[at, :] = (dot32(feat_ref[at, :], ws_ref[...]) + dot32(mean, wn_ref[...])).astype(
            jnp.bfloat16
        )
        return carry

    lax.fori_loop(0, tiles, encode, 0)
    pl.semaphore_wait(barrier, peers - 1)

    def serve(k):
        at = wide_at(k)
        asked = jnp.transpose(jnp.broadcast_to(want_ref[:, at], (8, WIDE)))[:, :1]
        served_s[at, :] = dot32(pick(asked, 0, node_rows, 1), emb_s[...]).astype(jnp.bfloat16)

    served_of = lambda p: served_s.at[rows_of(p), :]
    produce(serve, served_of, recv_s.at[rows_of(me), :], 0)
    recv_s[rows_of(me), :] = served_s[rows_of(me), :]
    small_s[...] = jnp.zeros(small_s.shape, jnp.float32)
    ship(bursts - 1, served_of, recv_s.at[rows_of(me), :], 0)
    settle(recv_s.at[pl.ds(block, recv_rows - block), :], 0)

    def forward(i, carry):
        at = pl.ds(pl.multiple_of(i * WIDE, WIDE), WIDE)
        cols = jnp.transpose(pair_ref[:, at])
        ends = cols[:, 0:2].astype(jnp.int32)
        left = dot32(pick(ends[:, 0:1], 0, recv_rows, 1), recv_s[...]).astype(jnp.bfloat16)
        right = dot32(pick(ends[:, 1:2], 0, recv_rows, 1), recv_s[...]).astype(jnp.bfloat16)
        pre = dot32(left, wh_ref[:width, :]) + dot32(right, wh_ref[width:, :]) + bias_ref[...]
        hidden = jnp.maximum(pre, 0.0)
        logit = jnp.sum(hidden * wo_ref[...], axis=1, keepdims=True)
        logit_ref[:, at] = jnp.transpose(jnp.broadcast_to(logit, (WIDE, LANES)))[:8]
        slope = cols[:, 2:3] * (jax.nn.sigmoid(logit) - cols[:, 3:4])
        delta = jnp.where(pre > 0, slope * wo_ref[...], 0.0)
        small_s[0:1, :] += jnp.sum(delta, axis=0, keepdims=True)
        small_s[1:2, :] += jnp.sum(slope * hidden, axis=0, keepdims=True)
        delta_b = delta.astype(jnp.bfloat16)
        left_s[at, :] = left
        right_s[at, :] = right
        delta_s[at, :] = delta_b
        pgl_s[at, :] = dot_nt(delta_b, wh_ref[:width, :]).astype(jnp.bfloat16)
        pgr_s[at, :] = dot_nt(delta_b, wh_ref[width:, :]).astype(jnp.bfloat16)
        return carry

    lax.fori_loop(0, pairs // WIDE, forward, 0)
    ends_row = pair_ref[0:2, :].astype(jnp.int32)

    def collect(k):
        first = burst_at(k) * WIDE
        total = dot32(pick(ends_row[0:1, :], first, WIDE, 0), pgl_s[...]) + dot32(
            pick(ends_row[1:2, :], first, WIDE, 0), pgr_s[...]
        )
        rgrad_s[wide_at(k), :] = total.astype(jnp.bfloat16)

    rgrad_of = lambda p: rgrad_s.at[rows_of(p), :]
    produce(collect, rgrad_of, back_s.at[rows_of(me), :], 1)
    back_s[rows_of(me), :] = rgrad_s[rows_of(me), :]
    ship(bursts - 1, rgrad_of, back_s.at[rows_of(me), :], 1)
    gw_s[2 * width : 3 * width, :] = dot_tn(left_s[...], delta_s[...])
    gw_s[3 * width :, :] = dot_tn(right_s[...], delta_s[...])
    settle(back_s.at[pl.ds(block, recv_rows - block), :], 1)

    def put(i, carry):
        at = pl.ds(pl.multiple_of(i * WIDE, WIDE), WIDE)
        hot = pick(want_ref[...], i * WIDE, WIDE, 0)
        gradb_s[at, :] = dot32(hot, back_s[...]).astype(jnp.bfloat16)
        return carry

    lax.fori_loop(0, node_rows // WIDE, put, 0)
    gw_s[:width, :] = dot_tn(feat_ref[...], gradb_s[...])
    gw_s[width : 2 * width, :] = dot_tn(agg_s[...], gradb_s[...])
    degree = jnp.concatenate([degt_ref[0, 0:1, :], degt_ref[1, 0:1, :]], axis=1)
    gt_s[...] = (dot_nt(wn_ref[...], gradb_s[...]) / degree).astype(jnp.bfloat16)

    def table_grad(first):
        cols = pl.ds(pl.multiple_of(first, TILE), TILE)
        return jnp.transpose(dot32(gt_s[...], adj_s[:, cols]))

    half = block // 2

    def return_halo(k):
        t = burst_at(k)
        both = jnp.concatenate(
            [
                table_grad(node_rows + t * TILE).reshape(burst, half, width),
                gw_s[tile_of(t), :].reshape(burst, half, width),
            ],
            axis=1,
        )
        last_s[pl.ds(t * burst, burst)] = both.astype(jnp.bfloat16)

    last_of = lambda p: last_s.at[p]
    produce(return_halo, last_of, lrecv_s.at[me], 2)
    lrecv_s[me] = last_s[me]
    ship(bursts - 1, last_of, lrecv_s.at[me], 2)

    def direct(i, carry):
        at = tile_of(i)
        gfeat_ref[at, :] = dot_nt(gradb_s[at, :], ws_ref[...]) + table_grad(i * TILE)
        return carry

    lax.fori_loop(0, tiles, direct, 0)
    settle(lrecv_s.at[pl.ds(1, peers - 1)], 2)

    own = jnp.sum(lrecv_s[...].astype(jnp.float32), axis=0)[half:]
    small = small_s[...]
    small_hi = small.astype(jnp.bfloat16).astype(jnp.float32)
    small_lo = small - small_hi
    lines = [
        part[r : r + 1, c : c + LANES]
        for part in (small_hi, small_lo)
        for r in range(2)
        for c in (0, LANES)
    ]
    share_s[...] = jnp.concatenate([own[:, :LANES], own[:, LANES:]] + lines, axis=0).astype(
        jnp.bfloat16
    )

    def place(i, carry):
        at = pl.ds(pl.multiple_of(i * WIDE, WIDE), WIDE)
        hot = pick(halo_ref[...], i * WIDE, WIDE, 0)
        gfeat_ref[at, :] += dot32(hot, lrecv_s[...].reshape(recv_rows, width))
        return carry

    place(0, 0)

    def share(i, carry):
        p = lax.rem(me + i * 51, peers)
        pltpu.make_async_remote_copy(
            src_ref=share_s,
            dst_ref=srecv_s.at[me],
            send_sem=send_sem.at[3],
            recv_sem=recv_sem.at[3],
            device_id=device(p),
            device_id_type=MESH,
        ).start()
        return carry

    lax.fori_loop(1, peers, share, 0)
    srecv_s[me] = share_s[...]
    lax.fori_loop(1, node_rows // WIDE, place, 0)
    settle(srecv_s.at[pl.ds(1, peers - 1)], 3)
    everyone = srecv_s[...].astype(jnp.float32)
    wts_ref[:, :LANES] = everyone[:, :8].reshape(4 * width, LANES)
    wts_ref[:, LANES:] = everyone[:, 8:16].reshape(4 * width, LANES)
    sums_ref[...] = jnp.sum(everyone[:, 16:], axis=0)


def train_step(
    adj, features, arrived, deg, degt, want_row, pair_rows, halo_pad, w_self, w_neigh, w_hidden,
    bias, w_out, peers
):
    node_rows, width = features.shape
    table_rows = adj.shape[1]
    recv_rows = want_row.shape[1]
    pairs = pair_rows.shape[1]
    block = recv_rows // peers
    lines = width * 4 * width // peers // LANES + 8
    bf16 = lambda *shape: pltpu.VMEM(shape, jnp.bfloat16)
    return pl.pallas_call(
        step_kernel,
        out_shape=(
            jax.ShapeDtypeStruct((8, pairs), jnp.float32),
            jax.ShapeDtypeStruct((node_rows, width), jnp.float32),
            jax.ShapeDtypeStruct((4 * width, width), jnp.float32),
            jax.ShapeDtypeStruct((8, LANES), jnp.float32),
        ),
        in_specs=[pl.BlockSpec(memory_space=pl.ANY)] + [VMEM] * 12,
        out_specs=(VMEM,) * 4,
        scratch_shapes=[
            bf16(node_rows, table_rows),
            bf16(node_rows, width),
            bf16(node_rows, width),
            bf16(recv_rows, width),
            bf16(recv_rows, width),
            bf16(pairs, width),
            bf16(pairs, width),
            bf16(pairs, width),
            bf16(pairs, width),
            bf16(pairs, width),
            bf16(recv_rows, width),
            bf16(recv_rows, width),
            bf16(node_rows, width),
            bf16(width, node_rows),
            pltpu.VMEM((4 * width, width), jnp.float32),
            pltpu.VMEM((8, width), jnp.float32),
            bf16(peers, block, width),
            bf16(peers, block, width),
            bf16(lines, LANES),
            bf16(peers, lines, LANES),
            pltpu.SemaphoreType.DMA((node_rows // TILE,)),
            pltpu.SemaphoreType.DMA((4,)),
            pltpu.SemaphoreType.DMA((4,)),
        ],
        compiler_params=pltpu.CompilerParams(
            vmem_limit_bytes=62 * 2**20, collective_id=0, has_side_effects=True
        ),
        cost_estimate=cost(30_000_000_000, 24 * 2**20),
        name="train_step",
    )(
        adj, features, arrived, deg, degt, want_row, pair_rows, halo_pad, w_self, w_neigh,
        w_hidden, bias, w_out,
    )


def per_device(
    features,
    edge_src,
    edge_dst,
    edge_count,
    halo_index,
    request_rows,
    pair_ends,
    labels,
    pair_weight,
    w_self,
    w_neigh,
    w_hidden,
    b_hidden,
    w_out,
):
    node_rows, width = features.shape
    peers = lax.axis_size(AXES)
    halo_len = halo_index.shape[2]
    halo_rows = peers * halo_len
    req_len = request_rows.shape[2]
    recv_rows = peers * req_len
    nodes = lax.iota(jnp.int32, node_rows)

    halo_pad = jnp.pad(halo_index[0], ((0, 0), (0, req_len - halo_len)), constant_values=-1)
    halo_pick = (halo_pad.reshape(-1)[:, None] == nodes[None, :]).astype(jnp.bfloat16)
    asked = jnp.concatenate([request_rows[0] // 64, request_rows[0] % 64], axis=1)
    asked = jnp.pad(
        asked.astype(jnp.float32)[:, None, :],
        ((0, 0), (halo_len, req_len - halo_len - 1), (0, width - 2 * req_len)),
    ).reshape(peers * req_len, width)
    outgoing = (dot32(halo_pick, features) + asked).astype(jnp.bfloat16)
    outgoing = outgoing.reshape(peers, req_len, width)
    first = exchange(outgoing)
    edge_src, edge_dst, _ = lax.optimization_barrier((edge_src, edge_dst, outgoing))

    adj, deg, degt = adjacency(edge_src, edge_dst, edge_count, node_rows, node_rows + halo_rows)
    arrived = first[:, :halo_len].reshape(halo_rows, width)
    codes = first[:, halo_len, : 2 * req_len].astype(jnp.int32)
    wanted = (codes[:, :req_len] * 64 + codes[:, req_len:]).reshape(recv_rows)
    want_row = wanted.reshape(1, recv_rows)
    pair_rows = jnp.concatenate(
        [
            pair_ends.T.astype(jnp.float32),
            pair_weight[None],
            labels.astype(jnp.float32)[None],
            jnp.zeros((4, pair_weight.shape[0]), jnp.float32),
        ],
        axis=0,
    )
    logits, grad_features, weights, small = train_step(
        adj, features, arrived, deg, degt, want_row, pair_rows, halo_pad.reshape(1, -1), w_self,
        w_neigh, w_hidden, b_hidden[None], w_out[None], peers
    )
    small = (small[:4] + small[4:]).reshape(2, width)
    return (
        logits[0],
        grad_features,
        weights[:width],
        weights[width : 2 * width],
        weights[2 * width :],
        small[0],
        small[1],
    )


def solution(mesh):
    split = P(AXES)
    in_specs = (
        P(AXES, None),
        split,
        split,
        split,
        P(AXES, None, None),
        P(AXES, None, None),
        P(AXES, None),
        split,
        split,
        P(),
        P(),
        P(),
        P(),
        P(),
    )
    out_specs = (split, P(AXES, None), P(), P(), P(), P(), P())
    return jax.shard_map(
        per_device, mesh=mesh, in_specs=in_specs, out_specs=out_specs, check_vma=False
    )
```

```python
import jax
import jax.numpy as jnp
from jax import lax
from jax.experimental import pallas as pl
from jax.experimental.pallas import tpu as pltpu
from jax.sharding import PartitionSpec as P

AXES = ("dom", "grp")
LANES = 128
GROUP = 8
STRIDE = LANES // GROUP
BATCH = 8
TILE = 256
WIDE = 512
TALL = 1024
MESH = pl.DeviceIdType.MESH
CLASH = 1 << 20
VMEM = pl.BlockSpec(memory_space=pltpu.VMEM)
SMEM = pl.BlockSpec(memory_space=pltpu.SMEM)


def exchange(x):
    return lax.all_to_all(x, AXES, split_axis=0, concat_axis=0, tiled=True)


def dot32(a, b):
    return jnp.dot(a, b, preferred_element_type=jnp.float32)


def dot_nt(a, b):
    return lax.dot_general(a, b, (((1,), (1,)), ((), ())), preferred_element_type=jnp.float32)


def dot_tn(a, b):
    return lax.dot_general(a, b, (((0,), (0,)), ((), ())), preferred_element_type=jnp.float32)


def params(mib):
    return pltpu.CompilerParams(vmem_limit_bytes=mib * 2**20)


def cost(flops, size):
    return pl.CostEstimate(flops=flops, bytes_accessed=size, transcendentals=0)


def tile_of(i):
    return pl.ds(pl.multiple_of(i * TILE, TILE), TILE)


def pick(index, first, count, axis):
    shape = (index.shape[0], count) if axis == 1 else (count, index.shape[1])
    ids = lax.broadcasted_iota(jnp.int32, shape, axis) + first
    return jnp.where(index == ids, 1.0, 0.0).astype(jnp.bfloat16)


def column(ref, i):
    rows = ref[:, tile_of(i)]
    return jnp.transpose(jnp.broadcast_to(rows, (8, TILE)) if ref.shape[0] == 1 else rows)


def slots_kernel(half, panels, count_ref, src_ref, dst_ref, row_ref, unit_ref):
    chunks = src_ref.shape[0]
    lane = lax.broadcasted_iota(jnp.int32, (chunks, LANES), 1)
    slot = lax.broadcasted_iota(jnp.int32, (chunks, LANES), 0) * LANES + lane
    live = slot < count_ref[0]
    src = src_ref[...]
    dst = dst_ref[...]
    upper = jnp.where(dst >= half, 1, 0)
    row = jnp.right_shift(src, 7) * half + dst - upper * half
    row = jnp.where(live, row, half * panels + lane // STRIDE)
    unit_ref[...] = jnp.where(live, jnp.bitwise_and(src, LANES - 1) + upper * LANES, 2 * LANES)
    clash = jnp.zeros((chunks, LANES), jnp.int32)
    for k in range(1, GROUP // 2 + 1):
        clash = clash + jnp.where(row == pltpu.roll(row, k * STRIDE, 1), 1, 0)
    any_clash = jnp.max(clash.astype(jnp.float32), axis=1, keepdims=True) > 0.0
    row_ref[...] = row + jnp.where(any_clash & (lane == 0), CLASH, 0)


def counts_kernel(half, panels, row_ref, unit_ref, adj_ref, deg_ref, degt_ref, even, odd, units):
    step = pl.program_id(0)
    chunks = unit_ref.shape[0]

    @pl.when(step == 0)
    def _():
        lane = lax.broadcasted_iota(jnp.int32, (LANES, LANES), 1)
        share = half * panels // (chunks // BATCH)

        def prepare(i, carry):
            part = pl.ds(pl.multiple_of(i * share, share), share)
            for k in range(BATCH):
                c = i * BATCH + k
                wide = jnp.transpose(
                    jnp.broadcast_to(unit_ref[pl.ds(c, 1), :], (LANES, LANES))
                )
                units[pl.ds(pl.multiple_of(c * LANES, LANES), LANES), :] = jnp.where(
                    wide == lane, 1, jnp.where(wide == lane + LANES, 65536, 0)
                )
            even[part, :] = jnp.zeros((share, LANES), jnp.int32)
            odd[part, :] = jnp.zeros((share, LANES), jnp.int32)
            return carry

        lax.fori_loop(0, chunks // BATCH, prepare, 0)

        def chunk(c, carry):
            base = pl.multiple_of(c * LANES, LANES)
            places = row_ref.at[pl.ds(base, LANES)]
            head = places[0]

            def load(s):
                words = odd if s % 2 else even
                at = [places[s + STRIDE * t] for t in range(GROUP)]
                new = [
                    words[pl.ds(a, 1), :] + units[pl.ds(base + (s + STRIDE * t), 1), :]
                    for t, a in enumerate(at)
                ]
                return words, at, new

            def store(words, at, new):
                for a, n in zip(at, new):
                    words[pl.ds(a, 1), :] = n

            @pl.when(head < CLASH)
            def _():
                held = load(0)
                for s in range(1, STRIDE):
                    following = load(s)
                    store(*held)
                    held = following
                store(*held)

            @pl.when(head >= CLASH)
            def _():
                for j in range(LANES):
                    words = odd if j % 2 else even
                    a = places[j]
                    if j == 0:
                        a = a - CLASH
                    words[pl.ds(a, 1), :] = words[pl.ds(a, 1), :] + units[pl.ds(base + j, 1), :]

            return carry

        lax.fori_loop(0, chunks, chunk, 0)

    first = step * TILE
    total = jnp.zeros((TILE, LANES), jnp.int32)
    for p in range(panels):
        part = pl.ds(pl.multiple_of(p * half + first, TILE), TILE)
        word = even[part, :] + odd[part, :]
        total = total + word
        cols = slice(p * LANES, (p + 1) * LANES)
        for h, count in enumerate((jnp.bitwise_and(word, 0xFFFF), jnp.right_shift(word, 16))):
            adj_ref[h, :, cols] = count.astype(jnp.float32).astype(jnp.bfloat16)
    for h, count in enumerate((jnp.bitwise_and(total, 0xFFFF), jnp.right_shift(total, 16))):
        degree = jnp.sum(count.astype(jnp.float32), axis=1, keepdims=True)
        wide = jnp.broadcast_to(jnp.maximum(degree, 1.0), (TILE, LANES))
        deg_ref[h] = wide
        degt_ref[h] = jnp.transpose(wide)[:8]


def adjacency(edge_src, edge_dst, edge_count, node_rows, table_rows):
    half = node_rows // 2
    panels = table_rows // LANES
    chunks = edge_src.shape[0] // LANES
    grid_shape = (chunks, LANES)
    row, unit = pl.pallas_call(
        lambda *refs: slots_kernel(half, panels, *refs),
        out_shape=(
            jax.ShapeDtypeStruct(grid_shape, jnp.int32),
            jax.ShapeDtypeStruct(grid_shape, jnp.int32),
        ),
        in_specs=[SMEM, VMEM, VMEM],
        out_specs=(VMEM, VMEM),
        compiler_params=params(60),
        name="slots",
    )(edge_count, edge_src.reshape(grid_shape), edge_dst.reshape(grid_shape))
    adj, deg, degt = pl.pallas_call(
        lambda *refs: counts_kernel(half, panels, *refs),
        grid=(half // TILE,),
        out_shape=(
            jax.ShapeDtypeStruct((2, half, table_rows), jnp.bfloat16),
            jax.ShapeDtypeStruct((2, half, LANES), jnp.float32),
            jax.ShapeDtypeStruct((2, 8, half), jnp.float32),
        ),
        in_specs=[SMEM, pl.BlockSpec(grid_shape, lambda i: (0, 0))],
        out_specs=(
            pl.BlockSpec((2, TILE, table_rows), lambda i: (0, i, 0)),
            pl.BlockSpec((2, TILE, LANES), lambda i: (0, i, 0)),
            pl.BlockSpec((2, 8, TILE), lambda i: (0, 0, i)),
        ),
        scratch_shapes=[
            pltpu.VMEM((half * panels + GROUP, LANES), jnp.int32),
            pltpu.VMEM((half * panels + GROUP, LANES), jnp.int32),
            pltpu.VMEM((edge_src.shape[0], LANES), jnp.int32),
        ],
        compiler_params=params(60),
        cost_estimate=cost(60_000_000, 16 * 2**20),
        name="counts",
    )(row.reshape(-1), unit)
    return adj.reshape(node_rows, table_rows), deg.reshape(node_rows, LANES), degt


def step_kernel(
    adj_ref,
    feat_ref,
    arr_ref,
    deg_ref,
    degt_ref,
    want_ref,
    pair_ref,
    halo_ref,
    ws_ref,
    wn_ref,
    wh_ref,
    bias_ref,
    wo_ref,
    logit_ref,
    gfeat_ref,
    gself_ref,
    gneigh_ref,
    ghid_ref,
    gbias_ref,
    gout_ref,
    adj_s,
    emb_s,
    agg_s,
    served_s,
    recv_s,
    left_s,
    right_s,
    delta_s,
    pgl_s,
    pgr_s,
    rgrad_s,
    back_s,
    gradb_s,
    gt_s,
    gw_s,
    small_s,
    cols_s,
    part_s,
    precv_s,
    halo_s,
    hrecv_s,
    hrows_s,
    share_s,
    srecv_s,
    adj_sem,
    send_sem,
    recv_sem,
):
    node_rows, width = feat_ref.shape
    recv_rows = want_ref.shape[1]
    pairs = pair_ref.shape[1]
    peers = part_s.shape[0]
    block = recv_rows // peers
    grp = lax.axis_size("grp")
    me = lax.axis_index("dom") * grp + lax.axis_index("grp")
    burst = WIDE // block
    bursts = peers // burst
    tiles = node_rows // TILE
    barrier = pltpu.get_barrier_semaphore()

    def device(p):
        return (p // grp, lax.rem(p, grp))

    def load_adj(i):
        return pltpu.make_async_copy(
            adj_ref.at[tile_of(i), :], adj_s.at[tile_of(i), :], adj_sem.at[i]
        )

    def fetch(i, carry):
        load_adj(i).start()
        return carry

    lax.fori_loop(0, tiles, fetch, 0)

    def greet(i, carry):
        pl.semaphore_signal(
            barrier, inc=1, device_id=device(lax.rem(me + i, peers)), device_id_type=MESH
        )
        return carry

    lax.fori_loop(1, peers, greet, 0)

    def rows_of(p):
        return pl.ds(pl.multiple_of(p * block, block), block)

    def burst_at(k):
        return lax.rem(me // burst + k, bursts)

    def ship(k, source, target, which):
        def one(i, carry):
            p = burst_at(k) * burst + lax.rem(lax.rem(me, burst) + i, burst)

            @pl.when(p != me)
            def _():
                pltpu.make_async_remote_copy(
                    src_ref=source(p),
                    dst_ref=target,
                    send_sem=send_sem.at[which],
                    recv_sem=recv_sem.at[which, k],
                    device_id=device(p),
                    device_id_type=MESH,
                ).start()

            return carry

        lax.fori_loop(0, burst, one, 0)

    def arrived(k, ref, unit, which):
        first = pl.ds(unit, (burst - 1) * unit) if unit else pl.ds(1, burst - 1)
        rest = pl.ds(0, burst * unit) if unit else pl.ds(0, burst)
        if isinstance(k, int) and k == 0:
            part = ref.at[first]
        else:
            part = ref.at[rest]
        pltpu.make_async_copy(part, part, recv_sem.at[which, k]).wait()

    def sent(part, which):
        pltpu.make_async_copy(part, part, send_sem.at[which]).wait()

    def source_at(k):
        return lax.rem(me // burst - k + bursts, bursts)

    def wide_at(k):
        return pl.ds(pl.multiple_of(burst_at(k) * WIDE, WIDE), WIDE)

    def produce(fill, source, target, which):
        fill(0)

        def middle(k, carry):
            fill(k)
            ship(k - 1, source, target, which)
            return carry

        lax.fori_loop(1, bursts, middle, 0)

    def encode(i, carry):
        load_adj(i).wait()
        at = tile_of(i)
        sums = dot32(adj_s[at, :node_rows], feat_ref[...]) + dot32(
            adj_s[at, node_rows:], arr_ref[...]
        )
        mean = (sums / deg_ref[at, :1]).astype(jnp.bfloat16)
        agg_s[at, :] = mean
        emb_s[at, :] = (dot32(feat_ref[at, :], ws_ref[...]) + dot32(mean, wn_ref[...])).astype(
            jnp.bfloat16
        )
        return carry

    lax.fori_loop(0, tiles, encode, 0)
    pl.semaphore_wait(barrier, peers - 1)

    def serve(k):
        at = wide_at(k)
        asked = jnp.transpose(jnp.broadcast_to(want_ref[:, at], (8, WIDE)))[:, :1]
        served_s[at, :] = dot32(pick(asked, 0, node_rows, 1), emb_s[...]).astype(jnp.bfloat16)

    served_of = lambda p: served_s.at[rows_of(p), :]
    produce(serve, served_of, recv_s.at[rows_of(me), :], 0)
    recv_s[rows_of(me), :] = served_s[rows_of(me), :]
    small_s[...] = jnp.zeros(small_s.shape, jnp.float32)
    ship(bursts - 1, served_of, recv_s.at[rows_of(me), :], 0)

    def columns(i, carry):
        at = pl.ds(pl.multiple_of(i * WIDE, WIDE), WIDE)
        cols_s[at, :] = jnp.transpose(pair_ref[:, at])
        return carry

    lax.fori_loop(0, pairs // WIDE, columns, 0)
    for k in range(bursts):
        arrived(k, recv_s, block, 0)
        b = source_at(k)
        here = pl.ds(pl.multiple_of(b * WIDE, WIDE), WIDE)

        def gather(i, carry):
            at = pl.ds(pl.multiple_of(i * TALL, TALL), TALL)
            for side, rows in ((0, left_s), (1, right_s)):
                ends = cols_s[at, side : side + 1].astype(jnp.int32)
                found = dot32(pick(ends, b * WIDE, WIDE, 1), recv_s[here, :]).astype(
                    jnp.bfloat16
                )
                rows[at, :] = found if k == 0 else rows[at, :] + found
            return carry

        lax.fori_loop(0, pairs // TALL, gather, 0)

    def forward(i, carry):
        at = pl.ds(pl.multiple_of(i * WIDE, WIDE), WIDE)
        cols = cols_s[at, :]
        left = left_s[at, :]
        right = right_s[at, :]
        pre = dot32(left, wh_ref[:width, :]) + dot32(right, wh_ref[width:, :]) + bias_ref[...]
        hidden = jnp.maximum(pre, 0.0)
        logit = jnp.sum(hidden * wo_ref[...], axis=1, keepdims=True)
        logit_ref[:, at] = jnp.transpose(jnp.broadcast_to(logit, (WIDE, LANES)))[:1]
        slope = cols[:, 2:3] * (jax.nn.sigmoid(logit) - cols[:, 3:4])
        delta = jnp.where(pre > 0, slope * wo_ref[...], 0.0)
        small_s[0:1, :] += jnp.sum(delta, axis=0, keepdims=True)
        small_s[1:2, :] += jnp.sum(slope * hidden, axis=0, keepdims=True)
        delta_b = delta.astype(jnp.bfloat16)
        delta_s[at, :] = delta_b
        pgl_s[at, :] = dot_nt(delta_b, wh_ref[:width, :]).astype(jnp.bfloat16)
        pgr_s[at, :] = dot_nt(delta_b, wh_ref[width:, :]).astype(jnp.bfloat16)
        return carry

    lax.fori_loop(0, pairs // WIDE, forward, 0)
    ends_row = pair_ref[0:2, :].astype(jnp.int32)

    def collect(k):
        first = burst_at(k) * WIDE
        total = dot32(pick(ends_row[0:1, :], first, WIDE, 0), pgl_s[...]) + dot32(
            pick(ends_row[1:2, :], first, WIDE, 0), pgr_s[...]
        )
        rgrad_s[wide_at(k), :] = total.astype(jnp.bfloat16)

    rgrad_of = lambda p: rgrad_s.at[rows_of(p), :]
    produce(collect, rgrad_of, back_s.at[rows_of(me), :], 1)
    back_s[rows_of(me), :] = rgrad_s[rows_of(me), :]
    ship(bursts - 1, rgrad_of, back_s.at[rows_of(me), :], 1)
    gw_s[2 * width : 3 * width, :] = dot_tn(left_s[...], delta_s[...])
    gw_s[3 * width :, :] = dot_tn(right_s[...], delta_s[...])
    for k in range(bursts):
        arrived(k, back_s, block, 1)
        b = source_at(k)
        here = pl.ds(pl.multiple_of(b * WIDE, WIDE), WIDE)

        def put(i, carry):
            at = pl.ds(pl.multiple_of(i * TALL, TALL), TALL)
            found = dot32(pick(want_ref[:, here], i * TALL, TALL, 0), back_s[here, :])
            gfeat_ref[at, :] = found if k == 0 else gfeat_ref[at, :] + found
            return carry

        lax.fori_loop(0, node_rows // TALL, put, 0)
    gradb_s[...] = gfeat_ref[...].astype(jnp.bfloat16)
    gw_s[:width, :] = dot_tn(feat_ref[...], gradb_s[...])
    gw_s[width : 2 * width, :] = dot_tn(agg_s[...], gradb_s[...])
    half = block // 2

    def halves(rows):
        wide = rows.reshape(burst, half, width)
        return jnp.concatenate([wide[:, :, :LANES], wide[:, :, LANES:]], axis=1).astype(
            jnp.bfloat16
        )

    def whole(blocks):
        wide = blocks.astype(jnp.float32)
        return jnp.concatenate([wide[:, :half], wide[:, half : 2 * half]], axis=2)

    def weight_terms(k):
        t = burst_at(k)
        part_s[pl.ds(t * burst, burst)] = halves(gw_s[tile_of(t), :])

    part_of = lambda p: part_s.at[p]
    produce(weight_terms, part_of, precv_s.at[me], 2)
    precv_s[me] = part_s[me]
    degree = jnp.concatenate([degt_ref[0, 0:1, :], degt_ref[1, 0:1, :]], axis=1)
    gt_s[...] = (dot_nt(wn_ref[...], gradb_s[...]) / degree).astype(jnp.bfloat16)
    ship(bursts - 1, part_of, precv_s.at[me], 2)

    def table_grad(first):
        cols = pl.ds(pl.multiple_of(first, TILE), TILE)
        return jnp.transpose(dot32(gt_s[...], adj_s[:, cols]))

    def return_halo(k):
        t = burst_at(k)
        halo_s[pl.ds(t * burst, burst)] = halves(table_grad(node_rows + t * TILE))

    halo_of = lambda p: halo_s.at[p]
    produce(return_halo, halo_of, hrecv_s.at[me], 3)
    hrecv_s[me] = halo_s[me]

    def direct(i, carry):
        at = tile_of(i)
        gfeat_ref[at, :] = dot_nt(gradb_s[at, :], ws_ref[...]) + table_grad(i * TILE)
        return carry

    direct(0, 0)
    ship(bursts - 1, halo_of, hrecv_s.at[me], 3)
    for k in range(bursts):
        arrived(k, precv_s, 0, 2)
    own = jnp.sum(precv_s[...].astype(jnp.float32), axis=0)
    small = small_s[...]
    small_hi = small.astype(jnp.bfloat16).astype(jnp.float32)
    small_lo = small - small_hi
    lines = [
        part[r : r + 1, c : c + LANES]
        for part in (small_hi, small_lo)
        for r in range(2)
        for c in (0, LANES)
    ]
    share_s[...] = jnp.concatenate([own] + lines, axis=0).astype(jnp.bfloat16)
    direct(1, 0)

    def share(i, carry):
        p = lax.rem(me + i * 51, peers)
        pltpu.make_async_remote_copy(
            src_ref=share_s,
            dst_ref=srecv_s.at[me],
            send_sem=send_sem.at[4],
            recv_sem=recv_sem.at[4, 0],
            device_id=device(p),
            device_id_type=MESH,
        ).start()
        return carry

    lax.fori_loop(1, peers, share, 0)
    srecv_s[me] = share_s[...]
    lax.fori_loop(2, tiles, direct, 0)
    for k in range(bursts):
        arrived(k, hrecv_s, 0, 3)
    hrows_s[...] = whole(hrecv_s[...]).reshape(peers * half, width).astype(jnp.bfloat16)

    def place(i, carry):
        at = pl.ds(pl.multiple_of(i * TALL, TALL), TALL)
        hot = pick(halo_ref[...], i * TALL, TALL, 0)
        gfeat_ref[at, :] += dot32(hot, hrows_s[...])
        return carry

    lax.fori_loop(0, node_rows // TALL, place, 0)
    for which, ref in ((0, served_s), (1, rgrad_s)):
        sent(ref.at[pl.ds(block, recv_rows - block), :], which)
    for which, ref in ((2, part_s), (3, halo_s), (4, srecv_s)):
        sent(ref.at[pl.ds(1, peers - 1)], which)
    others = srecv_s.at[pl.ds(1, peers - 1)]
    pltpu.make_async_copy(others, others, recv_sem.at[4, 0]).wait()
    everyone = whole(srecv_s[...])
    quarter = peers // 4
    gself_ref[...] = everyone[:quarter].reshape(width, width)
    gneigh_ref[...] = everyone[quarter : 2 * quarter].reshape(width, width)
    ghid_ref[...] = everyone[2 * quarter :].reshape(2 * width, width)
    total = jnp.sum(srecv_s[...].astype(jnp.float32)[:, block:], axis=0)
    total = total[:4] + total[4:]
    gbias_ref[...] = jnp.concatenate([total[0:1], total[1:2]], axis=1)
    gout_ref[...] = jnp.concatenate([total[2:3], total[3:4]], axis=1)


def train_step(
    adj, features, arrived, deg, degt, want_row, pair_rows, halo_pad, w_self, w_neigh, w_hidden,
    bias, w_out, peers
):
    node_rows, width = features.shape
    table_rows = adj.shape[1]
    recv_rows = want_row.shape[1]
    pairs = pair_rows.shape[1]
    block = recv_rows // peers
    lines = width * 4 * width // peers // LANES + 8
    bf16 = lambda *shape: pltpu.VMEM(shape, jnp.bfloat16)
    return pl.pallas_call(
        step_kernel,
        out_shape=(
            jax.ShapeDtypeStruct((1, pairs), jnp.float32),
            jax.ShapeDtypeStruct((node_rows, width), jnp.float32),
            jax.ShapeDtypeStruct((width, width), jnp.float32),
            jax.ShapeDtypeStruct((width, width), jnp.float32),
            jax.ShapeDtypeStruct((2 * width, width), jnp.float32),
            jax.ShapeDtypeStruct((1, width), jnp.float32),
            jax.ShapeDtypeStruct((1, width), jnp.float32),
        ),
        in_specs=[pl.BlockSpec(memory_space=pl.ANY)] + [VMEM] * 12,
        out_specs=(VMEM,) * 7,
        scratch_shapes=[
            bf16(node_rows, table_rows),
            bf16(node_rows, width),
            bf16(node_rows, width),
            bf16(recv_rows, width),
            bf16(recv_rows, width),
            bf16(pairs, width),
            bf16(pairs, width),
            bf16(pairs, width),
            bf16(pairs, width),
            bf16(pairs, width),
            bf16(recv_rows, width),
            bf16(recv_rows, width),
            bf16(node_rows, width),
            bf16(width, node_rows),
            pltpu.VMEM((4 * width, width), jnp.float32),
            pltpu.VMEM((8, width), jnp.float32),
            pltpu.VMEM((pairs, 8), jnp.float32),
            bf16(peers, block, LANES),
            bf16(peers, block, LANES),
            bf16(peers, block, LANES),
            bf16(peers, block, LANES),
            bf16(table_rows - node_rows, width),
            bf16(lines, LANES),
            bf16(peers, lines, LANES),
            pltpu.SemaphoreType.DMA((node_rows // TILE,)),
            pltpu.SemaphoreType.DMA((5,)),
            pltpu.SemaphoreType.DMA((5, recv_rows // WIDE)),
        ],
        compiler_params=pltpu.CompilerParams(
            vmem_limit_bytes=62 * 2**20, collective_id=0, has_side_effects=True
        ),
        cost_estimate=cost(30_000_000_000, 24 * 2**20),
        name="train_step",
    )(
        adj, features, arrived, deg, degt, want_row, pair_rows, halo_pad, w_self, w_neigh,
        w_hidden, bias, w_out,
    )


def per_device(
    features,
    edge_src,
    edge_dst,
    edge_count,
    halo_index,
    request_rows,
    pair_ends,
    labels,
    pair_weight,
    w_self,
    w_neigh,
    w_hidden,
    b_hidden,
    w_out,
):
    node_rows, width = features.shape
    peers = lax.axis_size(AXES)
    halo_len = halo_index.shape[2]
    halo_rows = peers * halo_len
    req_len = request_rows.shape[2]
    recv_rows = peers * req_len
    nodes = lax.iota(jnp.int32, node_rows)

    halo_pad = jnp.pad(halo_index[0], ((0, 0), (0, req_len - halo_len)), constant_values=-1)
    halo_pick = (halo_pad.reshape(-1)[:, None] == nodes[None, :]).astype(jnp.bfloat16)
    asked = jnp.concatenate([request_rows[0] // 64, request_rows[0] % 64], axis=1)
    asked = jnp.pad(
        asked.astype(jnp.float32)[:, None, :],
        ((0, 0), (halo_len, req_len - halo_len - 1), (0, width - 2 * req_len)),
    ).reshape(peers * req_len, width)
    outgoing = (dot32(halo_pick, features) + asked).astype(jnp.bfloat16)
    outgoing = outgoing.reshape(peers, req_len, width)
    first = exchange(outgoing)
    edge_src, edge_dst, _ = lax.optimization_barrier((edge_src, edge_dst, outgoing))

    adj, deg, degt = adjacency(edge_src, edge_dst, edge_count, node_rows, node_rows + halo_rows)
    arrived = first[:, :halo_len].reshape(halo_rows, width)
    codes = first[:, halo_len, : 2 * req_len].astype(jnp.int32)
    wanted = (codes[:, :req_len] * 64 + codes[:, req_len:]).reshape(recv_rows)
    want_row = wanted.reshape(1, recv_rows)
    pair_rows = jnp.concatenate(
        [
            pair_ends.T.astype(jnp.float32),
            pair_weight[None],
            labels.astype(jnp.float32)[None],
            jnp.zeros((4, pair_weight.shape[0]), jnp.float32),
        ],
        axis=0,
    )
    logits, grad_features, grad_self, grad_neigh, grad_hidden, grad_bias, grad_out = train_step(
        adj, features, arrived, deg, degt, want_row, pair_rows,
        halo_index[0].reshape(1, halo_rows), w_self, w_neigh, w_hidden, b_hidden[None],
        w_out[None], peers
    )
    return (
        logits[0],
        grad_features,
        grad_self,
        grad_neigh,
        grad_hidden,
        grad_bias[0],
        grad_out[0],
    )


def solution(mesh):
    split = P(AXES)
    in_specs = (
        P(AXES, None),
        split,
        split,
        split,
        P(AXES, None, None),
        P(AXES, None, None),
        P(AXES, None),
        split,
        split,
        P(),
        P(),
        P(),
        P(),
        P(),
    )
    out_specs = (split, P(AXES, None), P(), P(), P(), P(), P())
    return jax.shard_map(
        per_device, mesh=mesh, in_specs=in_specs, out_specs=out_specs, check_vma=False
    )
```

```python
import jax
import jax.numpy as jnp
from jax import lax
from jax.experimental import pallas as pl
from jax.experimental.pallas import tpu as pltpu
from jax.sharding import PartitionSpec as P

AXES = ("dom", "grp")
LANES = 128
GROUP = 8
STRIDE = LANES // GROUP
BATCH = 8
TILE = 256
WIDE = 512
TALL = 1024
LOGICAL = pl.DeviceIdType.LOGICAL
CLASH = 1 << 20
VMEM = pl.BlockSpec(memory_space=pltpu.VMEM)
SMEM = pl.BlockSpec(memory_space=pltpu.SMEM)
ANY = pl.BlockSpec(memory_space=pl.ANY)


def dot32(a, b):
    return jnp.dot(a, b, preferred_element_type=jnp.float32)


def dot_nt(a, b):
    return lax.dot_general(a, b, (((1,), (1,)), ((), ())), preferred_element_type=jnp.float32)


def dot_tn(a, b):
    return lax.dot_general(a, b, (((0,), (0,)), ((), ())), preferred_element_type=jnp.float32)


def params(mib):
    return pltpu.CompilerParams(vmem_limit_bytes=mib * 2**20)


def cost(flops, size):
    return pl.CostEstimate(flops=flops, bytes_accessed=size, transcendentals=0)


def tile_of(i):
    return pl.ds(pl.multiple_of(i * TILE, TILE), TILE)


def pick(index, first, count, axis):
    shape = (index.shape[0], count) if axis == 1 else (count, index.shape[1])
    ids = lax.broadcasted_iota(jnp.int32, shape, axis) + first
    return jnp.where(index == ids, 1.0, 0.0).astype(jnp.bfloat16)


def slots_kernel(half, panels, count_ref, src_ref, dst_ref, row_ref, unit_ref):
    chunks = src_ref.shape[0]
    lane = lax.broadcasted_iota(jnp.int32, (chunks, LANES), 1)
    slot = lax.broadcasted_iota(jnp.int32, (chunks, LANES), 0) * LANES + lane
    live = slot < count_ref[0]
    src = src_ref[...]
    dst = dst_ref[...]
    upper = jnp.where(dst >= half, 1, 0)
    row = jnp.right_shift(src, 7) * half + dst - upper * half
    row = jnp.where(live, row, half * panels + lane // STRIDE)
    unit_ref[...] = jnp.where(live, jnp.bitwise_and(src, LANES - 1) + upper * LANES, 2 * LANES)
    clash = jnp.zeros((chunks, LANES), jnp.int32)
    for k in range(1, GROUP // 2 + 1):
        clash = clash + jnp.where(row == pltpu.roll(row, k * STRIDE, 1), 1, 0)
    any_clash = jnp.max(clash.astype(jnp.float32), axis=1, keepdims=True) > 0.0
    row_ref[...] = row + jnp.where(any_clash & (lane == 0), CLASH, 0)


def counts_kernel(half, panels, row_ref, unit_ref, adj_ref, deg_ref, degt_ref, even, odd, units):
    step = pl.program_id(0)
    chunks = unit_ref.shape[0]

    @pl.when(step == 0)
    def _():
        lane = lax.broadcasted_iota(jnp.int32, (LANES, LANES), 1)
        share = half * panels // (chunks // BATCH)

        def prepare(i, carry):
            part = pl.ds(pl.multiple_of(i * share, share), share)
            for k in range(BATCH):
                c = i * BATCH + k
                wide = jnp.transpose(
                    jnp.broadcast_to(unit_ref[pl.ds(c, 1), :], (LANES, LANES))
                )
                units[pl.ds(pl.multiple_of(c * LANES, LANES), LANES), :] = jnp.where(
                    wide == lane, 1, jnp.where(wide == lane + LANES, 65536, 0)
                )
            even[part, :] = jnp.zeros((share, LANES), jnp.int32)
            odd[part, :] = jnp.zeros((share, LANES), jnp.int32)
            return carry

        lax.fori_loop(0, chunks // BATCH, prepare, 0)

        def chunk(c, carry):
            base = pl.multiple_of(c * LANES, LANES)
            places = row_ref.at[pl.ds(base, LANES)]
            head = places[0]

            def load(s):
                words = odd if s % 2 else even
                at = [places[s + STRIDE * t] for t in range(GROUP)]
                new = [
                    words[pl.ds(a, 1), :] + units[pl.ds(base + (s + STRIDE * t), 1), :]
                    for t, a in enumerate(at)
                ]
                return words, at, new

            def store(words, at, new):
                for a, n in zip(at, new):
                    words[pl.ds(a, 1), :] = n

            @pl.when(head < CLASH)
            def _():
                held = load(0)
                for s in range(1, STRIDE):
                    following = load(s)
                    store(*held)
                    held = following
                store(*held)

            @pl.when(head >= CLASH)
            def _():
                for j in range(LANES):
                    words = odd if j % 2 else even
                    a = places[j]
                    if j == 0:
                        a = a - CLASH
                    words[pl.ds(a, 1), :] = words[pl.ds(a, 1), :] + units[pl.ds(base + j, 1), :]

            return carry

        lax.fori_loop(0, chunks, chunk, 0)

    first = step * TILE
    total = jnp.zeros((TILE, LANES), jnp.int32)
    for p in range(panels):
        part = pl.ds(pl.multiple_of(p * half + first, TILE), TILE)
        word = even[part, :] + odd[part, :]
        total = total + word
        cols = slice(p * LANES, (p + 1) * LANES)
        for h, count in enumerate((jnp.bitwise_and(word, 0xFFFF), jnp.right_shift(word, 16))):
            adj_ref[h, :, cols] = count.astype(jnp.float32).astype(jnp.bfloat16)
    for h, count in enumerate((jnp.bitwise_and(total, 0xFFFF), jnp.right_shift(total, 16))):
        degree = jnp.sum(count.astype(jnp.float32), axis=1, keepdims=True)
        wide = jnp.broadcast_to(jnp.maximum(degree, 1.0), (TILE, LANES))
        deg_ref[h] = wide
        degt_ref[h] = jnp.transpose(wide)[:8]


def adjacency(edge_src, edge_dst, edge_count, node_rows, table_rows):
    half = node_rows // 2
    panels = table_rows // LANES
    chunks = edge_src.shape[0] // LANES
    grid_shape = (chunks, LANES)
    row, unit = pl.pallas_call(
        lambda *refs: slots_kernel(half, panels, *refs),
        out_shape=(
            jax.ShapeDtypeStruct(grid_shape, jnp.int32),
            jax.ShapeDtypeStruct(grid_shape, jnp.int32),
        ),
        in_specs=[SMEM, VMEM, VMEM],
        out_specs=(VMEM, VMEM),
        compiler_params=params(60),
        name="slots",
    )(edge_count, edge_src.reshape(grid_shape), edge_dst.reshape(grid_shape))
    adj, deg, degt = pl.pallas_call(
        lambda *refs: counts_kernel(half, panels, *refs),
        grid=(half // TILE,),
        out_shape=(
            jax.ShapeDtypeStruct((2, half, table_rows), jnp.bfloat16),
            jax.ShapeDtypeStruct((2, half, LANES), jnp.float32),
            jax.ShapeDtypeStruct((2, 8, half), jnp.float32),
        ),
        in_specs=[SMEM, pl.BlockSpec(grid_shape, lambda i: (0, 0))],
        out_specs=(
            pl.BlockSpec((2, TILE, table_rows), lambda i: (0, i, 0)),
            pl.BlockSpec((2, TILE, LANES), lambda i: (0, i, 0)),
            pl.BlockSpec((2, 8, TILE), lambda i: (0, 0, i)),
        ),
        scratch_shapes=[
            pltpu.VMEM((half * panels + GROUP, LANES), jnp.int32),
            pltpu.VMEM((half * panels + GROUP, LANES), jnp.int32),
            pltpu.VMEM((edge_src.shape[0], LANES), jnp.int32),
        ],
        compiler_params=params(60),
        cost_estimate=cost(60_000_000, 16 * 2**20),
        name="counts",
    )(row.reshape(-1), unit)
    return adj.reshape(node_rows, table_rows), deg.reshape(node_rows, LANES), degt


def step_kernel(
    adj_ref,
    feat_ref,
    deg_ref,
    degt_ref,
    ask_ref,
    halo_ref,
    ends_ref,
    weight_ref,
    label_ref,
    ws_ref,
    wn_ref,
    wh_ref,
    bias_ref,
    wo_ref,
    logit_ref,
    gfeat_ref,
    gself_ref,
    gneigh_ref,
    ghid_ref,
    gbias_ref,
    gout_ref,
    adj_s,
    gfeat_s,
    pair_s,
    hcol_s,
    hrow_s,
    wcol_s,
    wrow_s,
    first_s,
    frecv_s,
    arr_s,
    emb_s,
    agg_s,
    served_s,
    recv_s,
    left_s,
    right_s,
    delta_s,
    pgl_s,
    pgr_s,
    rgrad_s,
    back_s,
    gradb_s,
    gt_s,
    gw_s,
    small_s,
    cols_s,
    part_s,
    precv_s,
    halo_s,
    hrecv_s,
    hrows_s,
    share_s,
    srecv_s,
    adj_sem,
    send_sem,
    recv_sem,
):
    node_rows, width = feat_ref.shape
    block, peers = ask_ref.shape
    half = halo_ref.shape[0]
    recv_rows = peers * block
    pairs = ends_ref.shape[1]
    grp = lax.axis_size("grp")
    me = lax.axis_index("dom") * grp + lax.axis_index("grp")
    burst = WIDE // block
    bursts = peers // burst
    tiles = node_rows // TILE
    barrier = pltpu.get_barrier_semaphore()

    def load_adj(i):
        return pltpu.make_async_copy(
            adj_ref.at[tile_of(i), :], adj_s.at[tile_of(i), :], adj_sem.at[i]
        )

    def fetch(i, carry):
        load_adj(i).start()
        return carry

    lax.fori_loop(0, tiles, fetch, 0)

    def greet(i, carry):
        pl.semaphore_signal(
            barrier, inc=1, device_id=lax.rem(me + i, peers), device_id_type=LOGICAL
        )
        return carry

    lax.fori_loop(1, peers, greet, 0)

    def rows_of(p):
        return pl.ds(pl.multiple_of(p * block, block), block)

    def burst_at(k):
        return lax.rem(me // burst + k, bursts)

    def ship(k, source, target, which):
        def one(i, carry):
            p = burst_at(k) * burst + lax.rem(lax.rem(me, burst) + i, burst)

            @pl.when(p != me)
            def _():
                pltpu.make_async_remote_copy(
                    src_ref=source(p),
                    dst_ref=target,
                    send_sem=send_sem.at[which],
                    recv_sem=recv_sem.at[which, k],
                    device_id=p,
                    device_id_type=LOGICAL,
                ).start()

            return carry

        lax.fori_loop(0, burst, one, 0)

    def arrived(k, ref, unit, which):
        first = pl.ds(unit, (burst - 1) * unit) if unit else pl.ds(1, burst - 1)
        rest = pl.ds(0, burst * unit) if unit else pl.ds(0, burst)
        if isinstance(k, int) and k == 0:
            part = ref.at[first]
        else:
            part = ref.at[rest]
        pltpu.make_async_copy(part, part, recv_sem.at[which, k]).wait()

    def sent(part, which):
        pltpu.make_async_copy(part, part, send_sem.at[which]).wait()

    def source_at(k):
        return lax.rem(me // burst - k + bursts, bursts)

    def wide_at(k):
        return pl.ds(pl.multiple_of(burst_at(k) * WIDE, WIDE), WIDE)

    def produce(fill, source, target, which):
        fill(0)

        def middle(k, carry):
            fill(k)
            ship(k - 1, source, target, which)
            return carry

        lax.fori_loop(1, bursts, middle, 0)

    def halves(rows):
        wide = rows.reshape(burst, half, width)
        return jnp.concatenate([wide[:, :, :LANES], wide[:, :, LANES:]], axis=1)

    def whole(blocks):
        wide = blocks.astype(jnp.float32)
        return jnp.concatenate([wide[:, :half], wide[:, half : 2 * half]], axis=2)

    def spread(table, depth):
        shape = (table.shape[0], depth, table.shape[1])
        keep = lax.broadcasted_iota(jnp.int32, shape, 1) == lax.broadcasted_iota(
            jnp.int32, shape, 2
        )
        wide = jnp.broadcast_to(table[:, None, :], shape)
        one = jnp.sum(jnp.where(keep, wide, 0.0), axis=2, keepdims=True)
        return one.reshape(shape[0] * depth, 1)

    def as_row(col):
        return jnp.transpose(jnp.broadcast_to(col, (col.shape[0], LANES)))[:8]

    hcol_s[...] = spread(jnp.transpose(halo_ref[...].astype(jnp.float32)), half)
    asks = ask_ref[...]
    ask_table = jnp.transpose(
        jnp.concatenate(
            [
                jnp.right_shift(asks, 6).astype(jnp.float32),
                jnp.bitwise_and(asks, 63).astype(jnp.float32),
                jnp.zeros((LANES - 2 * block, peers), jnp.float32),
            ],
            axis=0,
        )
    )
    wcol_s[0:peers, :] = ask_table

    def outgoing(t, carry):
        hot = pick(hcol_s[tile_of(t), :].astype(jnp.int32), 0, node_rows, 1)
        part = pl.ds(pl.multiple_of(t * burst, burst), burst)
        asked = jnp.broadcast_to(wcol_s[part, :][:, None, :], (burst, 8, LANES))
        first_s[part] = jnp.concatenate(
            [halves(dot32(hot, feat_ref[...])), asked], axis=1
        ).astype(jnp.bfloat16)
        return carry

    lax.fori_loop(0, bursts, outgoing, 0)

    def local_sums(i, carry):
        load_adj(i).wait()
        at = tile_of(i)
        gfeat_s[at, :] = dot32(adj_s[at, :node_rows], feat_ref[...])
        return carry

    lax.fori_loop(0, tiles, local_sums, 0)
    pl.semaphore_wait(barrier, peers - 1)
    first_of = lambda p: first_s.at[p]
    for k in range(bursts):
        ship(k, first_of, frecv_s.at[me], 0)
    frecv_s[me] = first_s[me]
    pair_s[...] = jnp.concatenate(
        [
            ends_ref[...].astype(jnp.float32),
            weight_ref[...],
            label_ref[...].astype(jnp.float32),
            jnp.zeros((4, pairs), jnp.float32),
        ],
        axis=0,
    )

    def columns(i, carry):
        at = pl.ds(pl.multiple_of(i * WIDE, WIDE), WIDE)
        cols_s[at, :] = jnp.transpose(pair_s[:, at])
        return carry

    lax.fori_loop(0, pairs // WIDE, columns, 0)
    hrow_s[...] = as_row(hcol_s[...])
    for k in range(bursts):
        arrived(k, frecv_s, 0, 0)
    arr_s[...] = whole(frecv_s[...]).reshape(peers * half, width).astype(jnp.bfloat16)
    codes = jnp.max(frecv_s[...].astype(jnp.float32)[:, 2 * half :], axis=1)
    wcol_s[0:peers, :] = codes * 64.0 + pltpu.roll(codes, LANES - block, 1)

    def encode(i, carry):
        at = tile_of(i)
        sums = gfeat_s[at, :] + dot32(adj_s[at, node_rows:], arr_s[...])
        mean = (sums / deg_ref[at, :1]).astype(jnp.bfloat16)
        agg_s[at, :] = mean
        emb_s[at, :] = (dot32(feat_ref[at, :], ws_ref[...]) + dot32(mean, wn_ref[...])).astype(
            jnp.bfloat16
        )
        return carry

    lax.fori_loop(0, tiles, encode, 0)

    def serve(k):
        at = wide_at(k)
        part = pl.ds(pl.multiple_of(burst_at(k) * burst, burst), burst)
        asked = spread(wcol_s[part, :], block)
        wrow_s[:, at] = as_row(asked)
        hot = pick(asked.astype(jnp.int32), 0, node_rows, 1)
        served_s[at, :] = dot32(hot, emb_s[...]).astype(jnp.bfloat16)

    served_of = lambda p: served_s.at[rows_of(p), :]
    produce(serve, served_of, recv_s.at[rows_of(me), :], 1)
    recv_s[rows_of(me), :] = served_s[rows_of(me), :]
    small_s[...] = jnp.zeros(small_s.shape, jnp.float32)
    ship(bursts - 1, served_of, recv_s.at[rows_of(me), :], 1)

    for k in range(bursts):
        arrived(k, recv_s, block, 1)
        b = source_at(k)
        here = pl.ds(pl.multiple_of(b * WIDE, WIDE), WIDE)

        def gather(i, carry):
            at = pl.ds(pl.multiple_of(i * TALL, TALL), TALL)
            for side, rows in ((0, left_s), (1, right_s)):
                ends = cols_s[at, side : side + 1].astype(jnp.int32)
                found = dot32(pick(ends, b * WIDE, WIDE, 1), recv_s[here, :]).astype(
                    jnp.bfloat16
                )
                rows[at, :] = found if k == 0 else rows[at, :] + found
            return carry

        lax.fori_loop(0, pairs // TALL, gather, 0)

    def forward(i, carry):
        at = pl.ds(pl.multiple_of(i * WIDE, WIDE), WIDE)
        cols = cols_s[at, :]
        left = left_s[at, :]
        right = right_s[at, :]
        pre = dot32(left, wh_ref[:width, :]) + dot32(right, wh_ref[width:, :]) + bias_ref[...]
        hidden = jnp.maximum(pre, 0.0)
        logit = jnp.sum(hidden * wo_ref[...], axis=1, keepdims=True)
        logit_ref[:, at] = jnp.transpose(jnp.broadcast_to(logit, (WIDE, LANES)))[:1]
        slope = cols[:, 2:3] * (jax.nn.sigmoid(logit) - cols[:, 3:4])
        delta = jnp.where(pre > 0, slope * wo_ref[...], 0.0)
        small_s[0:1, :] += jnp.sum(delta, axis=0, keepdims=True)
        small_s[1:2, :] += jnp.sum(slope * hidden, axis=0, keepdims=True)
        delta_b = delta.astype(jnp.bfloat16)
        delta_s[at, :] = delta_b
        pgl_s[at, :] = dot_nt(delta_b, wh_ref[:width, :]).astype(jnp.bfloat16)
        pgr_s[at, :] = dot_nt(delta_b, wh_ref[width:, :]).astype(jnp.bfloat16)
        return carry

    lax.fori_loop(0, pairs // WIDE, forward, 0)
    ends_row = ends_ref[...]

    def collect(k):
        first = burst_at(k) * WIDE
        total = dot32(pick(ends_row[0:1, :], first, WIDE, 0), pgl_s[...]) + dot32(
            pick(ends_row[1:2, :], first, WIDE, 0), pgr_s[...]
        )
        rgrad_s[wide_at(k), :] = total.astype(jnp.bfloat16)

    rgrad_of = lambda p: rgrad_s.at[rows_of(p), :]
    produce(collect, rgrad_of, back_s.at[rows_of(me), :], 2)
    back_s[rows_of(me), :] = rgrad_s[rows_of(me), :]
    ship(bursts - 1, rgrad_of, back_s.at[rows_of(me), :], 2)
    gw_s[2 * width : 3 * width, :] = dot_tn(left_s[...], delta_s[...])
    gw_s[3 * width :, :] = dot_tn(right_s[...], delta_s[...])
    for k in range(bursts):
        arrived(k, back_s, block, 2)
        b = source_at(k)
        here = pl.ds(pl.multiple_of(b * WIDE, WIDE), WIDE)

        def put(i, carry):
            at = pl.ds(pl.multiple_of(i * TALL, TALL), TALL)
            found = dot32(pick(wrow_s[0:1, here].astype(jnp.int32), i * TALL, TALL, 0), back_s[here, :])
            gfeat_s[at, :] = found if k == 0 else gfeat_s[at, :] + found
            return carry

        lax.fori_loop(0, node_rows // TALL, put, 0)
    gradb_s[...] = gfeat_s[...].astype(jnp.bfloat16)
    gw_s[:width, :] = dot_tn(feat_ref[...], gradb_s[...])
    gw_s[width : 2 * width, :] = dot_tn(agg_s[...], gradb_s[...])
    def weight_terms(k):
        t = burst_at(k)
        part_s[pl.ds(t * burst, burst)] = halves(gw_s[tile_of(t), :]).astype(jnp.bfloat16)

    part_of = lambda p: part_s.at[p]
    produce(weight_terms, part_of, precv_s.at[me], 3)
    precv_s[me] = part_s[me]
    degree = jnp.concatenate([degt_ref[0, 0:1, :], degt_ref[1, 0:1, :]], axis=1)
    gt_s[...] = (dot_nt(wn_ref[...], gradb_s[...]) / degree).astype(jnp.bfloat16)
    ship(bursts - 1, part_of, precv_s.at[me], 3)

    def table_grad(first):
        cols = pl.ds(pl.multiple_of(first, TILE), TILE)
        return jnp.transpose(dot32(gt_s[...], adj_s[:, cols]))

    def return_halo(k):
        t = burst_at(k)
        halo_s[pl.ds(t * burst, burst)] = halves(
            table_grad(node_rows + t * TILE)
        ).astype(jnp.bfloat16)

    halo_of = lambda p: halo_s.at[p]
    produce(return_halo, halo_of, hrecv_s.at[me], 4)
    hrecv_s[me] = halo_s[me]

    def direct(i, carry):
        at = tile_of(i)
        gfeat_s[at, :] = dot_nt(gradb_s[at, :], ws_ref[...]) + table_grad(i * TILE)
        return carry

    direct(0, 0)
    ship(bursts - 1, halo_of, hrecv_s.at[me], 4)
    for k in range(bursts):
        arrived(k, precv_s, 0, 3)
    own = jnp.sum(precv_s[...].astype(jnp.float32), axis=0)
    small = small_s[...]
    small_hi = small.astype(jnp.bfloat16).astype(jnp.float32)
    small_lo = small - small_hi
    lines = [
        part[r : r + 1, c : c + LANES]
        for part in (small_hi, small_lo)
        for r in range(2)
        for c in (0, LANES)
    ]
    share_s[...] = jnp.concatenate([own] + lines, axis=0).astype(jnp.bfloat16)
    direct(1, 0)

    def share(i, carry):
        p = lax.rem(me + i * 51, peers)
        pltpu.make_async_remote_copy(
            src_ref=share_s,
            dst_ref=srecv_s.at[me],
            send_sem=send_sem.at[5],
            recv_sem=recv_sem.at[5, 0],
            device_id=p,
            device_id_type=LOGICAL,
        ).start()
        return carry

    lax.fori_loop(1, peers, share, 0)
    srecv_s[me] = share_s[...]
    lax.fori_loop(2, tiles, direct, 0)
    for k in range(bursts):
        arrived(k, hrecv_s, 0, 4)
    hrows_s[...] = whole(hrecv_s[...]).reshape(peers * half, width).astype(jnp.bfloat16)

    def place(i, carry):
        at = pl.ds(pl.multiple_of(i * TALL, TALL), TALL)
        hot = pick(hrow_s[0:1, :].astype(jnp.int32), i * TALL, TALL, 0)
        gfeat_s[at, :] += dot32(hot, hrows_s[...])
        return carry

    lax.fori_loop(0, node_rows // TALL, place, 0)
    result = pltpu.make_async_copy(gfeat_s, gfeat_ref, adj_sem.at[0])
    result.start()
    for which, ref in ((1, served_s), (2, rgrad_s)):
        sent(ref.at[pl.ds(block, recv_rows - block), :], which)
    for which, ref in ((0, frecv_s), (3, part_s), (4, halo_s), (5, srecv_s)):
        sent(ref.at[pl.ds(1, peers - 1)], which)
    others = srecv_s.at[pl.ds(1, peers - 1)]
    pltpu.make_async_copy(others, others, recv_sem.at[5, 0]).wait()
    everyone = whole(srecv_s[...])
    quarter = peers // 4
    gself_ref[...] = everyone[:quarter].reshape(width, width)
    gneigh_ref[...] = everyone[quarter : 2 * quarter].reshape(width, width)
    ghid_ref[...] = everyone[2 * quarter :].reshape(2 * width, width)
    total = jnp.sum(srecv_s[...].astype(jnp.float32)[:, block:], axis=0)
    total = total[:4] + total[4:]
    gbias_ref[...] = jnp.concatenate([total[0:1], total[1:2]], axis=1)
    gout_ref[...] = jnp.concatenate([total[2:3], total[3:4]], axis=1)
    result.wait()


def finish_kernel(*refs):
    count = len(refs) // 2
    refs[count][...] = refs[0][...]

    @pl.when(pl.program_id(0) == 0)
    def _():
        for i in range(1, count):
            refs[count + i][...] = refs[i][...]


def finish(arrays):
    rows, width = arrays[0].shape
    specs = [pl.BlockSpec((TILE, width), lambda i: (i, 0))] + [
        pl.BlockSpec(a.shape, lambda i: (0, 0)) for a in arrays[1:]
    ]
    return pl.pallas_call(
        finish_kernel,
        grid=(rows // TILE,),
        out_shape=tuple(jax.ShapeDtypeStruct(a.shape, a.dtype) for a in arrays),
        in_specs=specs,
        out_specs=tuple(specs),
        compiler_params=params(60),
        name="finish",
    )(*arrays)


def train_step(
    adj, features, deg, degt, ask, halo, ends, pair_weight, labels, w_self, w_neigh, w_hidden,
    bias, w_out
):
    node_rows, width = features.shape
    table_rows = adj.shape[1]
    block, peers = ask.shape
    half = halo.shape[0]
    recv_rows = peers * block
    pairs = ends.shape[1]
    lines = 2 * half + 8
    bf16 = lambda *shape: pltpu.VMEM(shape, jnp.bfloat16)
    return pl.pallas_call(
        step_kernel,
        out_shape=(
            jax.ShapeDtypeStruct((1, pairs), jnp.float32),
            jax.ShapeDtypeStruct((node_rows, width), jnp.float32),
            jax.ShapeDtypeStruct((width, width), jnp.float32),
            jax.ShapeDtypeStruct((width, width), jnp.float32),
            jax.ShapeDtypeStruct((2 * width, width), jnp.float32),
            jax.ShapeDtypeStruct((1, width), jnp.float32),
            jax.ShapeDtypeStruct((1, width), jnp.float32),
        ),
        in_specs=[ANY] + [VMEM] * 13,
        out_specs=(VMEM, ANY) + (VMEM,) * 5,
        scratch_shapes=[
            bf16(node_rows, table_rows),
            pltpu.VMEM((node_rows, width), jnp.float32),
            pltpu.VMEM((8, pairs), jnp.float32),
            pltpu.VMEM((peers * half, 1), jnp.float32),
            pltpu.VMEM((8, peers * half), jnp.float32),
            pltpu.VMEM((peers, LANES), jnp.float32),
            pltpu.VMEM((8, recv_rows), jnp.float32),
            bf16(peers, lines, LANES),
            bf16(peers, lines, LANES),
            bf16(peers * half, width),
            bf16(node_rows, width),
            bf16(node_rows, width),
            bf16(recv_rows, width),
            bf16(recv_rows, width),
            bf16(pairs, width),
            bf16(pairs, width),
            bf16(pairs, width),
            bf16(pairs, width),
            bf16(pairs, width),
            bf16(recv_rows, width),
            bf16(recv_rows, width),
            bf16(node_rows, width),
            bf16(width, node_rows),
            pltpu.VMEM((4 * width, width), jnp.float32),
            pltpu.VMEM((8, width), jnp.float32),
            pltpu.VMEM((pairs, 8), jnp.float32),
            bf16(peers, block, LANES),
            bf16(peers, block, LANES),
            bf16(peers, block, LANES),
            bf16(peers, block, LANES),
            bf16(peers * half, width),
            bf16(lines, LANES),
            bf16(peers, lines, LANES),
            pltpu.SemaphoreType.DMA((node_rows // TILE,)),
            pltpu.SemaphoreType.DMA((6,)),
            pltpu.SemaphoreType.DMA((6, recv_rows // WIDE)),
        ],
        compiler_params=pltpu.CompilerParams(
            vmem_limit_bytes=62 * 2**20, collective_id=0, has_side_effects=True
        ),
        cost_estimate=cost(30_000_000_000, 24 * 2**20),
        name="train_step",
    )(
        adj, features, deg, degt, ask, halo, ends, pair_weight, labels, w_self, w_neigh,
        w_hidden, bias, w_out,
    )


def per_device(
    features,
    edge_src,
    edge_dst,
    edge_count,
    halo_index,
    request_rows,
    pair_ends,
    labels,
    pair_weight,
    w_self,
    w_neigh,
    w_hidden,
    b_hidden,
    w_out,
):
    node_rows = features.shape[0]
    halo = halo_index[0].T
    adj, deg, degt = adjacency(edge_src, edge_dst, edge_count, node_rows, node_rows + halo.size)
    logits, grad_features, grad_self, grad_neigh, grad_hidden, grad_bias, grad_out = train_step(
        adj, features, deg, degt, request_rows[0].T, halo, pair_ends.T, pair_weight[None],
        labels[None], w_self, w_neigh, w_hidden, b_hidden[None], w_out[None]
    )
    grad_features, grad_self, grad_neigh, grad_hidden, grad_bias, grad_out, logits = finish(
        (grad_features, grad_self, grad_neigh, grad_hidden, grad_bias, grad_out, logits)
    )
    return (
        logits[0],
        grad_features,
        grad_self,
        grad_neigh,
        grad_hidden,
        grad_bias[0],
        grad_out[0],
    )


def solution(mesh):
    split = P(AXES)
    in_specs = (
        P(AXES, None),
        split,
        split,
        split,
        P(AXES, None, None),
        P(AXES, None, None),
        P(AXES, None),
        split,
        split,
        P(),
        P(),
        P(),
        P(),
        P(),
    )
    out_specs = (split, P(AXES, None), P(), P(), P(), P(), P())
    return jax.shard_map(
        per_device, mesh=mesh, in_specs=in_specs, out_specs=out_specs, check_vma=False
    )
```

```python
import jax
import jax.numpy as jnp
from jax import lax
from jax.experimental import pallas as pl
from jax.experimental.pallas import tpu as pltpu
from jax.sharding import PartitionSpec as P

AXES = ("dom", "grp")
LANES = 128
GROUP = 8
STRIDE = LANES // GROUP
TILE = 256
WIDE = 512
TALL = 1024
LOGICAL = pl.DeviceIdType.LOGICAL
CLASH = 1 << 20
VMEM = pl.BlockSpec(memory_space=pltpu.VMEM)
SMEM = pl.BlockSpec(memory_space=pltpu.SMEM)
ANY = pl.BlockSpec(memory_space=pl.ANY)


def dot32(a, b):
    return jnp.dot(a, b, preferred_element_type=jnp.float32)


def dot_nt(a, b):
    return lax.dot_general(a, b, (((1,), (1,)), ((), ())), preferred_element_type=jnp.float32)


def dot_tn(a, b):
    return lax.dot_general(a, b, (((0,), (0,)), ((), ())), preferred_element_type=jnp.float32)


def params(mib):
    return pltpu.CompilerParams(vmem_limit_bytes=mib * 2**20)


def cost(flops, size):
    return pl.CostEstimate(flops=flops, bytes_accessed=size, transcendentals=0)


def tile_of(i):
    return pl.ds(pl.multiple_of(i * TILE, TILE), TILE)


def pick(index, first, count, axis):
    shape = (index.shape[0], count) if axis == 1 else (count, index.shape[1])
    ids = lax.broadcasted_iota(jnp.int32, shape, axis) + first
    return jnp.where(index == ids, 1.0, 0.0).astype(jnp.bfloat16)


def slots_kernel(half, panels, count_ref, src_ref, dst_ref, row_ref, unit_ref):
    chunks = src_ref.shape[0]
    lane = lax.broadcasted_iota(jnp.int32, (chunks, LANES), 1)
    slot = lax.broadcasted_iota(jnp.int32, (chunks, LANES), 0) * LANES + lane
    live = slot < count_ref[0]
    src = src_ref[...]
    dst = dst_ref[...]
    upper = jnp.where(dst >= half, 1, 0)
    row = jnp.right_shift(src, 7) * half + dst - upper * half
    row = jnp.where(live, row, half * panels + lane // STRIDE)
    unit_ref[...] = jnp.where(live, jnp.bitwise_and(src, LANES - 1) + upper * LANES, 2 * LANES)
    clash = jnp.zeros((chunks, LANES), jnp.int32)
    for k in range(1, GROUP // 2 + 1):
        clash = clash + jnp.where(row == pltpu.roll(row, k * STRIDE, 1), 1, 0)
    any_clash = jnp.max(clash.astype(jnp.float32), axis=1, keepdims=True) > 0.0
    row_ref[...] = row + jnp.where(any_clash & (lane == 0), CLASH, 0)


def counts_kernel(half, panels, row_ref, unit_ref, adj_ref, deg_ref, degt_ref, even, odd, unit_a, unit_b):
    step = pl.program_id(0)
    chunks = unit_ref.shape[0]

    @pl.when(step == 0)
    def _():
        lane = lax.broadcasted_iota(jnp.int32, (LANES, LANES), 1)

        def clear(i, carry):
            even[tile_of(i), :] = jnp.zeros((TILE, LANES), jnp.int32)
            odd[tile_of(i), :] = jnp.zeros((TILE, LANES), jnp.int32)
            return carry

        lax.fori_loop(0, half * panels // TILE, clear, 0)

        def units_of(c):
            c = jnp.minimum(c, chunks - 1)
            wide = jnp.transpose(jnp.broadcast_to(unit_ref[pl.ds(c, 1), :], (LANES, LANES)))
            return jnp.where(wide == lane, 1, jnp.where(wide == lane + LANES, 65536, 0))

        unit_a[...] = units_of(0)

        def chunk(c, units, later):
            base = pl.multiple_of(c * LANES, LANES)
            places = row_ref.at[pl.ds(base, LANES)]
            head = places[0]

            def load(s):
                words = odd if s % 2 else even
                at = [places[s + STRIDE * t] for t in range(GROUP)]
                new = [
                    words[pl.ds(a, 1), :] + units[pl.ds(s + STRIDE * t, 1), :]
                    for t, a in enumerate(at)
                ]
                return words, at, new

            def store(words, at, new):
                for a, n in zip(at, new):
                    words[pl.ds(a, 1), :] = n

            @pl.when(head < CLASH)
            def _():
                coming = units_of(c + 1)
                held = load(0)
                for s in range(1, STRIDE):
                    following = load(s)
                    store(*held)
                    held = following
                store(*held)
                later[...] = coming

            @pl.when(head >= CLASH)
            def _():
                later[...] = units_of(c + 1)
                for j in range(LANES):
                    words = odd if j % 2 else even
                    a = places[j]
                    if j == 0:
                        a = a - CLASH
                    words[pl.ds(a, 1), :] = words[pl.ds(a, 1), :] + units[pl.ds(j, 1), :]

        def two(i, carry):
            chunk(2 * i, unit_a, unit_b)
            chunk(2 * i + 1, unit_b, unit_a)
            return carry

        lax.fori_loop(0, chunks // 2, two, 0)

    first = step * TILE
    total = jnp.zeros((TILE, LANES), jnp.int32)
    for p in range(panels):
        part = pl.ds(pl.multiple_of(p * half + first, TILE), TILE)
        word = even[part, :] + odd[part, :]
        total = total + word
        cols = slice(p * LANES, (p + 1) * LANES)
        for h, count in enumerate((jnp.bitwise_and(word, 0xFFFF), jnp.right_shift(word, 16))):
            adj_ref[h, :, cols] = count.astype(jnp.float32).astype(jnp.bfloat16)
    for h, count in enumerate((jnp.bitwise_and(total, 0xFFFF), jnp.right_shift(total, 16))):
        degree = jnp.sum(count.astype(jnp.float32), axis=1, keepdims=True)
        wide = jnp.broadcast_to(jnp.maximum(degree, 1.0), (TILE, LANES))
        deg_ref[h] = wide
        degt_ref[h] = jnp.transpose(wide)[:8]


def adjacency(edge_src, edge_dst, edge_count, node_rows, table_rows):
    half = node_rows // 2
    panels = table_rows // LANES
    chunks = edge_src.shape[0] // LANES
    grid_shape = (chunks, LANES)
    row, unit = pl.pallas_call(
        lambda *refs: slots_kernel(half, panels, *refs),
        out_shape=(
            jax.ShapeDtypeStruct(grid_shape, jnp.int32),
            jax.ShapeDtypeStruct(grid_shape, jnp.int32),
        ),
        in_specs=[SMEM, VMEM, VMEM],
        out_specs=(VMEM, VMEM),
        compiler_params=params(60),
        name="slots",
    )(edge_count, edge_src.reshape(grid_shape), edge_dst.reshape(grid_shape))
    adj, deg, degt = pl.pallas_call(
        lambda *refs: counts_kernel(half, panels, *refs),
        grid=(half // TILE,),
        out_shape=(
            jax.ShapeDtypeStruct((2, half, table_rows), jnp.bfloat16),
            jax.ShapeDtypeStruct((2, half, LANES), jnp.float32),
            jax.ShapeDtypeStruct((2, 8, half), jnp.float32),
        ),
        in_specs=[SMEM, pl.BlockSpec(grid_shape, lambda i: (0, 0))],
        out_specs=(
            pl.BlockSpec((2, TILE, table_rows), lambda i: (0, i, 0)),
            pl.BlockSpec((2, TILE, LANES), lambda i: (0, i, 0)),
            pl.BlockSpec((2, 8, TILE), lambda i: (0, 0, i)),
        ),
        scratch_shapes=[
            pltpu.VMEM((half * panels + GROUP, LANES), jnp.int32),
            pltpu.VMEM((half * panels + GROUP, LANES), jnp.int32),
            pltpu.VMEM((LANES, LANES), jnp.int32),
            pltpu.VMEM((LANES, LANES), jnp.int32),
        ],
        compiler_params=params(60),
        cost_estimate=cost(60_000_000, 16 * 2**20),
        name="counts",
    )(row.reshape(-1), unit)
    return adj.reshape(node_rows, table_rows), deg.reshape(node_rows, LANES), degt


def step_kernel(
    adj_ref,
    feat_ref,
    deg_ref,
    degt_ref,
    ask_ref,
    halo_ref,
    ends_ref,
    weight_ref,
    label_ref,
    ws_ref,
    wn_ref,
    wh_ref,
    bias_ref,
    wo_ref,
    logit_ref,
    gfeat_ref,
    gself_ref,
    gneigh_ref,
    ghid_ref,
    gbias_ref,
    gout_ref,
    adj_s,
    gfeat_s,
    pair_s,
    hcol_s,
    hrow_s,
    wcol_s,
    wrow_s,
    first_s,
    frecv_s,
    arr_s,
    emb_s,
    agg_s,
    served_s,
    recv_s,
    left_s,
    right_s,
    delta_s,
    pgl_s,
    pgr_s,
    rgrad_s,
    back_s,
    gradb_s,
    gt_s,
    gw_s,
    small_s,
    cols_s,
    part_s,
    precv_s,
    halo_s,
    hrecv_s,
    hrows_s,
    share_s,
    srecv_s,
    adj_sem,
    send_sem,
    recv_sem,
):
    node_rows, width = feat_ref.shape
    block, peers = ask_ref.shape
    half = halo_ref.shape[0]
    recv_rows = peers * block
    pairs = ends_ref.shape[1]
    grp = lax.axis_size("grp")
    me = lax.axis_index("dom") * grp + lax.axis_index("grp")
    burst = WIDE // block
    bursts = peers // burst
    tiles = node_rows // TILE
    barrier = pltpu.get_barrier_semaphore()

    def load_adj(i):
        return pltpu.make_async_copy(
            adj_ref.at[tile_of(i), :], adj_s.at[tile_of(i), :], adj_sem.at[i]
        )

    def fetch(i, carry):
        load_adj(i).start()
        return carry

    lax.fori_loop(0, tiles, fetch, 0)

    def greet(i, carry):
        pl.semaphore_signal(
            barrier, inc=1, device_id=lax.rem(me + i, peers), device_id_type=LOGICAL
        )
        return carry

    lax.fori_loop(1, peers, greet, 0)

    def rows_of(p):
        return pl.ds(pl.multiple_of(p * block, block), block)

    def burst_at(k):
        return lax.rem(me // burst + k, bursts)

    def ship(k, source, target, which):
        def one(i, carry):
            p = burst_at(k) * burst + lax.rem(lax.rem(me, burst) + i, burst)

            @pl.when(p != me)
            def _():
                pltpu.make_async_remote_copy(
                    src_ref=source(p),
                    dst_ref=target,
                    send_sem=send_sem.at[which],
                    recv_sem=recv_sem.at[which, k],
                    device_id=p,
                    device_id_type=LOGICAL,
                ).start()

            return carry

        lax.fori_loop(0, burst, one, 0)

    def arrived(k, ref, unit, which):
        first = pl.ds(unit, (burst - 1) * unit) if unit else pl.ds(1, burst - 1)
        rest = pl.ds(0, burst * unit) if unit else pl.ds(0, burst)
        if isinstance(k, int) and k == 0:
            part = ref.at[first]
        else:
            part = ref.at[rest]
        pltpu.make_async_copy(part, part, recv_sem.at[which, k]).wait()

    def sent(part, which):
        pltpu.make_async_copy(part, part, send_sem.at[which]).wait()

    def source_at(k):
        return lax.rem(me // burst - k + bursts, bursts)

    def wide_at(k):
        return pl.ds(pl.multiple_of(burst_at(k) * WIDE, WIDE), WIDE)

    def produce(fill, source, target, which):
        fill(0)

        def middle(k, carry):
            fill(k)
            ship(k - 1, source, target, which)
            return carry

        lax.fori_loop(1, bursts, middle, 0)

    def halves(rows):
        wide = rows.reshape(burst, half, width)
        return jnp.concatenate([wide[:, :, :LANES], wide[:, :, LANES:]], axis=1)

    def whole(blocks):
        wide = blocks.astype(jnp.float32)
        return jnp.concatenate([wide[:, :half], wide[:, half : 2 * half]], axis=2)

    def spread(table, depth):
        shape = (table.shape[0], depth, table.shape[1])
        keep = lax.broadcasted_iota(jnp.int32, shape, 1) == lax.broadcasted_iota(
            jnp.int32, shape, 2
        )
        wide = jnp.broadcast_to(table[:, None, :], shape)
        one = jnp.sum(jnp.where(keep, wide, 0.0), axis=2, keepdims=True)
        return one.reshape(shape[0] * depth, 1)

    def as_row(col):
        return jnp.transpose(jnp.broadcast_to(col, (col.shape[0], LANES)))[:8]

    hcol_s[...] = spread(jnp.transpose(halo_ref[...].astype(jnp.float32)), half)
    asks = ask_ref[...]
    ask_table = jnp.transpose(
        jnp.concatenate(
            [
                jnp.right_shift(asks, 6).astype(jnp.float32),
                jnp.bitwise_and(asks, 63).astype(jnp.float32),
                jnp.zeros((LANES - 2 * block, peers), jnp.float32),
            ],
            axis=0,
        )
    )
    wcol_s[0:peers, :] = ask_table

    def outgoing(t, carry):
        hot = pick(hcol_s[tile_of(t), :].astype(jnp.int32), 0, node_rows, 1)
        part = pl.ds(pl.multiple_of(t * burst, burst), burst)
        asked = jnp.broadcast_to(wcol_s[part, :][:, None, :], (burst, 8, LANES))
        first_s[part] = jnp.concatenate(
            [halves(dot32(hot, feat_ref[...])), asked], axis=1
        ).astype(jnp.bfloat16)
        return carry

    lax.fori_loop(0, bursts, outgoing, 0)

    def local_sums(i, carry):
        load_adj(i).wait()
        at = tile_of(i)
        gfeat_s[at, :] = dot32(adj_s[at, :node_rows], feat_ref[...])
        return carry

    lax.fori_loop(0, tiles, local_sums, 0)
    pl.semaphore_wait(barrier, peers - 1)
    first_of = lambda p: first_s.at[p]
    for k in range(bursts):
        ship(k, first_of, frecv_s.at[me], 0)
    frecv_s[me] = first_s[me]
    pair_s[...] = jnp.concatenate(
        [
            ends_ref[...].astype(jnp.float32),
            weight_ref[...],
            label_ref[...].astype(jnp.float32),
            jnp.zeros((4, pairs), jnp.float32),
        ],
        axis=0,
    )

    def columns(i, carry):
        at = pl.ds(pl.multiple_of(i * WIDE, WIDE), WIDE)
        cols_s[at, :] = jnp.transpose(pair_s[:, at])
        return carry

    lax.fori_loop(0, pairs // WIDE, columns, 0)
    hrow_s[...] = as_row(hcol_s[...])
    for k in range(bursts):
        arrived(k, frecv_s, 0, 0)
    arr_s[...] = whole(frecv_s[...]).reshape(peers * half, width).astype(jnp.bfloat16)
    codes = jnp.max(frecv_s[...].astype(jnp.float32)[:, 2 * half :], axis=1)
    wcol_s[0:peers, :] = codes * 64.0 + pltpu.roll(codes, LANES - block, 1)

    def encode(i, carry):
        at = tile_of(i)
        sums = gfeat_s[at, :] + dot32(adj_s[at, node_rows:], arr_s[...])
        mean = (sums / deg_ref[at, :1]).astype(jnp.bfloat16)
        agg_s[at, :] = mean
        emb_s[at, :] = (dot32(feat_ref[at, :], ws_ref[...]) + dot32(mean, wn_ref[...])).astype(
            jnp.bfloat16
        )
        return carry

    lax.fori_loop(0, tiles, encode, 0)

    def serve(k):
        at = wide_at(k)
        part = pl.ds(pl.multiple_of(burst_at(k) * burst, burst), burst)
        asked = spread(wcol_s[part, :], block)
        wrow_s[:, at] = as_row(asked)
        hot = pick(asked.astype(jnp.int32), 0, node_rows, 1)
        served_s[at, :] = dot32(hot, emb_s[...]).astype(jnp.bfloat16)

    served_of = lambda p: served_s.at[rows_of(p), :]
    produce(serve, served_of, recv_s.at[rows_of(me), :], 1)
    recv_s[rows_of(me), :] = served_s[rows_of(me), :]
    small_s[...] = jnp.zeros(small_s.shape, jnp.float32)
    ship(bursts - 1, served_of, recv_s.at[rows_of(me), :], 1)

    for k in range(bursts):
        arrived(k, recv_s, block, 1)
        b = source_at(k)
        here = pl.ds(pl.multiple_of(b * WIDE, WIDE), WIDE)

        def gather(i, carry):
            at = pl.ds(pl.multiple_of(i * TALL, TALL), TALL)
            for side, rows in ((0, left_s), (1, right_s)):
                ends = cols_s[at, side : side + 1].astype(jnp.int32)
                found = dot32(pick(ends, b * WIDE, WIDE, 1), recv_s[here, :]).astype(
                    jnp.bfloat16
                )
                rows[at, :] = found if k == 0 else rows[at, :] + found
            return carry

        lax.fori_loop(0, pairs // TALL, gather, 0)

    def forward(i, carry):
        at = pl.ds(pl.multiple_of(i * WIDE, WIDE), WIDE)
        cols = cols_s[at, :]
        left = left_s[at, :]
        right = right_s[at, :]
        pre = dot32(left, wh_ref[:width, :]) + dot32(right, wh_ref[width:, :]) + bias_ref[...]
        hidden = jnp.maximum(pre, 0.0)
        logit = jnp.sum(hidden * wo_ref[...], axis=1, keepdims=True)
        logit_ref[:, at] = jnp.transpose(jnp.broadcast_to(logit, (WIDE, LANES)))[:1]
        slope = cols[:, 2:3] * (jax.nn.sigmoid(logit) - cols[:, 3:4])
        delta = jnp.where(pre > 0, slope * wo_ref[...], 0.0)
        small_s[0:1, :] += jnp.sum(delta, axis=0, keepdims=True)
        small_s[1:2, :] += jnp.sum(slope * hidden, axis=0, keepdims=True)
        delta_b = delta.astype(jnp.bfloat16)
        delta_s[at, :] = delta_b
        pgl_s[at, :] = dot_nt(delta_b, wh_ref[:width, :]).astype(jnp.bfloat16)
        pgr_s[at, :] = dot_nt(delta_b, wh_ref[width:, :]).astype(jnp.bfloat16)
        return carry

    lax.fori_loop(0, pairs // WIDE, forward, 0)
    ends_row = ends_ref[...]

    def collect(k):
        first = burst_at(k) * WIDE
        total = dot32(pick(ends_row[0:1, :], first, WIDE, 0), pgl_s[...]) + dot32(
            pick(ends_row[1:2, :], first, WIDE, 0), pgr_s[...]
        )
        rgrad_s[wide_at(k), :] = total.astype(jnp.bfloat16)

    rgrad_of = lambda p: rgrad_s.at[rows_of(p), :]
    produce(collect, rgrad_of, back_s.at[rows_of(me), :], 2)
    back_s[rows_of(me), :] = rgrad_s[rows_of(me), :]
    ship(bursts - 1, rgrad_of, back_s.at[rows_of(me), :], 2)
    gw_s[2 * width : 3 * width, :] = dot_tn(left_s[...], delta_s[...])
    gw_s[3 * width :, :] = dot_tn(right_s[...], delta_s[...])
    for k in range(bursts):
        arrived(k, back_s, block, 2)
        b = source_at(k)
        here = pl.ds(pl.multiple_of(b * WIDE, WIDE), WIDE)

        def put(i, carry):
            at = pl.ds(pl.multiple_of(i * TALL, TALL), TALL)
            found = dot32(pick(wrow_s[0:1, here].astype(jnp.int32), i * TALL, TALL, 0), back_s[here, :])
            gfeat_s[at, :] = found if k == 0 else gfeat_s[at, :] + found
            return carry

        lax.fori_loop(0, node_rows // TALL, put, 0)
    gradb_s[...] = gfeat_s[...].astype(jnp.bfloat16)
    gw_s[:width, :] = dot_tn(feat_ref[...], gradb_s[...])
    gw_s[width : 2 * width, :] = dot_tn(agg_s[...], gradb_s[...])
    def weight_terms(k):
        t = burst_at(k)
        part_s[pl.ds(t * burst, burst)] = halves(gw_s[tile_of(t), :]).astype(jnp.bfloat16)

    part_of = lambda p: part_s.at[p]
    produce(weight_terms, part_of, precv_s.at[me], 3)
    precv_s[me] = part_s[me]
    degree = jnp.concatenate([degt_ref[0, 0:1, :], degt_ref[1, 0:1, :]], axis=1)
    gt_s[...] = (dot_nt(wn_ref[...], gradb_s[...]) / degree).astype(jnp.bfloat16)
    ship(bursts - 1, part_of, precv_s.at[me], 3)

    def table_grad(first):
        cols = pl.ds(pl.multiple_of(first, TILE), TILE)
        return jnp.transpose(dot32(gt_s[...], adj_s[:, cols]))

    def return_halo(k):
        t = burst_at(k)
        halo_s[pl.ds(t * burst, burst)] = halves(
            table_grad(node_rows + t * TILE)
        ).astype(jnp.bfloat16)

    halo_of = lambda p: halo_s.at[p]
    produce(return_halo, halo_of, hrecv_s.at[me], 4)
    hrecv_s[me] = halo_s[me]

    def direct(i, carry):
        at = tile_of(i)
        gfeat_s[at, :] = dot_nt(gradb_s[at, :], ws_ref[...]) + table_grad(i * TILE)
        return carry

    direct(0, 0)
    ship(bursts - 1, halo_of, hrecv_s.at[me], 4)
    for k in range(bursts):
        arrived(k, precv_s, 0, 3)
    own = jnp.sum(precv_s[...].astype(jnp.float32), axis=0)
    small = small_s[...]
    small_hi = small.astype(jnp.bfloat16).astype(jnp.float32)
    small_lo = small - small_hi
    lines = [
        part[r : r + 1, c : c + LANES]
        for part in (small_hi, small_lo)
        for r in range(2)
        for c in (0, LANES)
    ]
    share_s[...] = jnp.concatenate([own] + lines, axis=0).astype(jnp.bfloat16)
    direct(1, 0)

    core = lax.rem(me // grp, 2)
    partner = me + (1 - 2 * core) * grp
    groups = peers // (2 * grp)

    def share(i, carry):
        q = lax.rem((me // (2 * grp)) * grp + lax.rem(me, grp) + i * 27, peers // 2)
        p = (q // grp) * (2 * grp) + core * grp + lax.rem(q, grp)
        pltpu.make_async_remote_copy(
            src_ref=share_s,
            dst_ref=srecv_s.at[me],
            send_sem=send_sem.at[5],
            recv_sem=recv_sem.at[5, 0],
            device_id=p,
            device_id_type=LOGICAL,
        ).start()
        return carry

    lax.fori_loop(1, peers // 2, share, 0)
    srecv_s[me] = share_s[...]
    lax.fori_loop(2, tiles, direct, 0)
    for k in range(bursts):
        arrived(k, hrecv_s, 0, 4)
    hrows_s[...] = whole(hrecv_s[...]).reshape(peers * half, width).astype(jnp.bfloat16)

    def place(i, carry):
        at = pl.ds(pl.multiple_of(i * TALL, TALL), TALL)
        hot = pick(hrow_s[0:1, :].astype(jnp.int32), i * TALL, TALL, 0)
        gfeat_s[at, :] += dot32(hot, hrows_s[...])
        return carry

    lax.fori_loop(0, node_rows // TALL, place, 0)
    result = pltpu.make_async_copy(gfeat_s, gfeat_ref, adj_sem.at[0])
    result.start()
    others = srecv_s.at[pl.ds(1, peers // 2 - 1)]
    pltpu.make_async_copy(others, others, recv_sem.at[5, 0]).wait()

    def across(i, carry):
        part = srecv_s.at[pl.ds(i * (2 * grp) + core * grp, grp)]
        pltpu.make_async_remote_copy(
            src_ref=part,
            dst_ref=part,
            send_sem=send_sem.at[6],
            recv_sem=recv_sem.at[5, 1],
            device_id=partner,
            device_id_type=LOGICAL,
        ).start()
        return carry

    lax.fori_loop(0, groups, across, 0)
    sent(others, 5)
    sent(srecv_s.at[pl.ds(0, peers // 2)], 6)
    for which, ref in ((1, served_s), (2, rgrad_s)):
        sent(ref.at[pl.ds(block, recv_rows - block), :], which)
    for which, ref in ((0, frecv_s), (3, part_s), (4, halo_s)):
        sent(ref.at[pl.ds(1, peers - 1)], which)
    mates = srecv_s.at[pl.ds(0, peers // 2)]
    pltpu.make_async_copy(mates, mates, recv_sem.at[5, 1]).wait()
    everyone = whole(srecv_s[...])
    quarter = peers // 4
    gself_ref[...] = everyone[:quarter].reshape(width, width)
    gneigh_ref[...] = everyone[quarter : 2 * quarter].reshape(width, width)
    ghid_ref[...] = everyone[2 * quarter :].reshape(2 * width, width)
    total = jnp.sum(srecv_s[...].astype(jnp.float32)[:, block:], axis=0)
    total = total[:4] + total[4:]
    gbias_ref[...] = jnp.concatenate([total[0:1], total[1:2]], axis=1)
    gout_ref[...] = jnp.concatenate([total[2:3], total[3:4]], axis=1)
    result.wait()


def finish_kernel(count, *refs):
    taken, given, held = refs[:count], refs[count : 2 * count], refs[2 * count : 3 * count]
    in_sem, out_sem = refs[3 * count :]
    parts = []
    for a, h, b in zip(taken, held, given):
        rows = a.shape[0]
        step = TILE if rows > TILE else rows
        parts += [(a, h, b, pl.ds(r, step)) for r in range(0, rows, step)]
    moves = [
        (
            pltpu.make_async_copy(a.at[at, :], h.at[at, :], in_sem.at[n]),
            pltpu.make_async_copy(h.at[at, :], b.at[at, :], out_sem.at[n]),
        )
        for n, (a, h, b, at) in enumerate(parts)
    ]
    for fetch, _ in moves:
        fetch.start()
    for fetch, put in moves:
        fetch.wait()
        put.start()
    for _, put in moves:
        put.wait()


def finish(arrays):
    count = len(arrays)
    moves = sum(max(a.shape[0] // TILE, 1) for a in arrays)
    return pl.pallas_call(
        lambda *refs: finish_kernel(count, *refs),
        out_shape=tuple(jax.ShapeDtypeStruct(a.shape, a.dtype) for a in arrays),
        in_specs=[ANY] * count,
        out_specs=(ANY,) * count,
        scratch_shapes=[pltpu.VMEM(a.shape, a.dtype) for a in arrays]
        + [pltpu.SemaphoreType.DMA((moves,)), pltpu.SemaphoreType.DMA((moves,))],
        compiler_params=params(60),
        name="finish",
    )(*arrays)


def train_step(
    adj, features, deg, degt, ask, halo, ends, pair_weight, labels, w_self, w_neigh, w_hidden,
    bias, w_out
):
    node_rows, width = features.shape
    table_rows = adj.shape[1]
    block, peers = ask.shape
    half = halo.shape[0]
    recv_rows = peers * block
    pairs = ends.shape[1]
    lines = 2 * half + 8
    bf16 = lambda *shape: pltpu.VMEM(shape, jnp.bfloat16)
    return pl.pallas_call(
        step_kernel,
        out_shape=(
            jax.ShapeDtypeStruct((1, pairs), jnp.float32),
            jax.ShapeDtypeStruct((node_rows, width), jnp.float32),
            jax.ShapeDtypeStruct((width, width), jnp.float32),
            jax.ShapeDtypeStruct((width, width), jnp.float32),
            jax.ShapeDtypeStruct((2 * width, width), jnp.float32),
            jax.ShapeDtypeStruct((1, width), jnp.float32),
            jax.ShapeDtypeStruct((1, width), jnp.float32),
        ),
        in_specs=[ANY] + [VMEM] * 13,
        out_specs=(VMEM, ANY) + (VMEM,) * 5,
        scratch_shapes=[
            bf16(node_rows, table_rows),
            pltpu.VMEM((node_rows, width), jnp.float32),
            pltpu.VMEM((8, pairs), jnp.float32),
            pltpu.VMEM((peers * half, 1), jnp.float32),
            pltpu.VMEM((8, peers * half), jnp.float32),
            pltpu.VMEM((peers, LANES), jnp.float32),
            pltpu.VMEM((8, recv_rows), jnp.float32),
            bf16(peers, lines, LANES),
            bf16(peers, lines, LANES),
            bf16(peers * half, width),
            bf16(node_rows, width),
            bf16(node_rows, width),
            bf16(recv_rows, width),
            bf16(recv_rows, width),
            bf16(pairs, width),
            bf16(pairs, width),
            bf16(pairs, width),
            bf16(pairs, width),
            bf16(pairs, width),
            bf16(recv_rows, width),
            bf16(recv_rows, width),
            bf16(node_rows, width),
            bf16(width, node_rows),
            pltpu.VMEM((4 * width, width), jnp.float32),
            pltpu.VMEM((8, width), jnp.float32),
            pltpu.VMEM((pairs, 8), jnp.float32),
            bf16(peers, block, LANES),
            bf16(peers, block, LANES),
            bf16(peers, block, LANES),
            bf16(peers, block, LANES),
            bf16(peers * half, width),
            bf16(lines, LANES),
            bf16(peers, lines, LANES),
            pltpu.SemaphoreType.DMA((node_rows // TILE,)),
            pltpu.SemaphoreType.DMA((7,)),
            pltpu.SemaphoreType.DMA((6, recv_rows // WIDE)),
        ],
        compiler_params=pltpu.CompilerParams(
            vmem_limit_bytes=62 * 2**20, collective_id=0, has_side_effects=True
        ),
        cost_estimate=cost(30_000_000_000, 24 * 2**20),
        name="train_step",
    )(
        adj, features, deg, degt, ask, halo, ends, pair_weight, labels, w_self, w_neigh,
        w_hidden, bias, w_out,
    )


def per_device(
    features,
    edge_src,
    edge_dst,
    edge_count,
    halo_index,
    request_rows,
    pair_ends,
    labels,
    pair_weight,
    w_self,
    w_neigh,
    w_hidden,
    b_hidden,
    w_out,
):
    node_rows = features.shape[0]
    halo = halo_index[0].T
    adj, deg, degt = adjacency(edge_src, edge_dst, edge_count, node_rows, node_rows + halo.size)
    logits, grad_features, grad_self, grad_neigh, grad_hidden, grad_bias, grad_out = train_step(
        adj, features, deg, degt, request_rows[0].T, halo, pair_ends.T, pair_weight[None],
        labels[None], w_self, w_neigh, w_hidden, b_hidden[None], w_out[None]
    )
    grad_features, grad_self, grad_neigh, grad_hidden, grad_bias, grad_out, logits = finish(
        (grad_features, grad_self, grad_neigh, grad_hidden, grad_bias, grad_out, logits)
    )
    return (
        logits[0],
        grad_features,
        grad_self,
        grad_neigh,
        grad_hidden,
        grad_bias[0],
        grad_out[0],
    )


def solution(mesh):
    split = P(AXES)
    in_specs = (
        P(AXES, None),
        split,
        split,
        split,
        P(AXES, None, None),
        P(AXES, None, None),
        P(AXES, None),
        split,
        split,
        P(),
        P(),
        P(),
        P(),
        P(),
    )
    out_specs = (split, P(AXES, None), P(), P(), P(), P(), P())
    return jax.shard_map(
        per_device, mesh=mesh, in_specs=in_specs, out_specs=out_specs, check_vma=False
    )
```

```python
import jax
import jax.numpy as jnp
from jax import lax
from jax.experimental import pallas as pl
from jax.experimental.pallas import tpu as pltpu
from jax.sharding import PartitionSpec as P

AXES = ("dom", "grp")
LANES = 128
GROUP = 8
STRIDE = LANES // GROUP
TILE = 256
WIDE = 512
TALL = 1024
LOGICAL = pl.DeviceIdType.LOGICAL
CLASH = 1 << 20
VMEM = pl.BlockSpec(memory_space=pltpu.VMEM)
SMEM = pl.BlockSpec(memory_space=pltpu.SMEM)
ANY = pl.BlockSpec(memory_space=pl.ANY)


def dot32(a, b):
    return jnp.dot(a, b, preferred_element_type=jnp.float32)


def dot_nt(a, b):
    return lax.dot_general(a, b, (((1,), (1,)), ((), ())), preferred_element_type=jnp.float32)


def dot_tn(a, b):
    return lax.dot_general(a, b, (((0,), (0,)), ((), ())), preferred_element_type=jnp.float32)


def params(mib):
    return pltpu.CompilerParams(vmem_limit_bytes=mib * 2**20)


def cost(flops, size):
    return pl.CostEstimate(flops=flops, bytes_accessed=size, transcendentals=0)


def tile_of(i):
    return pl.ds(pl.multiple_of(i * TILE, TILE), TILE)


def pick(index, first, count, axis):
    shape = (index.shape[0], count) if axis == 1 else (count, index.shape[1])
    ids = lax.broadcasted_iota(jnp.int32, shape, axis) + first
    return jnp.where(index == ids, 1.0, 0.0).astype(jnp.bfloat16)


def edge_words(half, panels, count, src, dst):
    shape = src.shape
    lane = lax.broadcasted_iota(jnp.int32, shape, 1)
    live = lax.broadcasted_iota(jnp.int32, shape, 0) * LANES + lane < count
    upper = jnp.where(dst >= half, 1, 0)
    row = jnp.right_shift(src, 7) * half + dst - upper * half
    row = jnp.where(live, row, half * panels + lane // STRIDE)
    unit = jnp.where(live, jnp.bitwise_and(src, LANES - 1) + upper * LANES, 2 * LANES)
    clash = jnp.zeros(shape, jnp.int32)
    for k in range(1, GROUP // 2 + 1):
        clash = clash + jnp.where(row == pltpu.roll(row, k * STRIDE, 1), 1, 0)
    any_clash = jnp.max(clash.astype(jnp.float32), axis=1, keepdims=True) > 0.0
    return row + jnp.where(any_clash & (lane == 0), CLASH, 0), unit


def counts_kernel(
    half, panels, count_ref, src_ref, dst_ref, adj_ref, degt_ref, even, odd, unit_a, unit_b,
    row_v, row_ref, unit_ref, row_sem
):
    step = pl.program_id(0)
    chunks = unit_ref.shape[0]

    @pl.when(step == 0)
    def _():
        row_v[...], unit_ref[...] = edge_words(
            half, panels, count_ref[0], src_ref[...], dst_ref[...]
        )
        words = pltpu.make_async_copy(row_v, row_ref, row_sem)
        words.start()
        lane = lax.broadcasted_iota(jnp.int32, (LANES, LANES), 1)

        def clear(i, carry):
            even[tile_of(i), :] = jnp.zeros((TILE, LANES), jnp.int32)
            odd[tile_of(i), :] = jnp.zeros((TILE, LANES), jnp.int32)
            return carry

        lax.fori_loop(0, half * panels // TILE, clear, 0)
        words.wait()

        def units_of(c):
            c = jnp.minimum(c, chunks - 1)
            wide = jnp.transpose(jnp.broadcast_to(unit_ref[pl.ds(c, 1), :], (LANES, LANES)))
            return jnp.where(wide == lane, 1, jnp.where(wide == lane + LANES, 65536, 0))

        unit_a[...] = units_of(0)

        def chunk(c, units, later):
            places = row_ref.at[c]
            head = places[0]

            def load(s):
                words = odd if s % 2 else even
                at = [places[s + STRIDE * t] for t in range(GROUP)]
                new = [
                    words[pl.ds(a, 1), :] + units[pl.ds(s + STRIDE * t, 1), :]
                    for t, a in enumerate(at)
                ]
                return words, at, new

            def store(words, at, new):
                for a, n in zip(at, new):
                    words[pl.ds(a, 1), :] = n

            @pl.when(head < CLASH)
            def _():
                coming = units_of(c + 1)
                held = load(0)
                for s in range(1, STRIDE):
                    following = load(s)
                    store(*held)
                    held = following
                store(*held)
                later[...] = coming

            @pl.when(head >= CLASH)
            def _():
                later[...] = units_of(c + 1)
                for j in range(LANES):
                    words = odd if j % 2 else even
                    a = places[j]
                    if j == 0:
                        a = a - CLASH
                    words[pl.ds(a, 1), :] = words[pl.ds(a, 1), :] + units[pl.ds(j, 1), :]

        def two(i, carry):
            chunk(2 * i, unit_a, unit_b)
            chunk(2 * i + 1, unit_b, unit_a)
            return carry

        lax.fori_loop(0, chunks // 2, two, 0)

    first = step * TILE
    total = jnp.zeros((TILE, LANES), jnp.int32)
    for p in range(panels):
        part = pl.ds(pl.multiple_of(p * half + first, TILE), TILE)
        word = even[part, :] + odd[part, :]
        total = total + word
        cols = slice(p * LANES, (p + 1) * LANES)
        for h, count in enumerate((jnp.bitwise_and(word, 0xFFFF), jnp.right_shift(word, 16))):
            adj_ref[h, :, cols] = count.astype(jnp.float32).astype(jnp.bfloat16)
    for h, count in enumerate((jnp.bitwise_and(total, 0xFFFF), jnp.right_shift(total, 16))):
        degree = jnp.sum(count.astype(jnp.float32), axis=1, keepdims=True)
        wide = jnp.broadcast_to(jnp.maximum(degree, 1.0), (TILE, LANES))
        degt_ref[h] = jnp.transpose(wide)[:8]


def adjacency(edge_src, edge_dst, edge_count, node_rows, table_rows):
    half = node_rows // 2
    panels = table_rows // LANES
    chunks = edge_src.shape[0] // LANES
    grid_shape = (chunks, LANES)
    adj, degt = pl.pallas_call(
        lambda *refs: counts_kernel(half, panels, *refs),
        grid=(half // TILE,),
        out_shape=(
            jax.ShapeDtypeStruct((2, half, table_rows), jnp.bfloat16),
            jax.ShapeDtypeStruct((2, 8, half), jnp.float32),
        ),
        in_specs=[SMEM] + [pl.BlockSpec(grid_shape, lambda i: (0, 0))] * 2,
        out_specs=(
            pl.BlockSpec((2, TILE, table_rows), lambda i: (0, i, 0)),
            pl.BlockSpec((2, 8, TILE), lambda i: (0, 0, i)),
        ),
        scratch_shapes=[
            pltpu.VMEM((half * panels + GROUP, LANES), jnp.int32),
            pltpu.VMEM((half * panels + GROUP, LANES), jnp.int32),
            pltpu.VMEM((LANES, LANES), jnp.int32),
            pltpu.VMEM((LANES, LANES), jnp.int32),
            pltpu.VMEM(grid_shape, jnp.int32),
            pltpu.SMEM(grid_shape, jnp.int32),
            pltpu.VMEM(grid_shape, jnp.int32),
            pltpu.SemaphoreType.DMA,
        ],
        compiler_params=params(60),
        cost_estimate=cost(60_000_000, 16 * 2**20),
        name="counts",
    )(edge_count, edge_src.reshape(grid_shape), edge_dst.reshape(grid_shape))
    return adj.reshape(node_rows, table_rows), degt


def step_kernel(
    adj_ref,
    feat_ref,
    degt_ref,
    ask_ref,
    halo_ref,
    ends_ref,
    weight_ref,
    label_ref,
    ws_ref,
    wn_ref,
    wh_ref,
    bias_ref,
    wo_ref,
    logit_ref,
    gfeat_ref,
    gself_ref,
    gneigh_ref,
    ghid_ref,
    gbias_ref,
    gout_ref,
    adj_s,
    gfeat_s,
    pair_s,
    deg_s,
    hcol_s,
    hrow_s,
    wcol_s,
    wrow_s,
    first_s,
    frecv_s,
    arr_s,
    emb_s,
    agg_s,
    served_s,
    recv_s,
    left_s,
    right_s,
    delta_s,
    pgl_s,
    pgr_s,
    rgrad_s,
    back_s,
    gradb_s,
    gt_s,
    gw_s,
    small_s,
    cols_s,
    part_s,
    precv_s,
    hpart_s,
    hprecv_s,
    halo_s,
    hrecv_s,
    hrows_s,
    share_s,
    srecv_s,
    adj_sem,
    send_sem,
    recv_sem,
):
    node_rows, width = feat_ref.shape
    block, peers = ask_ref.shape
    half = halo_ref.shape[0]
    recv_rows = peers * block
    pairs = ends_ref.shape[1]
    grp = lax.axis_size("grp")
    me = lax.axis_index("dom") * grp + lax.axis_index("grp")
    burst = WIDE // block
    bursts = peers // burst
    tiles = node_rows // TILE
    barrier = pltpu.get_barrier_semaphore()

    def load_adj(i):
        return pltpu.make_async_copy(
            adj_ref.at[tile_of(i), :], adj_s.at[tile_of(i), :], adj_sem.at[i]
        )

    def fetch(i, carry):
        load_adj(i).start()
        return carry

    lax.fori_loop(0, tiles, fetch, 0)

    def greet(i, carry):
        for u in range(7):
            pl.semaphore_signal(
                barrier,
                inc=1,
                device_id=jnp.bitwise_and(me + (i * 7 + u + 1), peers - 1),
                device_id_type=LOGICAL,
            )
        return carry

    pl.semaphore_signal(
        barrier,
        inc=1,
        device_id=jnp.bitwise_and(me + (peers - 1), peers - 1),
        device_id_type=LOGICAL,
    )
    lax.fori_loop(0, (peers - 2) // 7, greet, 0)

    def rows_of(p):
        return pl.ds(pl.multiple_of(p * block, block), block)

    def burst_at(k):
        return lax.rem(me // burst + k, bursts)

    def ship(k, source, target, which):
        low = jnp.bitwise_and(me, burst - 1)
        first = burst_at(k) * burst

        def one(i):
            p = first + jnp.bitwise_and(low + i, burst - 1)
            pltpu.make_async_remote_copy(
                src_ref=source(p),
                dst_ref=target,
                send_sem=send_sem.at[which],
                recv_sem=recv_sem.at[which, k],
                device_id=p,
                device_id_type=LOGICAL,
            ).start()

        @pl.when(k > 0)
        def _():
            one(0)

        for i in range(1, burst):
            one(i)

    def arrived(k, ref, unit, which):
        first = pl.ds(unit, (burst - 1) * unit) if unit else pl.ds(1, burst - 1)
        rest = pl.ds(0, burst * unit) if unit else pl.ds(0, burst)
        if isinstance(k, int) and k == 0:
            part = ref.at[first]
        else:
            part = ref.at[rest]
        pltpu.make_async_copy(part, part, recv_sem.at[which, k]).wait()

    def sent(part, which):
        pltpu.make_async_copy(part, part, send_sem.at[which]).wait()

    def source_at(k):
        return lax.rem(me // burst - k + bursts, bursts)

    def wide_at(k):
        return pl.ds(pl.multiple_of(burst_at(k) * WIDE, WIDE), WIDE)

    def produce(fill, source, target, which):
        fill(0)

        def middle(k, carry):
            fill(k)
            ship(k - 1, source, target, which)
            return carry

        lax.fori_loop(1, bursts, middle, 0)

    def halves(rows):
        wide = rows.reshape(burst, half, width)
        return jnp.concatenate([wide[:, :, :LANES], wide[:, :, LANES:]], axis=1)

    def whole(blocks):
        wide = blocks.astype(jnp.float32)
        return jnp.concatenate([wide[:, :half], wide[:, half : 2 * half]], axis=2)

    def spread(table, depth):
        shape = (table.shape[0], depth, table.shape[1])
        keep = lax.broadcasted_iota(jnp.int32, shape, 1) == lax.broadcasted_iota(
            jnp.int32, shape, 2
        )
        wide = jnp.broadcast_to(table[:, None, :], shape)
        one = jnp.sum(jnp.where(keep, wide, 0.0), axis=2, keepdims=True)
        return one.reshape(shape[0] * depth, 1)

    def as_row(col):
        return jnp.transpose(jnp.broadcast_to(col, (col.shape[0], LANES)))[:8]

    deg_s[...] = jnp.concatenate([degt_ref[0], degt_ref[1]], axis=1)
    hcol_s[...] = spread(jnp.transpose(halo_ref[...].astype(jnp.float32)), half)
    asks = ask_ref[...]
    ask_table = jnp.transpose(
        jnp.concatenate(
            [
                jnp.right_shift(asks, 6).astype(jnp.float32),
                jnp.bitwise_and(asks, 63).astype(jnp.float32),
                jnp.zeros((LANES - 2 * block, peers), jnp.float32),
            ],
            axis=0,
        )
    )
    wcol_s[0:peers, :] = ask_table

    def outgoing(t, carry):
        hot = pick(hcol_s[tile_of(t), :].astype(jnp.int32), 0, node_rows, 1)
        part = pl.ds(pl.multiple_of(t * burst, burst), burst)
        asked = jnp.broadcast_to(wcol_s[part, :][:, None, :], (burst, 8, LANES))
        first_s[part] = jnp.concatenate(
            [halves(dot32(hot, feat_ref[...])), asked], axis=1
        ).astype(jnp.bfloat16)
        return carry

    lax.fori_loop(0, bursts, outgoing, 0)

    def local_sums(i, carry):
        load_adj(i).wait()
        at = tile_of(i)
        gfeat_s[at, :] = dot32(adj_s[at, :node_rows], feat_ref[...])
        return carry

    lax.fori_loop(0, tiles, local_sums, 0)
    pl.semaphore_wait(barrier, peers - 1)
    first_of = lambda p: first_s.at[p]
    for k in range(bursts):
        ship(k, first_of, frecv_s.at[me], 0)
    frecv_s[me] = first_s[me]
    pair_s[...] = jnp.concatenate(
        [
            ends_ref[...].astype(jnp.float32),
            weight_ref[...],
            label_ref[...].astype(jnp.float32),
            jnp.zeros((4, pairs), jnp.float32),
        ],
        axis=0,
    )

    def columns(i, carry):
        at = pl.ds(pl.multiple_of(i * WIDE, WIDE), WIDE)
        cols_s[at, :] = jnp.transpose(pair_s[:, at])
        return carry

    lax.fori_loop(0, pairs // WIDE, columns, 0)
    hrow_s[...] = as_row(hcol_s[...])
    for k in range(bursts):
        arrived(k, frecv_s, 0, 0)
    arr_s[...] = whole(frecv_s[...]).reshape(peers * half, width).astype(jnp.bfloat16)
    codes = jnp.max(frecv_s[...].astype(jnp.float32)[:, 2 * half :], axis=1)
    wcol_s[0:peers, :] = codes * 64.0 + pltpu.roll(codes, LANES - block, 1)

    def encode(i, carry):
        at = tile_of(i)
        sums = gfeat_s[at, :] + dot32(adj_s[at, node_rows:], arr_s[...])
        degree = jnp.transpose(deg_s[:, at])[:, :1]
        mean = (sums / degree).astype(jnp.bfloat16)
        agg_s[at, :] = mean
        emb_s[at, :] = (dot32(feat_ref[at, :], ws_ref[...]) + dot32(mean, wn_ref[...])).astype(
            jnp.bfloat16
        )
        return carry

    lax.fori_loop(0, tiles, encode, 0)

    def serve(k):
        at = wide_at(k)
        part = pl.ds(pl.multiple_of(burst_at(k) * burst, burst), burst)
        asked = spread(wcol_s[part, :], block)
        wrow_s[:, at] = as_row(asked)
        hot = pick(asked.astype(jnp.int32), 0, node_rows, 1)
        served_s[at, :] = dot32(hot, emb_s[...]).astype(jnp.bfloat16)

    served_of = lambda p: served_s.at[rows_of(p), :]
    produce(serve, served_of, recv_s.at[rows_of(me), :], 1)
    recv_s[rows_of(me), :] = served_s[rows_of(me), :]
    small_s[...] = jnp.zeros(small_s.shape, jnp.float32)
    ship(bursts - 1, served_of, recv_s.at[rows_of(me), :], 1)

    for k in range(bursts):
        arrived(k, recv_s, block, 1)
        b = source_at(k)
        here = pl.ds(pl.multiple_of(b * WIDE, WIDE), WIDE)

        def gather(i, carry):
            at = pl.ds(pl.multiple_of(i * TALL, TALL), TALL)
            for side, rows in ((0, left_s), (1, right_s)):
                ends = cols_s[at, side : side + 1].astype(jnp.int32)
                found = dot32(pick(ends, b * WIDE, WIDE, 1), recv_s[here, :]).astype(
                    jnp.bfloat16
                )
                rows[at, :] = found if k == 0 else rows[at, :] + found
            return carry

        lax.fori_loop(0, pairs // TALL, gather, 0)

    def forward(i, carry):
        at = pl.ds(pl.multiple_of(i * WIDE, WIDE), WIDE)
        cols = cols_s[at, :]
        left = left_s[at, :]
        right = right_s[at, :]
        pre = dot32(left, wh_ref[:width, :]) + dot32(right, wh_ref[width:, :]) + bias_ref[...]
        hidden = jnp.maximum(pre, 0.0)
        logit = jnp.sum(hidden * wo_ref[...], axis=1, keepdims=True)
        logit_ref[:, at] = jnp.transpose(jnp.broadcast_to(logit, (WIDE, LANES)))[:1]
        slope = cols[:, 2:3] * (jax.nn.sigmoid(logit) - cols[:, 3:4])
        delta = jnp.where(pre > 0, slope * wo_ref[...], 0.0)
        small_s[0:1, :] += jnp.sum(delta, axis=0, keepdims=True)
        small_s[1:2, :] += jnp.sum(slope * hidden, axis=0, keepdims=True)
        delta_b = delta.astype(jnp.bfloat16)
        delta_s[at, :] = delta_b
        pgl_s[at, :] = dot_nt(delta_b, wh_ref[:width, :]).astype(jnp.bfloat16)
        pgr_s[at, :] = dot_nt(delta_b, wh_ref[width:, :]).astype(jnp.bfloat16)
        return carry

    lax.fori_loop(0, pairs // WIDE, forward, 0)
    ends_row = ends_ref[...]

    def collect(k):
        first = burst_at(k) * WIDE
        total = dot32(pick(ends_row[0:1, :], first, WIDE, 0), pgl_s[...]) + dot32(
            pick(ends_row[1:2, :], first, WIDE, 0), pgr_s[...]
        )
        rgrad_s[wide_at(k), :] = total.astype(jnp.bfloat16)

    rgrad_of = lambda p: rgrad_s.at[rows_of(p), :]
    produce(collect, rgrad_of, back_s.at[rows_of(me), :], 2)
    back_s[rows_of(me), :] = rgrad_s[rows_of(me), :]
    ship(bursts - 1, rgrad_of, back_s.at[rows_of(me), :], 2)
    gw_s[2 * width : 3 * width, :] = dot_tn(left_s[...], delta_s[...])
    gw_s[3 * width :, :] = dot_tn(right_s[...], delta_s[...])

    def eighths(rows):
        wide = rows.reshape(burst // 2, 8, width)
        both = jnp.concatenate([wide[:, None, :, :LANES], wide[:, None, :, LANES:]], axis=1)
        return both.reshape(burst, 8, LANES).astype(jnp.bfloat16)

    def joined(blocks):
        wide = blocks.reshape(peers // 2, 2, 8, LANES)
        return jnp.concatenate([wide[:, 0], wide[:, 1]], axis=2).reshape(2 * width, width)

    def eighth_of(t):
        return pl.ds(pl.multiple_of(t * LANES, LANES), LANES)

    for k in range(bursts):
        t = burst_at(k)
        hpart_s[pl.ds(t * burst, burst)] = eighths(gw_s[eighth_of(t + bursts), :])
    hpart_of = lambda p: hpart_s.at[p]
    hprecv_s[me] = hpart_s[me]
    for k in range(bursts):
        ship(k, hpart_of, hprecv_s.at[me], 7)
    for k in range(bursts):
        arrived(k, back_s, block, 2)
        b = source_at(k)
        here = pl.ds(pl.multiple_of(b * WIDE, WIDE), WIDE)

        def put(i, carry):
            at = pl.ds(pl.multiple_of(i * TALL, TALL), TALL)
            found = dot32(pick(wrow_s[0:1, here].astype(jnp.int32), i * TALL, TALL, 0), back_s[here, :])
            gfeat_s[at, :] = found if k == 0 else gfeat_s[at, :] + found
            return carry

        lax.fori_loop(0, node_rows // TALL, put, 0)
    gradb_s[...] = gfeat_s[...].astype(jnp.bfloat16)
    gw_s[:width, :] = dot_tn(feat_ref[...], gradb_s[...])
    gw_s[width : 2 * width, :] = dot_tn(agg_s[...], gradb_s[...])
    def weight_terms(k):
        t = burst_at(k)
        part_s[pl.ds(t * burst, burst)] = eighths(gw_s[eighth_of(t), :])

    part_of = lambda p: part_s.at[p]
    produce(weight_terms, part_of, precv_s.at[me], 3)
    precv_s[me] = part_s[me]
    gt_s[...] = (dot_nt(wn_ref[...], gradb_s[...]) / deg_s[0:1, :]).astype(jnp.bfloat16)
    ship(bursts - 1, part_of, precv_s.at[me], 3)

    def table_grad(first):
        cols = pl.ds(pl.multiple_of(first, TILE), TILE)
        return jnp.transpose(dot32(gt_s[...], adj_s[:, cols]))

    def return_halo(k):
        t = burst_at(k)
        halo_s[pl.ds(t * burst, burst)] = halves(
            table_grad(node_rows + t * TILE)
        ).astype(jnp.bfloat16)

    halo_of = lambda p: halo_s.at[p]
    produce(return_halo, halo_of, hrecv_s.at[me], 4)
    hrecv_s[me] = halo_s[me]

    def direct(i, carry):
        at = tile_of(i)
        gfeat_s[at, :] = dot_nt(gradb_s[at, :], ws_ref[...]) + table_grad(i * TILE)
        return carry

    direct(0, 0)
    ship(bursts - 1, halo_of, hrecv_s.at[me], 4)
    for k in range(bursts):
        arrived(k, precv_s, 0, 3)
        arrived(k, hprecv_s, 0, 7)
    own = jnp.concatenate(
        [
            jnp.sum(precv_s[...].astype(jnp.float32), axis=0),
            jnp.sum(hprecv_s[...].astype(jnp.float32), axis=0),
        ],
        axis=0,
    )
    small = small_s[...]
    small_hi = small.astype(jnp.bfloat16).astype(jnp.float32)
    small_lo = small - small_hi
    lines = [
        part[r : r + 1, c : c + LANES]
        for part in (small_hi, small_lo)
        for r in range(2)
        for c in (0, LANES)
    ]
    share_s[...] = jnp.concatenate([own] + lines, axis=0).astype(jnp.bfloat16)
    direct(1, 0)

    core = lax.rem(me // grp, 2)
    partner = me + (1 - 2 * core) * grp
    groups = peers // (2 * grp)

    def share(i, carry):
        own_q = (me // (2 * grp)) * grp + lax.rem(me, grp)
        for u in range(7):
            q = jnp.bitwise_and(own_q + (i * 7 + u + 1) * 27, peers // 2 - 1)
            pltpu.make_async_remote_copy(
                src_ref=share_s,
                dst_ref=srecv_s.at[me],
                send_sem=send_sem.at[5],
                recv_sem=recv_sem.at[5, 0],
                device_id=q + (q // grp) * grp + core * grp,
                device_id_type=LOGICAL,
            ).start()
        return carry

    lax.fori_loop(0, (peers // 2 - 1) // 7, share, 0)
    srecv_s[me] = share_s[...]
    lax.fori_loop(2, tiles, direct, 0)
    for k in range(bursts):
        arrived(k, hrecv_s, 0, 4)
    hrows_s[...] = whole(hrecv_s[...]).reshape(peers * half, width).astype(jnp.bfloat16)

    def place(i, carry):
        at = pl.ds(pl.multiple_of(i * TALL, TALL), TALL)
        hot = pick(hrow_s[0:1, :].astype(jnp.int32), i * TALL, TALL, 0)
        gfeat_s[at, :] += dot32(hot, hrows_s[...])
        return carry

    lax.fori_loop(0, node_rows // TALL, place, 0)
    result = pltpu.make_async_copy(gfeat_s, gfeat_ref, adj_sem.at[0])
    result.start()
    others = srecv_s.at[pl.ds(1, peers // 2 - 1)]
    pltpu.make_async_copy(others, others, recv_sem.at[5, 0]).wait()

    def across(i, carry):
        part = srecv_s.at[pl.ds(i * (2 * grp) + core * grp, grp)]
        pltpu.make_async_remote_copy(
            src_ref=part,
            dst_ref=part,
            send_sem=send_sem.at[6],
            recv_sem=recv_sem.at[5, 1],
            device_id=partner,
            device_id_type=LOGICAL,
        ).start()
        return carry

    lax.fori_loop(0, groups, across, 0)
    sent(others, 5)
    sent(srecv_s.at[pl.ds(0, peers // 2)], 6)
    for which, ref in ((1, served_s), (2, rgrad_s)):
        sent(ref.at[pl.ds(block, recv_rows - block), :], which)
    for which, ref in ((0, frecv_s), (3, part_s), (4, halo_s), (7, hpart_s)):
        sent(ref.at[pl.ds(1, peers - 1)], which)
    mates = srecv_s.at[pl.ds(0, peers // 2)]
    pltpu.make_async_copy(mates, mates, recv_sem.at[5, 1]).wait()
    everyone = srecv_s[...].astype(jnp.float32)
    node_terms = joined(everyone[:, :8])
    gself_ref[...] = node_terms[:width]
    gneigh_ref[...] = node_terms[width:]
    ghid_ref[...] = joined(everyone[:, 8:16])
    total = jnp.sum(everyone[:, block:], axis=0)
    total = total[:4] + total[4:]
    gbias_ref[...] = jnp.concatenate([total[0:1], total[1:2]], axis=1)
    gout_ref[...] = jnp.concatenate([total[2:3], total[3:4]], axis=1)
    result.wait()


def finish_kernel(count, *refs):
    taken, given, held = refs[:count], refs[count : 2 * count], refs[2 * count : 3 * count]
    in_sem, out_sem = refs[3 * count :]
    parts = []
    for a, h, b in zip(taken, held, given):
        rows = a.shape[0]
        step = TILE if rows > TILE else rows
        parts += [(a, h, b, pl.ds(r, step)) for r in range(0, rows, step)]
    moves = [
        (
            pltpu.make_async_copy(a.at[at, :], h.at[at, :], in_sem.at[n]),
            pltpu.make_async_copy(h.at[at, :], b.at[at, :], out_sem.at[n]),
        )
        for n, (a, h, b, at) in enumerate(parts)
    ]
    for fetch, _ in moves:
        fetch.start()
    for fetch, put in moves:
        fetch.wait()
        put.start()
    for _, put in moves:
        put.wait()


def finish(arrays):
    count = len(arrays)
    moves = sum(max(a.shape[0] // TILE, 1) for a in arrays)
    return pl.pallas_call(
        lambda *refs: finish_kernel(count, *refs),
        out_shape=tuple(jax.ShapeDtypeStruct(a.shape, a.dtype) for a in arrays),
        in_specs=[ANY] * count,
        out_specs=(ANY,) * count,
        scratch_shapes=[pltpu.VMEM(a.shape, a.dtype) for a in arrays]
        + [pltpu.SemaphoreType.DMA((moves,)), pltpu.SemaphoreType.DMA((moves,))],
        compiler_params=params(60),
        name="finish",
    )(*arrays)


def train_step(
    adj, features, degt, ask, halo, ends, pair_weight, labels, w_self, w_neigh, w_hidden,
    bias, w_out
):
    node_rows, width = features.shape
    table_rows = adj.shape[1]
    block, peers = ask.shape
    half = halo.shape[0]
    recv_rows = peers * block
    pairs = ends.shape[1]
    lines = 2 * half + 8
    bf16 = lambda *shape: pltpu.VMEM(shape, jnp.bfloat16)
    return pl.pallas_call(
        step_kernel,
        out_shape=(
            jax.ShapeDtypeStruct((1, pairs), jnp.float32),
            jax.ShapeDtypeStruct((node_rows, width), jnp.float32),
            jax.ShapeDtypeStruct((width, width), jnp.float32),
            jax.ShapeDtypeStruct((width, width), jnp.float32),
            jax.ShapeDtypeStruct((2 * width, width), jnp.float32),
            jax.ShapeDtypeStruct((1, width), jnp.float32),
            jax.ShapeDtypeStruct((1, width), jnp.float32),
        ),
        in_specs=[ANY] + [VMEM] * 12,
        out_specs=(VMEM, ANY) + (VMEM,) * 5,
        scratch_shapes=[
            bf16(node_rows, table_rows),
            pltpu.VMEM((node_rows, width), jnp.float32),
            pltpu.VMEM((8, pairs), jnp.float32),
            pltpu.VMEM((8, node_rows), jnp.float32),
            pltpu.VMEM((peers * half, 1), jnp.float32),
            pltpu.VMEM((8, peers * half), jnp.float32),
            pltpu.VMEM((peers, LANES), jnp.float32),
            pltpu.VMEM((8, recv_rows), jnp.float32),
            bf16(peers, lines, LANES),
            bf16(peers, lines, LANES),
            bf16(peers * half, width),
            bf16(node_rows, width),
            bf16(node_rows, width),
            bf16(recv_rows, width),
            bf16(recv_rows, width),
            bf16(pairs, width),
            bf16(pairs, width),
            bf16(pairs, width),
            bf16(pairs, width),
            bf16(pairs, width),
            bf16(recv_rows, width),
            bf16(recv_rows, width),
            bf16(node_rows, width),
            bf16(width, node_rows),
            pltpu.VMEM((4 * width, width), jnp.float32),
            pltpu.VMEM((8, width), jnp.float32),
            pltpu.VMEM((pairs, 8), jnp.float32),
            bf16(peers, half, LANES),
            bf16(peers, half, LANES),
            bf16(peers, half, LANES),
            bf16(peers, half, LANES),
            bf16(peers, block, LANES),
            bf16(peers, block, LANES),
            bf16(peers * half, width),
            bf16(lines, LANES),
            bf16(peers, lines, LANES),
            pltpu.SemaphoreType.DMA((node_rows // TILE,)),
            pltpu.SemaphoreType.DMA((8,)),
            pltpu.SemaphoreType.DMA((8, recv_rows // WIDE)),
        ],
        compiler_params=pltpu.CompilerParams(
            vmem_limit_bytes=62 * 2**20, collective_id=0, has_side_effects=True
        ),
        cost_estimate=cost(30_000_000_000, 24 * 2**20),
        name="train_step",
    )(
        adj, features, degt, ask, halo, ends, pair_weight, labels, w_self, w_neigh,
        w_hidden, bias, w_out,
    )


def per_device(
    features,
    edge_src,
    edge_dst,
    edge_count,
    halo_index,
    request_rows,
    pair_ends,
    labels,
    pair_weight,
    w_self,
    w_neigh,
    w_hidden,
    b_hidden,
    w_out,
):
    node_rows = features.shape[0]
    halo = halo_index[0].T
    adj, degt = adjacency(edge_src, edge_dst, edge_count, node_rows, node_rows + halo.size)
    logits, grad_features, grad_self, grad_neigh, grad_hidden, grad_bias, grad_out = train_step(
        adj, features, degt, request_rows[0].T, halo, pair_ends.T, pair_weight[None],
        labels[None], w_self, w_neigh, w_hidden, b_hidden[None], w_out[None]
    )
    grad_features, grad_self, grad_neigh, grad_hidden, grad_bias, grad_out, logits = finish(
        (grad_features, grad_self, grad_neigh, grad_hidden, grad_bias, grad_out, logits)
    )
    return (
        logits[0],
        grad_features,
        grad_self,
        grad_neigh,
        grad_hidden,
        grad_bias[0],
        grad_out[0],
    )


def solution(mesh):
    split = P(AXES)
    in_specs = (
        P(AXES, None),
        split,
        split,
        split,
        P(AXES, None, None),
        P(AXES, None, None),
        P(AXES, None),
        split,
        split,
        P(),
        P(),
        P(),
        P(),
        P(),
    )
    out_specs = (split, P(AXES, None), P(), P(), P(), P(), P())
    return jax.shard_map(
        per_device, mesh=mesh, in_specs=in_specs, out_specs=out_specs, check_vma=False
    )
```

```python
import jax
import jax.numpy as jnp
from jax import lax
from jax.experimental import pallas as pl
from jax.experimental.pallas import tpu as pltpu
from jax.sharding import PartitionSpec as P

AXES = ("dom", "grp")
LANES = 128
GROUP = 8
STRIDE = LANES // GROUP
TILE = 256
WIDE = 512
TALL = 1024
LOGICAL = pl.DeviceIdType.LOGICAL
CLASH = 1 << 20
VMEM = pl.BlockSpec(memory_space=pltpu.VMEM)
SMEM = pl.BlockSpec(memory_space=pltpu.SMEM)
ANY = pl.BlockSpec(memory_space=pl.ANY)


def dot32(a, b):
    return jnp.dot(a, b, preferred_element_type=jnp.float32)


def dot_nt(a, b):
    return lax.dot_general(a, b, (((1,), (1,)), ((), ())), preferred_element_type=jnp.float32)


def dot_tn(a, b):
    return lax.dot_general(a, b, (((0,), (0,)), ((), ())), preferred_element_type=jnp.float32)


def params(mib):
    return pltpu.CompilerParams(vmem_limit_bytes=mib * 2**20)


def cost(flops, size):
    return pl.CostEstimate(flops=flops, bytes_accessed=size, transcendentals=0)


def tile_of(i):
    return pl.ds(pl.multiple_of(i * TILE, TILE), TILE)


def pick(index, first, count, axis):
    shape = (index.shape[0], count) if axis == 1 else (count, index.shape[1])
    ids = lax.broadcasted_iota(jnp.int32, shape, axis) + first
    return jnp.where(index == ids, 1.0, 0.0).astype(jnp.bfloat16)


def edge_words(half, panels, count, src, dst):
    shape = src.shape
    lane = lax.broadcasted_iota(jnp.int32, shape, 1)
    live = lax.broadcasted_iota(jnp.int32, shape, 0) * LANES + lane < count
    upper = jnp.where(dst >= half, 1, 0)
    row = jnp.right_shift(src, 7) * half + dst - upper * half
    row = jnp.where(live, row, half * panels + lane // STRIDE)
    unit = jnp.where(live, jnp.bitwise_and(src, LANES - 1) + upper * LANES, 2 * LANES)
    clash = jnp.zeros(shape, jnp.int32)
    for k in range(1, GROUP // 2 + 1):
        clash = clash + jnp.where(row == pltpu.roll(row, k * STRIDE, 1), 1, 0)
    any_clash = jnp.max(clash.astype(jnp.float32), axis=1, keepdims=True) > 0.0
    return row + jnp.where(any_clash & (lane == 0), CLASH, 0), unit


def counts_kernel(
    half, panels, count_ref, src_ref, dst_ref, adj_ref, degt_ref, even, odd, unit_a, unit_b,
    row_v, row_ref, unit_ref, row_sem
):
    step = pl.program_id(0)
    chunks = unit_ref.shape[0]

    @pl.when(step == 0)
    def _():
        row_v[...], unit_ref[...] = edge_words(
            half, panels, count_ref[0], src_ref[...], dst_ref[...]
        )
        words = pltpu.make_async_copy(row_v, row_ref, row_sem)
        words.start()
        lane = lax.broadcasted_iota(jnp.int32, (LANES, LANES), 1)

        def clear(i, carry):
            even[tile_of(i), :] = jnp.zeros((TILE, LANES), jnp.int32)
            odd[tile_of(i), :] = jnp.zeros((TILE, LANES), jnp.int32)
            return carry

        lax.fori_loop(0, half * panels // TILE, clear, 0)
        words.wait()

        def units_of(c):
            c = jnp.minimum(c, chunks - 1)
            wide = jnp.transpose(jnp.broadcast_to(unit_ref[pl.ds(c, 1), :], (LANES, LANES)))
            return jnp.where(wide == lane, 1, jnp.where(wide == lane + LANES, 65536, 0))

        unit_a[...] = units_of(0)

        def chunk(c, units, later):
            places = row_ref.at[c]
            head = places[0]

            def load(s):
                words = odd if s % 2 else even
                at = [places[s + STRIDE * t] for t in range(GROUP)]
                new = [
                    words[pl.ds(a, 1), :] + units[pl.ds(s + STRIDE * t, 1), :]
                    for t, a in enumerate(at)
                ]
                return words, at, new

            def store(words, at, new):
                for a, n in zip(at, new):
                    words[pl.ds(a, 1), :] = n

            @pl.when(head < CLASH)
            def _():
                coming = units_of(c + 1)
                held = load(0)
                for s in range(1, STRIDE):
                    following = load(s)
                    store(*held)
                    held = following
                store(*held)
                later[...] = coming

            @pl.when(head >= CLASH)
            def _():
                later[...] = units_of(c + 1)
                for j in range(LANES):
                    words = odd if j % 2 else even
                    a = places[j]
                    if j == 0:
                        a = a - CLASH
                    words[pl.ds(a, 1), :] = words[pl.ds(a, 1), :] + units[pl.ds(j, 1), :]

        def two(i, carry):
            chunk(2 * i, unit_a, unit_b)
            chunk(2 * i + 1, unit_b, unit_a)
            return carry

        lax.fori_loop(0, chunks // 2, two, 0)

    first = step * TILE
    total = jnp.zeros((TILE, LANES), jnp.int32)
    for p in range(panels):
        part = pl.ds(pl.multiple_of(p * half + first, TILE), TILE)
        word = even[part, :] + odd[part, :]
        total = total + word
        cols = slice(p * LANES, (p + 1) * LANES)
        for h, count in enumerate((jnp.bitwise_and(word, 0xFFFF), jnp.right_shift(word, 16))):
            adj_ref[h, :, cols] = count.astype(jnp.float32).astype(jnp.bfloat16)
    for h, count in enumerate((jnp.bitwise_and(total, 0xFFFF), jnp.right_shift(total, 16))):
        degree = jnp.sum(count.astype(jnp.float32), axis=1, keepdims=True)
        wide = jnp.broadcast_to(jnp.maximum(degree, 1.0), (TILE, LANES))
        degt_ref[h] = jnp.transpose(wide)[:8]


def adjacency(edge_src, edge_dst, edge_count, node_rows, table_rows):
    half = node_rows // 2
    panels = table_rows // LANES
    chunks = edge_src.shape[0] // LANES
    grid_shape = (chunks, LANES)
    adj, degt = pl.pallas_call(
        lambda *refs: counts_kernel(half, panels, *refs),
        grid=(half // TILE,),
        out_shape=(
            jax.ShapeDtypeStruct((2, half, table_rows), jnp.bfloat16),
            jax.ShapeDtypeStruct((2, 8, half), jnp.float32),
        ),
        in_specs=[SMEM] + [pl.BlockSpec(grid_shape, lambda i: (0, 0))] * 2,
        out_specs=(
            pl.BlockSpec((2, TILE, table_rows), lambda i: (0, i, 0)),
            pl.BlockSpec((2, 8, TILE), lambda i: (0, 0, i)),
        ),
        scratch_shapes=[
            pltpu.VMEM((half * panels + GROUP, LANES), jnp.int32),
            pltpu.VMEM((half * panels + GROUP, LANES), jnp.int32),
            pltpu.VMEM((LANES, LANES), jnp.int32),
            pltpu.VMEM((LANES, LANES), jnp.int32),
            pltpu.VMEM(grid_shape, jnp.int32),
            pltpu.SMEM(grid_shape, jnp.int32),
            pltpu.VMEM(grid_shape, jnp.int32),
            pltpu.SemaphoreType.DMA,
        ],
        compiler_params=params(60),
        cost_estimate=cost(60_000_000, 16 * 2**20),
        name="counts",
    )(edge_count, edge_src.reshape(grid_shape), edge_dst.reshape(grid_shape))
    return adj.reshape(node_rows, table_rows), degt


def step_kernel(
    adj_ref,
    feat_ref,
    degt_ref,
    ask_ref,
    halo_ref,
    ends_ref,
    weight_ref,
    label_ref,
    ws_ref,
    wn_ref,
    wh_ref,
    bias_ref,
    wo_ref,
    logit_ref,
    gfeat_ref,
    gself_ref,
    gneigh_ref,
    ghid_ref,
    gbias_ref,
    gout_ref,
    adj_s,
    gfeat_s,
    pair_s,
    deg_s,
    hcol_s,
    hrow_s,
    wcol_s,
    wfull_s,
    feat_t,
    agg_t,
    wrow_s,
    first_s,
    frecv_s,
    arr_s,
    emb_s,
    agg_s,
    served_s,
    recv_s,
    left_s,
    right_s,
    delta_s,
    pgl_s,
    pgr_s,
    rgrad_s,
    back_s,
    gradb_s,
    gt_s,
    gw_s,
    small_s,
    cols_s,
    part_s,
    precv_s,
    hpart_s,
    hprecv_s,
    halo_s,
    hrecv_s,
    hrows_s,
    share_s,
    srecv_s,
    adj_sem,
    send_sem,
    recv_sem,
):
    node_rows, width = feat_ref.shape
    block, peers = ask_ref.shape
    half = halo_ref.shape[0]
    recv_rows = peers * block
    pairs = ends_ref.shape[1]
    grp = lax.axis_size("grp")
    me = lax.axis_index("dom") * grp + lax.axis_index("grp")
    burst = WIDE // block
    bursts = peers // burst
    hburst = burst // 2
    tiles = node_rows // TILE
    barrier = pltpu.get_barrier_semaphore()

    def load_adj(i):
        return pltpu.make_async_copy(
            adj_ref.at[tile_of(i), :], adj_s.at[tile_of(i), :], adj_sem.at[i]
        )

    def fetch(i, carry):
        load_adj(i).start()
        return carry

    lax.fori_loop(0, tiles, fetch, 0)

    def greet(i, carry):
        for u in range(7):
            pl.semaphore_signal(
                barrier,
                inc=1,
                device_id=jnp.bitwise_and(me + (i * 7 + u + 1), peers - 1),
                device_id_type=LOGICAL,
            )
        return carry

    pl.semaphore_signal(
        barrier,
        inc=1,
        device_id=jnp.bitwise_and(me + (peers - 1), peers - 1),
        device_id_type=LOGICAL,
    )
    lax.fori_loop(0, (peers - 2) // 7, greet, 0)

    def rows_of(p):
        return pl.ds(pl.multiple_of(p * block, block), block)

    def burst_at(k):
        return lax.rem(me // burst + k, bursts)

    def ship(k, source, target, which):
        low = jnp.bitwise_and(me, burst - 1)
        first = burst_at(k) * burst

        def one(i):
            p = first + jnp.bitwise_and(low + i, burst - 1)
            pltpu.make_async_remote_copy(
                src_ref=source(p),
                dst_ref=target,
                send_sem=send_sem.at[which],
                recv_sem=recv_sem.at[which, k],
                device_id=p,
                device_id_type=LOGICAL,
            ).start()

        @pl.when(k > 0)
        def _():
            one(0)

        for i in range(1, burst):
            one(i)

    def arrived(k, ref, unit, which):
        first = pl.ds(unit, (burst - 1) * unit) if unit else pl.ds(1, burst - 1)
        rest = pl.ds(0, burst * unit) if unit else pl.ds(0, burst)
        if isinstance(k, int) and k == 0:
            part = ref.at[first]
        else:
            part = ref.at[rest]
        pltpu.make_async_copy(part, part, recv_sem.at[which, k]).wait()

    def sent(part, which):
        pltpu.make_async_copy(part, part, send_sem.at[which]).wait()

    def source_at(k):
        return lax.rem(me // burst - k + bursts, bursts)

    def produce(fill, source, target, which):
        fill(0)

        def middle(k, carry):
            fill(k)
            ship(k - 1, source, target, which)
            return carry

        lax.fori_loop(1, bursts, middle, 0)

    def halves(rows):
        wide = rows.reshape(burst, half, width)
        return jnp.concatenate([wide[:, :, :LANES], wide[:, :, LANES:]], axis=1)

    def whole(blocks):
        wide = blocks.astype(jnp.float32)
        return jnp.concatenate([wide[:, :half], wide[:, half : 2 * half]], axis=2)

    def spread(table, depth):
        shape = (table.shape[0], depth, table.shape[1])
        keep = lax.broadcasted_iota(jnp.int32, shape, 1) == lax.broadcasted_iota(
            jnp.int32, shape, 2
        )
        wide = jnp.broadcast_to(table[:, None, :], shape)
        one = jnp.sum(jnp.where(keep, wide, 0.0), axis=2, keepdims=True)
        return one.reshape(shape[0] * depth, 1)

    def as_row(col):
        return jnp.transpose(jnp.broadcast_to(col, (col.shape[0], LANES)))[:8]

    deg_s[...] = jnp.concatenate([degt_ref[0], degt_ref[1]], axis=1)
    hcol_s[...] = spread(jnp.transpose(halo_ref[...].astype(jnp.float32)), half)
    asks = ask_ref[...]
    ask_table = jnp.transpose(
        jnp.concatenate(
            [
                jnp.right_shift(asks, 6).astype(jnp.float32),
                jnp.bitwise_and(asks, 63).astype(jnp.float32),
                jnp.zeros((LANES - 2 * block, peers), jnp.float32),
            ],
            axis=0,
        )
    )
    wcol_s[0:peers, :] = ask_table

    def outgoing(t, carry):
        hot = pick(hcol_s[tile_of(t), :].astype(jnp.int32), 0, node_rows, 1)
        part = pl.ds(pl.multiple_of(t * burst, burst), burst)
        asked = jnp.broadcast_to(wcol_s[part, :][:, None, :], (burst, 8, LANES))
        first_s[part] = jnp.concatenate(
            [halves(dot32(hot, feat_ref[...])), asked], axis=1
        ).astype(jnp.bfloat16)
        return carry

    lax.fori_loop(0, bursts, outgoing, 0)

    def local_sums(i, carry):
        load_adj(i).wait()
        at = tile_of(i)
        gfeat_s[at, :] = dot32(adj_s[at, :node_rows], feat_ref[...])
        return carry

    lax.fori_loop(0, tiles, local_sums, 0)
    pl.semaphore_wait(barrier, peers - 1)
    first_of = lambda p: first_s.at[p]
    for k in range(bursts):
        ship(k, first_of, frecv_s.at[me], 0)
    frecv_s[me] = first_s[me]
    pair_s[...] = jnp.concatenate(
        [
            ends_ref[...].astype(jnp.float32),
            weight_ref[...],
            label_ref[...].astype(jnp.float32),
            jnp.zeros((4, pairs), jnp.float32),
        ],
        axis=0,
    )

    def columns(i, carry):
        at = pl.ds(pl.multiple_of(i * WIDE, WIDE), WIDE)
        cols_s[at, :] = jnp.transpose(pair_s[:, at])
        return carry

    lax.fori_loop(0, pairs // WIDE, columns, 0)
    hrow_s[...] = as_row(hcol_s[...])
    for k in range(bursts):
        arrived(k, frecv_s, 0, 0)
    arr_s[...] = whole(frecv_s[...]).reshape(peers * half, width).astype(jnp.bfloat16)
    codes = jnp.max(frecv_s[...].astype(jnp.float32)[:, 2 * half :], axis=1)
    wcol_s[0:peers, :] = codes * 64.0 + pltpu.roll(codes, LANES - block, 1)

    def ship_half(n, source, target, which):
        k = n // 2
        low = jnp.bitwise_and(me, hburst - 1)
        first = half_at(n)

        def one(i):
            p = first + jnp.bitwise_and(low + i, hburst - 1)
            pltpu.make_async_remote_copy(
                src_ref=source(p),
                dst_ref=target,
                send_sem=send_sem.at[which],
                recv_sem=recv_sem.at[which, k],
                device_id=p,
                device_id_type=LOGICAL,
            ).start()

        @pl.when(n > 0)
        def _():
            one(0)

        for i in range(1, hburst):
            one(i)

    def produce_halves(fill, source, target, which):
        fill(0)

        def middle(n, carry):
            fill(n)
            ship_half(n - 1, source, target, which)
            return carry

        lax.fori_loop(1, 2 * bursts, middle, 0)

    def encode(i, carry):
        at = pl.ds(pl.multiple_of(i * TALL, TALL), TALL)
        sums = gfeat_s[at, :] + dot32(adj_s[at, node_rows:], arr_s[...])
        degree = jnp.transpose(deg_s[:, at])[:, :1]
        mean = (sums / degree).astype(jnp.bfloat16)
        agg_s[at, :] = mean
        emb_s[at, :] = (dot32(feat_ref[at, :], ws_ref[...]) + dot32(mean, wn_ref[...])).astype(
            jnp.bfloat16
        )
        return carry

    lax.fori_loop(0, node_rows // TALL, encode, 0)

    def half_at(n):
        k, sub = n // 2, lax.rem(n, 2)
        low = jnp.bitwise_and(me, burst - 1) // hburst
        return burst_at(k) * burst + jnp.bitwise_and(low + sub, 1) * hburst

    def serve(n):
        p = half_at(n)
        at = pl.ds(pl.multiple_of(p * block, TILE), TILE)
        asked = spread(wcol_s[pl.ds(pl.multiple_of(p, hburst), hburst), :], block)
        wfull_s[at, :] = asked
        hot = pick(asked.astype(jnp.int32), 0, node_rows, 1)
        served_s[at, :] = dot32(hot, emb_s[...]).astype(jnp.bfloat16)

    served_of = lambda p: served_s.at[rows_of(p), :]
    produce_halves(serve, served_of, recv_s.at[rows_of(me), :], 1)
    recv_s[rows_of(me), :] = served_s[rows_of(me), :]
    small_s[...] = jnp.zeros(small_s.shape, jnp.float32)
    ship_half(2 * bursts - 1, served_of, recv_s.at[rows_of(me), :], 1)
    feat_t[...] = jnp.transpose(feat_ref[...])
    agg_t[...] = jnp.transpose(agg_s[...])

    def ask_rows(i, carry):
        at = pl.ds(pl.multiple_of(i * WIDE, WIDE), WIDE)
        wrow_s[:, at] = as_row(wfull_s[at, :])
        return carry

    lax.fori_loop(0, recv_rows // WIDE, ask_rows, 0)

    for k in range(bursts):
        arrived(k, recv_s, block, 1)
        b = source_at(k)
        here = pl.ds(pl.multiple_of(b * WIDE, WIDE), WIDE)

        def gather(i, carry):
            at = pl.ds(pl.multiple_of(i * TALL, TALL), TALL)
            for side, rows in ((0, left_s), (1, right_s)):
                ends = cols_s[at, side : side + 1].astype(jnp.int32)
                found = dot32(pick(ends, b * WIDE, WIDE, 1), recv_s[here, :]).astype(
                    jnp.bfloat16
                )
                rows[at, :] = found if k == 0 else rows[at, :] + found
            return carry

        lax.fori_loop(0, pairs // TALL, gather, 0)

    def forward(i, carry):
        at = pl.ds(pl.multiple_of(i * TALL, TALL), TALL)
        cols = cols_s[at, :]
        left = left_s[at, :]
        right = right_s[at, :]
        pre = dot32(left, wh_ref[:width, :]) + dot32(right, wh_ref[width:, :]) + bias_ref[...]
        hidden = jnp.maximum(pre, 0.0)
        logit = jnp.sum(hidden * wo_ref[...], axis=1, keepdims=True)
        logit_ref[:, at] = jnp.transpose(jnp.broadcast_to(logit, (TALL, LANES)))[:1]
        slope = cols[:, 2:3] * (jax.nn.sigmoid(logit) - cols[:, 3:4])
        delta = jnp.where(pre > 0, slope * wo_ref[...], 0.0)
        small_s[0:1, :] += jnp.sum(delta, axis=0, keepdims=True)
        small_s[1:2, :] += jnp.sum(slope * hidden, axis=0, keepdims=True)
        delta_b = delta.astype(jnp.bfloat16)
        delta_s[at, :] = delta_b
        pgl_s[at, :] = dot_nt(delta_b, wh_ref[:width, :]).astype(jnp.bfloat16)
        pgr_s[at, :] = dot_nt(delta_b, wh_ref[width:, :]).astype(jnp.bfloat16)
        return carry

    lax.fori_loop(0, pairs // TALL, forward, 0)
    ends_row = ends_ref[...]

    def collect(n):
        first = half_at(n) * block
        total = dot32(pick(ends_row[0:1, :], first, TILE, 0), pgl_s[...]) + dot32(
            pick(ends_row[1:2, :], first, TILE, 0), pgr_s[...]
        )
        rgrad_s[pl.ds(pl.multiple_of(first, TILE), TILE), :] = total.astype(jnp.bfloat16)

    rgrad_of = lambda p: rgrad_s.at[rows_of(p), :]
    produce_halves(collect, rgrad_of, back_s.at[rows_of(me), :], 2)
    back_s[rows_of(me), :] = rgrad_s[rows_of(me), :]
    ship_half(2 * bursts - 1, rgrad_of, back_s.at[rows_of(me), :], 2)
    gw_s[2 * width : 3 * width, :] = dot_tn(left_s[...], delta_s[...])
    gw_s[3 * width :, :] = dot_tn(right_s[...], delta_s[...])

    def eighths(rows):
        wide = rows.reshape(burst // 2, 8, width)
        both = jnp.concatenate([wide[:, None, :, :LANES], wide[:, None, :, LANES:]], axis=1)
        return both.reshape(burst, 8, LANES).astype(jnp.bfloat16)

    def joined(blocks):
        wide = blocks.reshape(peers // 2, 2, 8, LANES)
        return jnp.concatenate([wide[:, 0], wide[:, 1]], axis=2).reshape(2 * width, width)

    def eighth_of(t):
        return pl.ds(pl.multiple_of(t * LANES, LANES), LANES)

    for k in range(bursts):
        t = burst_at(k)
        hpart_s[pl.ds(t * burst, burst)] = eighths(gw_s[eighth_of(t + bursts), :])
    hpart_of = lambda p: hpart_s.at[p]
    hprecv_s[me] = hpart_s[me]
    for k in range(bursts):
        ship(k, hpart_of, hprecv_s.at[me], 7)
    for k in range(bursts):
        arrived(k, back_s, block, 2)
        b = source_at(k)
        here = pl.ds(pl.multiple_of(b * WIDE, WIDE), WIDE)

        def put(i, carry):
            at = pl.ds(pl.multiple_of(i * TALL, TALL), TALL)
            found = dot32(pick(wrow_s[0:1, here].astype(jnp.int32), i * TALL, TALL, 0), back_s[here, :])
            gfeat_s[at, :] = found if k == 0 else gfeat_s[at, :] + found
            return carry

        lax.fori_loop(0, node_rows // TALL, put, 0)
    gradb_s[...] = gfeat_s[...].astype(jnp.bfloat16)
    gw_s[:width, :] = dot32(feat_t[...], gradb_s[...])
    gw_s[width : 2 * width, :] = dot32(agg_t[...], gradb_s[...])
    def weight_terms(k):
        t = burst_at(k)
        part_s[pl.ds(t * burst, burst)] = eighths(gw_s[eighth_of(t), :])

    part_of = lambda p: part_s.at[p]
    produce(weight_terms, part_of, precv_s.at[me], 3)
    precv_s[me] = part_s[me]
    gt_s[...] = (dot_nt(wn_ref[...], gradb_s[...]) / deg_s[0:1, :]).astype(jnp.bfloat16)
    ship(bursts - 1, part_of, precv_s.at[me], 3)

    def table_grad(first):
        cols = pl.ds(pl.multiple_of(first, TILE), TILE)
        return jnp.transpose(dot32(gt_s[...], adj_s[:, cols]))

    def return_halo(k):
        t = burst_at(k)
        halo_s[pl.ds(t * burst, burst)] = halves(
            table_grad(node_rows + t * TILE)
        ).astype(jnp.bfloat16)

    halo_of = lambda p: halo_s.at[p]
    produce(return_halo, halo_of, hrecv_s.at[me], 4)
    hrecv_s[me] = halo_s[me]

    def direct(i, carry):
        at = tile_of(i)
        gfeat_s[at, :] = dot_nt(gradb_s[at, :], ws_ref[...]) + table_grad(i * TILE)
        return carry

    direct(0, 0)
    ship(bursts - 1, halo_of, hrecv_s.at[me], 4)
    for k in range(bursts):
        arrived(k, precv_s, 0, 3)
        arrived(k, hprecv_s, 0, 7)
    own = jnp.concatenate(
        [
            jnp.sum(precv_s[...].astype(jnp.float32), axis=0),
            jnp.sum(hprecv_s[...].astype(jnp.float32), axis=0),
        ],
        axis=0,
    )
    small = small_s[...]
    small_hi = small.astype(jnp.bfloat16).astype(jnp.float32)
    small_lo = small - small_hi
    lines = [
        part[r : r + 1, c : c + LANES]
        for part in (small_hi, small_lo)
        for r in range(2)
        for c in (0, LANES)
    ]
    share_s[...] = jnp.concatenate([own] + lines, axis=0).astype(jnp.bfloat16)
    direct(1, 0)

    core = lax.rem(me // grp, 2)
    partner = me + (1 - 2 * core) * grp
    groups = peers // (2 * grp)

    def share(i, carry):
        own_q = (me // (2 * grp)) * grp + lax.rem(me, grp)
        for u in range(7):
            q = jnp.bitwise_and(own_q + (i * 7 + u + 1) * 27, peers // 2 - 1)
            pltpu.make_async_remote_copy(
                src_ref=share_s,
                dst_ref=srecv_s.at[me],
                send_sem=send_sem.at[5],
                recv_sem=recv_sem.at[5, 0],
                device_id=q + (q // grp) * grp + core * grp,
                device_id_type=LOGICAL,
            ).start()
        return carry

    lax.fori_loop(0, (peers // 2 - 1) // 7, share, 0)
    srecv_s[me] = share_s[...]
    lax.fori_loop(2, tiles, direct, 0)
    for k in range(bursts):
        arrived(k, hrecv_s, 0, 4)
    hrows_s[...] = whole(hrecv_s[...]).reshape(peers * half, width).astype(jnp.bfloat16)

    def place(i, carry):
        at = pl.ds(pl.multiple_of(i * TALL, TALL), TALL)
        hot = pick(hrow_s[0:1, :].astype(jnp.int32), i * TALL, TALL, 0)
        gfeat_s[at, :] += dot32(hot, hrows_s[...])
        return carry

    lax.fori_loop(0, node_rows // TALL, place, 0)
    result = pltpu.make_async_copy(gfeat_s, gfeat_ref, adj_sem.at[0])
    result.start()
    others = srecv_s.at[pl.ds(1, peers // 2 - 1)]
    pltpu.make_async_copy(others, others, recv_sem.at[5, 0]).wait()

    def across(i, carry):
        part = srecv_s.at[pl.ds(i * (2 * grp) + core * grp, grp)]
        pltpu.make_async_remote_copy(
            src_ref=part,
            dst_ref=part,
            send_sem=send_sem.at[6],
            recv_sem=recv_sem.at[5, 1],
            device_id=partner,
            device_id_type=LOGICAL,
        ).start()
        return carry

    lax.fori_loop(0, groups, across, 0)
    sent(others, 5)
    sent(srecv_s.at[pl.ds(0, peers // 2)], 6)
    for which, ref in ((1, served_s), (2, rgrad_s)):
        sent(ref.at[pl.ds(block, recv_rows - block), :], which)
    for which, ref in ((0, frecv_s), (3, part_s), (4, halo_s), (7, hpart_s)):
        sent(ref.at[pl.ds(1, peers - 1)], which)
    mates = srecv_s.at[pl.ds(0, peers // 2)]
    pltpu.make_async_copy(mates, mates, recv_sem.at[5, 1]).wait()
    everyone = srecv_s[...].astype(jnp.float32)
    node_terms = joined(everyone[:, :8])
    gself_ref[...] = node_terms[:width]
    gneigh_ref[...] = node_terms[width:]
    ghid_ref[...] = joined(everyone[:, 8:16])
    total = jnp.sum(everyone[:, block:], axis=0)
    total = total[:4] + total[4:]
    gbias_ref[...] = jnp.concatenate([total[0:1], total[1:2]], axis=1)
    gout_ref[...] = jnp.concatenate([total[2:3], total[3:4]], axis=1)
    result.wait()


def finish_kernel(count, *refs):
    taken, given, held = refs[:count], refs[count : 2 * count], refs[2 * count : 3 * count]
    in_sem, out_sem = refs[3 * count :]
    parts = []
    for a, h, b in zip(taken, held, given):
        rows = a.shape[0]
        step = TILE if rows > TILE else rows
        parts += [(a, h, b, pl.ds(r, step)) for r in range(0, rows, step)]
    moves = [
        (
            pltpu.make_async_copy(a.at[at, :], h.at[at, :], in_sem.at[n]),
            pltpu.make_async_copy(h.at[at, :], b.at[at, :], out_sem.at[n]),
        )
        for n, (a, h, b, at) in enumerate(parts)
    ]
    for fetch, _ in moves:
        fetch.start()
    for fetch, put in moves:
        fetch.wait()
        put.start()
    for _, put in moves:
        put.wait()


def finish(arrays):
    count = len(arrays)
    moves = sum(max(a.shape[0] // TILE, 1) for a in arrays)
    return pl.pallas_call(
        lambda *refs: finish_kernel(count, *refs),
        out_shape=tuple(jax.ShapeDtypeStruct(a.shape, a.dtype) for a in arrays),
        in_specs=[ANY] * count,
        out_specs=(ANY,) * count,
        scratch_shapes=[pltpu.VMEM(a.shape, a.dtype) for a in arrays]
        + [pltpu.SemaphoreType.DMA((moves,)), pltpu.SemaphoreType.DMA((moves,))],
        compiler_params=params(60),
        name="finish",
    )(*arrays)


def train_step(
    adj, features, degt, ask, halo, ends, pair_weight, labels, w_self, w_neigh, w_hidden,
    bias, w_out
):
    node_rows, width = features.shape
    table_rows = adj.shape[1]
    block, peers = ask.shape
    half = halo.shape[0]
    recv_rows = peers * block
    pairs = ends.shape[1]
    lines = 2 * half + 8
    bf16 = lambda *shape: pltpu.VMEM(shape, jnp.bfloat16)
    return pl.pallas_call(
        step_kernel,
        out_shape=(
            jax.ShapeDtypeStruct((1, pairs), jnp.float32),
            jax.ShapeDtypeStruct((node_rows, width), jnp.float32),
            jax.ShapeDtypeStruct((width, width), jnp.float32),
            jax.ShapeDtypeStruct((width, width), jnp.float32),
            jax.ShapeDtypeStruct((2 * width, width), jnp.float32),
            jax.ShapeDtypeStruct((1, width), jnp.float32),
            jax.ShapeDtypeStruct((1, width), jnp.float32),
        ),
        in_specs=[ANY] + [VMEM] * 12,
        out_specs=(VMEM, ANY) + (VMEM,) * 5,
        scratch_shapes=[
            bf16(node_rows, table_rows),
            pltpu.VMEM((node_rows, width), jnp.float32),
            pltpu.VMEM((8, pairs), jnp.float32),
            pltpu.VMEM((8, node_rows), jnp.float32),
            pltpu.VMEM((peers * half, 1), jnp.float32),
            pltpu.VMEM((8, peers * half), jnp.float32),
            pltpu.VMEM((peers, LANES), jnp.float32),
            pltpu.VMEM((recv_rows, 1), jnp.float32),
            bf16(width, node_rows),
            bf16(width, node_rows),
            pltpu.VMEM((8, recv_rows), jnp.float32),
            bf16(peers, lines, LANES),
            bf16(peers, lines, LANES),
            bf16(peers * half, width),
            bf16(node_rows, width),
            bf16(node_rows, width),
            bf16(recv_rows, width),
            bf16(recv_rows, width),
            bf16(pairs, width),
            bf16(pairs, width),
            bf16(pairs, width),
            bf16(pairs, width),
            bf16(pairs, width),
            bf16(recv_rows, width),
            bf16(recv_rows, width),
            bf16(node_rows, width),
            bf16(width, node_rows),
            pltpu.VMEM((4 * width, width), jnp.float32),
            pltpu.VMEM((8, width), jnp.float32),
            pltpu.VMEM((pairs, 8), jnp.float32),
            bf16(peers, half, LANES),
            bf16(peers, half, LANES),
            bf16(peers, half, LANES),
            bf16(peers, half, LANES),
            bf16(peers, block, LANES),
            bf16(peers, block, LANES),
            bf16(peers * half, width),
            bf16(lines, LANES),
            bf16(peers, lines, LANES),
            pltpu.SemaphoreType.DMA((node_rows // TILE,)),
            pltpu.SemaphoreType.DMA((8,)),
            pltpu.SemaphoreType.DMA((8, recv_rows // WIDE)),
        ],
        compiler_params=pltpu.CompilerParams(
            vmem_limit_bytes=62 * 2**20, collective_id=0, has_side_effects=True
        ),
        cost_estimate=cost(30_000_000_000, 24 * 2**20),
        name="train_step",
    )(
        adj, features, degt, ask, halo, ends, pair_weight, labels, w_self, w_neigh,
        w_hidden, bias, w_out,
    )


def per_device(
    features,
    edge_src,
    edge_dst,
    edge_count,
    halo_index,
    request_rows,
    pair_ends,
    labels,
    pair_weight,
    w_self,
    w_neigh,
    w_hidden,
    b_hidden,
    w_out,
):
    node_rows = features.shape[0]
    halo = halo_index[0].T
    adj, degt = adjacency(edge_src, edge_dst, edge_count, node_rows, node_rows + halo.size)
    logits, grad_features, grad_self, grad_neigh, grad_hidden, grad_bias, grad_out = train_step(
        adj, features, degt, request_rows[0].T, halo, pair_ends.T, pair_weight[None],
        labels[None], w_self, w_neigh, w_hidden, b_hidden[None], w_out[None]
    )
    grad_features, grad_self, grad_neigh, grad_hidden, grad_bias, grad_out, logits = finish(
        (grad_features, grad_self, grad_neigh, grad_hidden, grad_bias, grad_out, logits)
    )
    return (
        logits[0],
        grad_features,
        grad_self,
        grad_neigh,
        grad_hidden,
        grad_bias[0],
        grad_out[0],
    )


def solution(mesh):
    split = P(AXES)
    in_specs = (
        P(AXES, None),
        split,
        split,
        split,
        P(AXES, None, None),
        P(AXES, None, None),
        P(AXES, None),
        split,
        split,
        P(),
        P(),
        P(),
        P(),
        P(),
    )
    out_specs = (split, P(AXES, None), P(), P(), P(), P(), P())
    return jax.shard_map(
        per_device, mesh=mesh, in_specs=in_specs, out_specs=out_specs, check_vma=False
    )
```

```python
import jax
import jax.numpy as jnp
from jax import lax
from jax.experimental import pallas as pl
from jax.experimental.pallas import tpu as pltpu
from jax.sharding import PartitionSpec as P

AXES = ("dom", "grp")
LANES = 128
GROUP = 8
STRIDE = LANES // GROUP
TILE = 256
WIDE = 512
TALL = 1024
LOGICAL = pl.DeviceIdType.LOGICAL
CLASH = 1 << 20
VMEM = pl.BlockSpec(memory_space=pltpu.VMEM)
SMEM = pl.BlockSpec(memory_space=pltpu.SMEM)
ANY = pl.BlockSpec(memory_space=pl.ANY)


def dot32(a, b):
    return jnp.dot(a, b, preferred_element_type=jnp.float32)


def dot_nt(a, b):
    return lax.dot_general(a, b, (((1,), (1,)), ((), ())), preferred_element_type=jnp.float32)


def dot_tn(a, b):
    return lax.dot_general(a, b, (((0,), (0,)), ((), ())), preferred_element_type=jnp.float32)


def params(mib):
    return pltpu.CompilerParams(vmem_limit_bytes=mib * 2**20)


def cost(flops, size):
    return pl.CostEstimate(flops=flops, bytes_accessed=size, transcendentals=0)


def tile_of(i):
    return pl.ds(pl.multiple_of(i * TILE, TILE), TILE)


def pick(index, first, count, axis):
    shape = (index.shape[0], count) if axis == 1 else (count, index.shape[1])
    ids = lax.broadcasted_iota(jnp.int32, shape, axis) + first
    return jnp.where(index == ids, 1.0, 0.0).astype(jnp.bfloat16)


def edge_words(half, panels, count, src, dst):
    shape = src.shape
    lane = lax.broadcasted_iota(jnp.int32, shape, 1)
    live = lax.broadcasted_iota(jnp.int32, shape, 0) * LANES + lane < count
    upper = jnp.where(dst >= half, 1, 0)
    row = jnp.right_shift(src, 7) * half + dst - upper * half
    row = jnp.where(live, row, half * panels + lane // STRIDE)
    unit = jnp.where(live, jnp.bitwise_and(src, LANES - 1) + upper * LANES, 2 * LANES)
    clash = jnp.zeros(shape, jnp.int32)
    for k in range(1, GROUP // 2 + 1):
        clash = clash + jnp.where(row == pltpu.roll(row, k * STRIDE, 1), 1, 0)
    any_clash = jnp.max(clash.astype(jnp.float32), axis=1, keepdims=True) > 0.0
    return row + jnp.where(any_clash & (lane == 0), CLASH, 0), unit


def counts_kernel(
    half, panels, count_ref, src_ref, dst_ref, adj_ref, degt_ref, even, odd, unit_a, unit_b,
    row_v, row_ref, unit_ref, row_sem
):
    step = pl.program_id(0)
    chunks = unit_ref.shape[0]

    @pl.when(step == 0)
    def _():
        row_v[...], unit_ref[...] = edge_words(
            half, panels, count_ref[0], src_ref[...], dst_ref[...]
        )
        words = pltpu.make_async_copy(row_v, row_ref, row_sem)
        words.start()
        lane = lax.broadcasted_iota(jnp.int32, (LANES, LANES), 1)

        def clear(i, carry):
            even[tile_of(i), :] = jnp.zeros((TILE, LANES), jnp.int32)
            odd[tile_of(i), :] = jnp.zeros((TILE, LANES), jnp.int32)
            return carry

        lax.fori_loop(0, half * panels // TILE, clear, 0)
        words.wait()

        def units_of(c):
            c = jnp.minimum(c, chunks - 1)
            wide = jnp.transpose(jnp.broadcast_to(unit_ref[pl.ds(c, 1), :], (LANES, LANES)))
            return jnp.where(wide == lane, 1, jnp.where(wide == lane + LANES, 65536, 0))

        unit_a[...] = units_of(0)

        def chunk(c, units, later):
            places = row_ref.at[c]
            head = places[0]

            def load(s):
                words = odd if s % 2 else even
                at = [places[s + STRIDE * t] for t in range(GROUP)]
                new = [
                    words[pl.ds(a, 1), :] + units[pl.ds(s + STRIDE * t, 1), :]
                    for t, a in enumerate(at)
                ]
                return words, at, new

            def store(words, at, new):
                for a, n in zip(at, new):
                    words[pl.ds(a, 1), :] = n

            @pl.when(head < CLASH)
            def _():
                coming = units_of(c + 1)
                held = load(0)
                for s in range(1, STRIDE):
                    following = load(s)
                    store(*held)
                    held = following
                store(*held)
                later[...] = coming

            @pl.when(head >= CLASH)
            def _():
                later[...] = units_of(c + 1)
                for j in range(LANES):
                    words = odd if j % 2 else even
                    a = places[j]
                    if j == 0:
                        a = a - CLASH
                    words[pl.ds(a, 1), :] = words[pl.ds(a, 1), :] + units[pl.ds(j, 1), :]

        def two(i, carry):
            chunk(2 * i, unit_a, unit_b)
            chunk(2 * i + 1, unit_b, unit_a)
            return carry

        lax.fori_loop(0, chunks // 2, two, 0)

    first = step * TILE
    total = jnp.zeros((TILE, LANES), jnp.int32)
    for p in range(panels):
        part = pl.ds(pl.multiple_of(p * half + first, TILE), TILE)
        word = even[part, :] + odd[part, :]
        total = total + word
        cols = slice(p * LANES, (p + 1) * LANES)
        for h, count in enumerate((jnp.bitwise_and(word, 0xFFFF), jnp.right_shift(word, 16))):
            adj_ref[h, :, cols] = count.astype(jnp.float32).astype(jnp.bfloat16)
    for h, count in enumerate((jnp.bitwise_and(total, 0xFFFF), jnp.right_shift(total, 16))):
        degree = jnp.sum(count.astype(jnp.float32), axis=1, keepdims=True)
        wide = jnp.broadcast_to(jnp.maximum(degree, 1.0), (TILE, LANES))
        degt_ref[h] = jnp.transpose(wide)[:8]


def adjacency(edge_src, edge_dst, edge_count, node_rows, table_rows):
    half = node_rows // 2
    panels = table_rows // LANES
    chunks = edge_src.shape[0] // LANES
    grid_shape = (chunks, LANES)
    adj, degt = pl.pallas_call(
        lambda *refs: counts_kernel(half, panels, *refs),
        grid=(half // TILE,),
        out_shape=(
            jax.ShapeDtypeStruct((2, half, table_rows), jnp.bfloat16),
            jax.ShapeDtypeStruct((2, 8, half), jnp.float32),
        ),
        in_specs=[SMEM] + [pl.BlockSpec(grid_shape, lambda i: (0, 0))] * 2,
        out_specs=(
            pl.BlockSpec((2, TILE, table_rows), lambda i: (0, i, 0)),
            pl.BlockSpec((2, 8, TILE), lambda i: (0, 0, i)),
        ),
        scratch_shapes=[
            pltpu.VMEM((half * panels + GROUP, LANES), jnp.int32),
            pltpu.VMEM((half * panels + GROUP, LANES), jnp.int32),
            pltpu.VMEM((LANES, LANES), jnp.int32),
            pltpu.VMEM((LANES, LANES), jnp.int32),
            pltpu.VMEM(grid_shape, jnp.int32),
            pltpu.SMEM(grid_shape, jnp.int32),
            pltpu.VMEM(grid_shape, jnp.int32),
            pltpu.SemaphoreType.DMA,
        ],
        compiler_params=params(60),
        cost_estimate=cost(60_000_000, 16 * 2**20),
        name="counts",
    )(edge_count, edge_src.reshape(grid_shape), edge_dst.reshape(grid_shape))
    return adj.reshape(node_rows, table_rows), degt


def step_kernel(
    adj_ref,
    feat_in,
    degt_ref,
    ask_ref,
    halo_ref,
    ends_ref,
    weight_ref,
    label_ref,
    ws_in,
    wn_in,
    wh_in,
    bias_ref,
    wo_ref,
    logit_ref,
    gfeat_ref,
    gself_ref,
    gneigh_ref,
    ghid_ref,
    gbias_ref,
    gout_ref,
    adj_s,
    feat_ref,
    ws_ref,
    wn_ref,
    wh_ref,
    gfeat_s,
    pair_s,
    deg_s,
    hcol_s,
    hrow_s,
    wcol_s,
    wfull_s,
    feat_t,
    agg_t,
    wrow_s,
    ask_s,
    arecv_s,
    first_s,
    frecv_s,
    arr_s,
    emb_s,
    agg_s,
    served_s,
    recv_s,
    left_s,
    right_s,
    delta_s,
    pgl_s,
    pgr_s,
    rgrad_s,
    back_s,
    gradb_s,
    gt_s,
    gw_s,
    small_s,
    cols_s,
    part_s,
    precv_s,
    hpart_s,
    hprecv_s,
    halo_s,
    hrecv_s,
    hrows_s,
    share_s,
    srecv_s,
    in_sem,
    adj_sem,
    send_sem,
    recv_sem,
):
    node_rows, width = feat_ref.shape
    block, peers = ask_ref.shape
    half = halo_ref.shape[0]
    recv_rows = peers * block
    pairs = ends_ref.shape[1]
    grp = lax.axis_size("grp")
    me = lax.axis_index("dom") * grp + lax.axis_index("grp")
    burst = WIDE // block
    bursts = peers // burst
    hburst = burst // 2
    tiles = node_rows // TILE
    barrier = pltpu.get_barrier_semaphore()

    def load_adj(i):
        return pltpu.make_async_copy(
            adj_ref.at[tile_of(i), :], adj_s.at[tile_of(i), :], adj_sem.at[i]
        )

    loads = [
        pltpu.make_async_copy(a, b, in_sem.at[n])
        for n, (a, b) in enumerate(
            ((feat_in, feat_ref), (ws_in, ws_ref), (wn_in, wn_ref), (wh_in, wh_ref))
        )
    ]
    for load in loads:
        load.start()

    def fetch(i, carry):
        load_adj(i).start()
        return carry


    def greet(i, carry):
        for u in range(7):
            pl.semaphore_signal(
                barrier,
                inc=1,
                device_id=jnp.bitwise_and(me + (i * 7 + u + 1), peers - 1),
                device_id_type=LOGICAL,
            )
        return carry

    pl.semaphore_signal(
        barrier,
        inc=1,
        device_id=jnp.bitwise_and(me + (peers - 1), peers - 1),
        device_id_type=LOGICAL,
    )
    lax.fori_loop(0, (peers - 2) // 7, greet, 0)
    lax.fori_loop(0, tiles, fetch, 0)
    for load in loads:
        load.wait()

    def rows_of(p):
        return pl.ds(pl.multiple_of(p * block, block), block)

    def burst_at(k):
        return lax.rem(me // burst + k, bursts)

    def ship(k, source, target, which):
        low = jnp.bitwise_and(me, burst - 1)
        first = burst_at(k) * burst

        def one(i):
            p = first + jnp.bitwise_and(low + i, burst - 1)
            pltpu.make_async_remote_copy(
                src_ref=source(p),
                dst_ref=target,
                send_sem=send_sem.at[which],
                recv_sem=recv_sem.at[which, k],
                device_id=p,
                device_id_type=LOGICAL,
            ).start()

        @pl.when(k > 0)
        def _():
            one(0)

        for i in range(1, burst):
            one(i)

    def arrived(k, ref, unit, which):
        first = pl.ds(unit, (burst - 1) * unit) if unit else pl.ds(1, burst - 1)
        rest = pl.ds(0, burst * unit) if unit else pl.ds(0, burst)
        if isinstance(k, int) and k == 0:
            part = ref.at[first]
        else:
            part = ref.at[rest]
        pltpu.make_async_copy(part, part, recv_sem.at[which, k]).wait()

    def sent(part, which):
        pltpu.make_async_copy(part, part, send_sem.at[which]).wait()

    def source_at(k):
        return lax.rem(me // burst - k + bursts, bursts)

    def produce(fill, source, target, which):
        fill(0)

        def middle(k, carry):
            fill(k)
            ship(k - 1, source, target, which)
            return carry

        lax.fori_loop(1, bursts, middle, 0)

    def halves(rows):
        wide = rows.reshape(burst, half, width)
        return jnp.concatenate([wide[:, :, :LANES], wide[:, :, LANES:]], axis=1)

    def whole(blocks):
        wide = blocks.astype(jnp.float32)
        return jnp.concatenate([wide[:, :half], wide[:, half : 2 * half]], axis=2)

    def spread(table, depth):
        shape = (table.shape[0], depth, table.shape[1])
        keep = lax.broadcasted_iota(jnp.int32, shape, 1) == lax.broadcasted_iota(
            jnp.int32, shape, 2
        )
        wide = jnp.broadcast_to(table[:, None, :], shape)
        one = jnp.sum(jnp.where(keep, wide, 0.0), axis=2, keepdims=True)
        return one.reshape(shape[0] * depth, 1)

    def as_row(col):
        return jnp.transpose(jnp.broadcast_to(col, (col.shape[0], LANES)))[:8]

    deg_s[...] = jnp.concatenate([degt_ref[0], degt_ref[1]], axis=1)
    hcol_s[...] = spread(jnp.transpose(halo_ref[...].astype(jnp.float32)), half)
    ask_table = jnp.transpose(
        jnp.concatenate(
            [ask_ref[...].astype(jnp.float32), jnp.zeros((LANES - block, peers), jnp.float32)],
            axis=0,
        )
    )
    ask_s[...] = ask_table.astype(jnp.int32).reshape(peers, 1, LANES)

    def outgoing(t, carry):
        hot = pick(hcol_s[tile_of(t), :].astype(jnp.int32), 0, node_rows, 1)
        part = pl.ds(pl.multiple_of(t * burst, burst), burst)
        first_s[part] = halves(dot32(hot, feat_ref[...])).astype(jnp.bfloat16)
        return carry

    lax.fori_loop(0, bursts, outgoing, 0)

    def local_sums(i, carry):
        load_adj(i).wait()
        at = tile_of(i)
        gfeat_s[at, :] = dot32(adj_s[at, :node_rows], feat_ref[...])
        return carry

    lax.fori_loop(0, tiles, local_sums, 0)
    pl.semaphore_wait(barrier, peers - 1)
    first_of = lambda p: first_s.at[p]
    for k in range(bursts):
        ship(k, first_of, frecv_s.at[me], 0)
    ask_of = lambda p: ask_s.at[p]
    for k in range(bursts):
        ship(k, ask_of, arecv_s.at[me], 8)
    frecv_s[me] = first_s[me]
    arecv_s[me] = ask_s[me]
    pair_s[...] = jnp.concatenate(
        [
            ends_ref[...].astype(jnp.float32),
            weight_ref[...],
            label_ref[...].astype(jnp.float32),
            jnp.zeros((4, pairs), jnp.float32),
        ],
        axis=0,
    )

    def columns(i, carry):
        at = pl.ds(pl.multiple_of(i * WIDE, WIDE), WIDE)
        cols_s[at, :] = jnp.transpose(pair_s[:, at])
        return carry

    lax.fori_loop(0, pairs // WIDE, columns, 0)
    hrow_s[...] = as_row(hcol_s[...])
    for k in range(bursts):
        arrived(k, frecv_s, 0, 0)
        arrived(k, arecv_s, 0, 8)
    arr_s[...] = whole(frecv_s[...]).reshape(peers * half, width).astype(jnp.bfloat16)
    wcol_s[0:peers, :] = jnp.max(arecv_s[...], axis=1).astype(jnp.float32)

    def ship_half(n, source, target, which):
        k = n // 2
        low = jnp.bitwise_and(me, hburst - 1)
        first = half_at(n)

        def one(i):
            p = first + jnp.bitwise_and(low + i, hburst - 1)
            pltpu.make_async_remote_copy(
                src_ref=source(p),
                dst_ref=target,
                send_sem=send_sem.at[which],
                recv_sem=recv_sem.at[which, k],
                device_id=p,
                device_id_type=LOGICAL,
            ).start()

        @pl.when(n > 0)
        def _():
            one(0)

        for i in range(1, hburst):
            one(i)

    def produce_halves(fill, source, target, which):
        fill(0)

        def middle(n, carry):
            fill(n)
            ship_half(n - 1, source, target, which)
            return carry

        lax.fori_loop(1, 2 * bursts, middle, 0)

    def encode(i, carry):
        at = pl.ds(pl.multiple_of(i * TALL, TALL), TALL)
        sums = gfeat_s[at, :] + dot32(adj_s[at, node_rows:], arr_s[...])
        degree = jnp.transpose(deg_s[:, at])[:, :1]
        mean = (sums / degree).astype(jnp.bfloat16)
        agg_s[at, :] = mean
        emb_s[at, :] = (dot32(feat_ref[at, :], ws_ref[...]) + dot32(mean, wn_ref[...])).astype(
            jnp.bfloat16
        )
        return carry

    lax.fori_loop(0, node_rows // TALL, encode, 0)

    def half_at(n):
        k, sub = n // 2, lax.rem(n, 2)
        low = jnp.bitwise_and(me, burst - 1) // hburst
        return burst_at(k) * burst + jnp.bitwise_and(low + sub, 1) * hburst

    def serve(n):
        p = half_at(n)
        at = pl.ds(pl.multiple_of(p * block, TILE), TILE)
        asked = spread(wcol_s[pl.ds(pl.multiple_of(p, hburst), hburst), :], block)
        wfull_s[at, :] = asked
        hot = pick(asked.astype(jnp.int32), 0, node_rows, 1)
        served_s[at, :] = dot32(hot, emb_s[...]).astype(jnp.bfloat16)

    served_of = lambda p: served_s.at[rows_of(p), :]
    produce_halves(serve, served_of, recv_s.at[rows_of(me), :], 1)
    recv_s[rows_of(me), :] = served_s[rows_of(me), :]
    small_s[...] = jnp.zeros(small_s.shape, jnp.float32)
    ship_half(2 * bursts - 1, served_of, recv_s.at[rows_of(me), :], 1)
    feat_t[...] = jnp.transpose(feat_ref[...])
    agg_t[...] = jnp.transpose(agg_s[...])

    def ask_rows(i, carry):
        at = pl.ds(pl.multiple_of(i * WIDE, WIDE), WIDE)
        wrow_s[:, at] = as_row(wfull_s[at, :])
        return carry

    lax.fori_loop(0, recv_rows // WIDE, ask_rows, 0)

    for k in range(bursts):
        arrived(k, recv_s, block, 1)
        b = source_at(k)
        here = pl.ds(pl.multiple_of(b * WIDE, WIDE), WIDE)

        def gather(i, carry):
            at = pl.ds(pl.multiple_of(i * TALL, TALL), TALL)
            for side, rows in ((0, left_s), (1, right_s)):
                ends = cols_s[at, side : side + 1].astype(jnp.int32)
                found = dot32(pick(ends, b * WIDE, WIDE, 1), recv_s[here, :]).astype(
                    jnp.bfloat16
                )
                rows[at, :] = found if k == 0 else rows[at, :] + found
            return carry

        lax.fori_loop(0, pairs // TALL, gather, 0)

    def forward(i, carry):
        at = pl.ds(pl.multiple_of(i * TALL, TALL), TALL)
        cols = cols_s[at, :]
        left = left_s[at, :]
        right = right_s[at, :]
        pre = dot32(left, wh_ref[:width, :]) + dot32(right, wh_ref[width:, :]) + bias_ref[...]
        hidden = jnp.maximum(pre, 0.0)
        logit = jnp.sum(hidden * wo_ref[...], axis=1, keepdims=True)
        logit_ref[:, at] = jnp.transpose(jnp.broadcast_to(logit, (TALL, LANES)))[:1]
        slope = cols[:, 2:3] * (jax.nn.sigmoid(logit) - cols[:, 3:4])
        delta = jnp.where(pre > 0, slope * wo_ref[...], 0.0)
        small_s[0:1, :] += jnp.sum(delta, axis=0, keepdims=True)
        small_s[1:2, :] += jnp.sum(slope * hidden, axis=0, keepdims=True)
        delta_b = delta.astype(jnp.bfloat16)
        delta_s[at, :] = delta_b
        pgl_s[at, :] = dot_nt(delta_b, wh_ref[:width, :]).astype(jnp.bfloat16)
        pgr_s[at, :] = dot_nt(delta_b, wh_ref[width:, :]).astype(jnp.bfloat16)
        return carry

    lax.fori_loop(0, pairs // TALL, forward, 0)
    ends_row = ends_ref[...]

    def collect(n):
        first = half_at(n) * block
        total = dot32(pick(ends_row[0:1, :], first, TILE, 0), pgl_s[...]) + dot32(
            pick(ends_row[1:2, :], first, TILE, 0), pgr_s[...]
        )
        rgrad_s[pl.ds(pl.multiple_of(first, TILE), TILE), :] = total.astype(jnp.bfloat16)

    rgrad_of = lambda p: rgrad_s.at[rows_of(p), :]
    produce_halves(collect, rgrad_of, back_s.at[rows_of(me), :], 2)
    back_s[rows_of(me), :] = rgrad_s[rows_of(me), :]
    ship_half(2 * bursts - 1, rgrad_of, back_s.at[rows_of(me), :], 2)
    gw_s[2 * width : 3 * width, :] = dot_tn(left_s[...], delta_s[...])
    gw_s[3 * width :, :] = dot_tn(right_s[...], delta_s[...])

    def eighths(rows):
        wide = rows.reshape(burst // 2, 8, width)
        both = jnp.concatenate([wide[:, None, :, :LANES], wide[:, None, :, LANES:]], axis=1)
        return both.reshape(burst, 8, LANES).astype(jnp.bfloat16)

    def joined(blocks):
        wide = blocks.reshape(peers // 2, 2, 8, LANES)
        return jnp.concatenate([wide[:, 0], wide[:, 1]], axis=2).reshape(2 * width, width)

    def eighth_of(t):
        return pl.ds(pl.multiple_of(t * LANES, LANES), LANES)

    for k in range(bursts):
        t = burst_at(k)
        hpart_s[pl.ds(t * burst, burst)] = eighths(gw_s[eighth_of(t + bursts), :])
    hpart_of = lambda p: hpart_s.at[p]
    hprecv_s[me] = hpart_s[me]
    for k in range(bursts):
        ship(k, hpart_of, hprecv_s.at[me], 7)
    for k in range(bursts):
        arrived(k, back_s, block, 2)
        b = source_at(k)
        here = pl.ds(pl.multiple_of(b * WIDE, WIDE), WIDE)

        def put(i, carry):
            at = pl.ds(pl.multiple_of(i * TALL, TALL), TALL)
            found = dot32(pick(wrow_s[0:1, here].astype(jnp.int32), i * TALL, TALL, 0), back_s[here, :])
            gfeat_s[at, :] = found if k == 0 else gfeat_s[at, :] + found
            return carry

        lax.fori_loop(0, node_rows // TALL, put, 0)
    gradb_s[...] = gfeat_s[...].astype(jnp.bfloat16)
    gw_s[:width, :] = dot32(feat_t[...], gradb_s[...])
    gw_s[width : 2 * width, :] = dot32(agg_t[...], gradb_s[...])
    def weight_terms(k):
        t = burst_at(k)
        part_s[pl.ds(t * burst, burst)] = eighths(gw_s[eighth_of(t), :])

    part_of = lambda p: part_s.at[p]
    produce(weight_terms, part_of, precv_s.at[me], 3)
    precv_s[me] = part_s[me]
    gt_s[...] = (dot_nt(wn_ref[...], gradb_s[...]) / deg_s[0:1, :]).astype(jnp.bfloat16)
    ship(bursts - 1, part_of, precv_s.at[me], 3)

    def table_grad(first):
        cols = pl.ds(pl.multiple_of(first, TILE), TILE)
        return jnp.transpose(dot32(gt_s[...], adj_s[:, cols]))

    def return_halo(k):
        t = burst_at(k)
        halo_s[pl.ds(t * burst, burst)] = halves(
            table_grad(node_rows + t * TILE)
        ).astype(jnp.bfloat16)

    halo_of = lambda p: halo_s.at[p]
    produce(return_halo, halo_of, hrecv_s.at[me], 4)
    hrecv_s[me] = halo_s[me]

    def direct(i, carry):
        at = tile_of(i)
        gfeat_s[at, :] = dot_nt(gradb_s[at, :], ws_ref[...]) + table_grad(i * TILE)
        return carry

    direct(0, 0)
    ship(bursts - 1, halo_of, hrecv_s.at[me], 4)
    for k in range(bursts):
        arrived(k, precv_s, 0, 3)
        arrived(k, hprecv_s, 0, 7)
    own = jnp.concatenate(
        [
            jnp.sum(precv_s[...].astype(jnp.float32), axis=0),
            jnp.sum(hprecv_s[...].astype(jnp.float32), axis=0),
        ],
        axis=0,
    )
    small = small_s[...]
    small_hi = small.astype(jnp.bfloat16).astype(jnp.float32)
    small_lo = small - small_hi
    lines = [
        part[r : r + 1, c : c + LANES]
        for part in (small_hi, small_lo)
        for r in range(2)
        for c in (0, LANES)
    ]
    share_s[...] = jnp.concatenate([own] + lines, axis=0).astype(jnp.bfloat16)
    direct(1, 0)

    core = lax.rem(me // grp, 2)
    partner = me + (1 - 2 * core) * grp
    groups = peers // (2 * grp)

    def share(i, carry):
        own_q = (me // (2 * grp)) * grp + lax.rem(me, grp)
        for u in range(7):
            q = jnp.bitwise_and(own_q + (i * 7 + u + 1) * 27, peers // 2 - 1)
            pltpu.make_async_remote_copy(
                src_ref=share_s,
                dst_ref=srecv_s.at[me],
                send_sem=send_sem.at[5],
                recv_sem=recv_sem.at[5, 0],
                device_id=q + (q // grp) * grp + core * grp,
                device_id_type=LOGICAL,
            ).start()
        return carry

    lax.fori_loop(0, (peers // 2 - 1) // 7, share, 0)
    srecv_s[me] = share_s[...]
    lax.fori_loop(2, tiles, direct, 0)
    for k in range(bursts):
        arrived(k, hrecv_s, 0, 4)
    hrows_s[...] = whole(hrecv_s[...]).reshape(peers * half, width).astype(jnp.bfloat16)

    def place(i, carry):
        at = pl.ds(pl.multiple_of(i * TALL, TALL), TALL)
        hot = pick(hrow_s[0:1, :].astype(jnp.int32), i * TALL, TALL, 0)
        gfeat_s[at, :] += dot32(hot, hrows_s[...])
        return carry

    lax.fori_loop(0, node_rows // TALL, place, 0)
    result = pltpu.make_async_copy(gfeat_s, gfeat_ref, adj_sem.at[0])
    result.start()
    others = srecv_s.at[pl.ds(1, peers // 2 - 1)]
    pltpu.make_async_copy(others, others, recv_sem.at[5, 0]).wait()

    def across(i, carry):
        part = srecv_s.at[pl.ds(i * (2 * grp) + core * grp, grp)]
        pltpu.make_async_remote_copy(
            src_ref=part,
            dst_ref=part,
            send_sem=send_sem.at[6],
            recv_sem=recv_sem.at[5, 1],
            device_id=partner,
            device_id_type=LOGICAL,
        ).start()
        return carry

    lax.fori_loop(0, groups, across, 0)
    sent(others, 5)
    sent(srecv_s.at[pl.ds(0, peers // 2)], 6)
    for which, ref in ((1, served_s), (2, rgrad_s)):
        sent(ref.at[pl.ds(block, recv_rows - block), :], which)
    for which, ref in ((0, frecv_s), (3, part_s), (4, halo_s), (7, hpart_s), (8, arecv_s)):
        sent(ref.at[pl.ds(1, peers - 1)], which)
    mates = srecv_s.at[pl.ds(0, peers // 2)]
    pltpu.make_async_copy(mates, mates, recv_sem.at[5, 1]).wait()
    everyone = srecv_s[...].astype(jnp.float32)
    node_terms = joined(everyone[:, :8])
    gself_ref[...] = node_terms[:width]
    gneigh_ref[...] = node_terms[width:]
    ghid_ref[...] = joined(everyone[:, 8:16])
    total = jnp.sum(everyone[:, block:], axis=0)
    total = total[:4] + total[4:]
    gbias_ref[...] = jnp.concatenate([total[0:1], total[1:2]], axis=1)
    gout_ref[...] = jnp.concatenate([total[2:3], total[3:4]], axis=1)
    result.wait()


def finish_kernel(count, *refs):
    taken, given, held = refs[:count], refs[count : 2 * count], refs[2 * count : 3 * count]
    in_sem, out_sem = refs[3 * count :]
    parts = []
    for a, h, b in zip(taken, held, given):
        rows = a.shape[0]
        step = TILE if rows > TILE else rows
        parts += [(a, h, b, pl.ds(r, step)) for r in range(0, rows, step)]
    moves = [
        (
            pltpu.make_async_copy(a.at[at, :], h.at[at, :], in_sem.at[n]),
            pltpu.make_async_copy(h.at[at, :], b.at[at, :], out_sem.at[n]),
        )
        for n, (a, h, b, at) in enumerate(parts)
    ]
    for fetch, _ in moves:
        fetch.start()
    for fetch, put in moves:
        fetch.wait()
        put.start()
    for _, put in moves:
        put.wait()


def finish(arrays):
    count = len(arrays)
    moves = sum(max(a.shape[0] // TILE, 1) for a in arrays)
    return pl.pallas_call(
        lambda *refs: finish_kernel(count, *refs),
        out_shape=tuple(jax.ShapeDtypeStruct(a.shape, a.dtype) for a in arrays),
        in_specs=[ANY] * count,
        out_specs=(ANY,) * count,
        scratch_shapes=[pltpu.VMEM(a.shape, a.dtype) for a in arrays]
        + [pltpu.SemaphoreType.DMA((moves,)), pltpu.SemaphoreType.DMA((moves,))],
        compiler_params=params(60),
        name="finish",
    )(*arrays)


def train_step(
    adj, features, degt, ask, halo, ends, pair_weight, labels, w_self, w_neigh, w_hidden,
    bias, w_out
):
    node_rows, width = features.shape
    table_rows = adj.shape[1]
    block, peers = ask.shape
    half = halo.shape[0]
    recv_rows = peers * block
    pairs = ends.shape[1]
    lines = 2 * half + 8
    bf16 = lambda *shape: pltpu.VMEM(shape, jnp.bfloat16)
    return pl.pallas_call(
        step_kernel,
        out_shape=(
            jax.ShapeDtypeStruct((1, pairs), jnp.float32),
            jax.ShapeDtypeStruct((node_rows, width), jnp.float32),
            jax.ShapeDtypeStruct((width, width), jnp.float32),
            jax.ShapeDtypeStruct((width, width), jnp.float32),
            jax.ShapeDtypeStruct((2 * width, width), jnp.float32),
            jax.ShapeDtypeStruct((1, width), jnp.float32),
            jax.ShapeDtypeStruct((1, width), jnp.float32),
        ),
        in_specs=[ANY, ANY] + [VMEM] * 6 + [ANY] * 3 + [VMEM] * 2,
        out_specs=(VMEM, ANY) + (VMEM,) * 5,
        scratch_shapes=[
            bf16(node_rows, table_rows),
            bf16(node_rows, width),
            bf16(width, width),
            bf16(width, width),
            bf16(2 * width, width),
            pltpu.VMEM((node_rows, width), jnp.float32),
            pltpu.VMEM((8, pairs), jnp.float32),
            pltpu.VMEM((8, node_rows), jnp.float32),
            pltpu.VMEM((peers * half, 1), jnp.float32),
            pltpu.VMEM((8, peers * half), jnp.float32),
            pltpu.VMEM((peers, LANES), jnp.float32),
            pltpu.VMEM((recv_rows, 1), jnp.float32),
            bf16(width, node_rows),
            bf16(width, node_rows),
            pltpu.VMEM((8, recv_rows), jnp.float32),
            pltpu.VMEM((peers, 1, LANES), jnp.int32),
            pltpu.VMEM((peers, 1, LANES), jnp.int32),
            bf16(peers, block, LANES),
            bf16(peers, block, LANES),
            bf16(peers * half, width),
            bf16(node_rows, width),
            bf16(node_rows, width),
            bf16(recv_rows, width),
            bf16(recv_rows, width),
            bf16(pairs, width),
            bf16(pairs, width),
            bf16(pairs, width),
            bf16(pairs, width),
            bf16(pairs, width),
            bf16(recv_rows, width),
            bf16(recv_rows, width),
            bf16(node_rows, width),
            bf16(width, node_rows),
            pltpu.VMEM((4 * width, width), jnp.float32),
            pltpu.VMEM((8, width), jnp.float32),
            pltpu.VMEM((pairs, 8), jnp.float32),
            bf16(peers, half, LANES),
            bf16(peers, half, LANES),
            bf16(peers, half, LANES),
            bf16(peers, half, LANES),
            bf16(peers, block, LANES),
            bf16(peers, block, LANES),
            bf16(peers * half, width),
            bf16(lines, LANES),
            bf16(peers, lines, LANES),
            pltpu.SemaphoreType.DMA((4,)),
            pltpu.SemaphoreType.DMA((node_rows // TILE,)),
            pltpu.SemaphoreType.DMA((9,)),
            pltpu.SemaphoreType.DMA((9, recv_rows // WIDE)),
        ],
        compiler_params=pltpu.CompilerParams(
            vmem_limit_bytes=62 * 2**20, collective_id=0, has_side_effects=True
        ),
        cost_estimate=cost(30_000_000_000, 24 * 2**20),
        name="train_step",
    )(
        adj, features, degt, ask, halo, ends, pair_weight, labels, w_self, w_neigh,
        w_hidden, bias, w_out,
    )


def per_device(
    features,
    edge_src,
    edge_dst,
    edge_count,
    halo_index,
    request_rows,
    pair_ends,
    labels,
    pair_weight,
    w_self,
    w_neigh,
    w_hidden,
    b_hidden,
    w_out,
):
    node_rows = features.shape[0]
    halo = halo_index[0].T
    adj, degt = adjacency(edge_src, edge_dst, edge_count, node_rows, node_rows + halo.size)
    logits, grad_features, grad_self, grad_neigh, grad_hidden, grad_bias, grad_out = train_step(
        adj, features, degt, request_rows[0].T, halo, pair_ends.T, pair_weight[None],
        labels[None], w_self, w_neigh, w_hidden, b_hidden[None], w_out[None]
    )
    grad_features, grad_self, grad_neigh, grad_hidden, grad_bias, grad_out, logits = finish(
        (grad_features, grad_self, grad_neigh, grad_hidden, grad_bias, grad_out, logits)
    )
    return (
        logits[0],
        grad_features,
        grad_self,
        grad_neigh,
        grad_hidden,
        grad_bias[0],
        grad_out[0],
    )


def solution(mesh):
    split = P(AXES)
    in_specs = (
        P(AXES, None),
        split,
        split,
        split,
        P(AXES, None, None),
        P(AXES, None, None),
        P(AXES, None),
        split,
        split,
        P(),
        P(),
        P(),
        P(),
        P(),
    )
    out_specs = (split, P(AXES, None), P(), P(), P(), P(), P())
    return jax.shard_map(
        per_device, mesh=mesh, in_specs=in_specs, out_specs=out_specs, check_vma=False
    )
```

```python
import jax
import jax.numpy as jnp
from jax import lax
from jax.experimental import pallas as pl
from jax.experimental.pallas import tpu as pltpu
from jax.sharding import PartitionSpec as P

AXES = ("dom", "grp")
LANES = 128
GROUP = 4
STRIDE = LANES // GROUP
TILE = 256
WIDE = 512
TALL = 1024
LOGICAL = pl.DeviceIdType.LOGICAL
CLASH = 1 << 20
VMEM = pl.BlockSpec(memory_space=pltpu.VMEM)
SMEM = pl.BlockSpec(memory_space=pltpu.SMEM)
ANY = pl.BlockSpec(memory_space=pl.ANY)


def dot32(a, b):
    return jnp.dot(a, b, preferred_element_type=jnp.float32)


def dot_nt(a, b):
    return lax.dot_general(a, b, (((1,), (1,)), ((), ())), preferred_element_type=jnp.float32)


def dot_tn(a, b):
    return lax.dot_general(a, b, (((0,), (0,)), ((), ())), preferred_element_type=jnp.float32)


def params(mib):
    return pltpu.CompilerParams(vmem_limit_bytes=mib * 2**20)


def cost(flops, size):
    return pl.CostEstimate(flops=flops, bytes_accessed=size, transcendentals=0)


def tile_of(i):
    return pl.ds(pl.multiple_of(i * TILE, TILE), TILE)


def pick(index, first, count, axis):
    shape = (index.shape[0], count) if axis == 1 else (count, index.shape[1])
    ids = lax.broadcasted_iota(jnp.int32, shape, axis) + first
    return jnp.where(index == ids, 1.0, 0.0).astype(jnp.bfloat16)


def edge_words(half, panels, count, src, dst):
    shape = src.shape
    lane = lax.broadcasted_iota(jnp.int32, shape, 1)
    live = lax.broadcasted_iota(jnp.int32, shape, 0) * LANES + lane < count
    upper = jnp.where(dst >= half, 1, 0)
    row = jnp.right_shift(src, 7) * half + dst - upper * half
    row = jnp.where(live, row, half * panels + lane // STRIDE)
    unit = jnp.where(live, jnp.bitwise_and(src, LANES - 1) + upper * LANES, 2 * LANES)
    clash = jnp.zeros(shape, jnp.int32)
    for k in range(1, GROUP // 2 + 1):
        clash = clash + jnp.where(row == pltpu.roll(row, k * STRIDE, 1), 1, 0)
    any_clash = jnp.max(clash.astype(jnp.float32), axis=1, keepdims=True) > 0.0
    return row + jnp.where(any_clash & (lane == 0), CLASH, 0), unit


def counts_kernel(
    half, panels, count_ref, src_ref, dst_ref, adj_ref, degt_ref, even, odd, unit_a, unit_b,
    row_v, row_ref, unit_ref, row_sem
):
    step = pl.program_id(0)
    chunks = unit_ref.shape[0]

    @pl.when(step == 0)
    def _():
        row_v[...], unit_ref[...] = edge_words(
            half, panels, count_ref[0], src_ref[...], dst_ref[...]
        )
        words = pltpu.make_async_copy(row_v, row_ref, row_sem)
        words.start()
        lane = lax.broadcasted_iota(jnp.int32, (LANES, LANES), 1)

        def clear(i, carry):
            even[tile_of(i), :] = jnp.zeros((TILE, LANES), jnp.int32)
            odd[tile_of(i), :] = jnp.zeros((TILE, LANES), jnp.int32)
            return carry

        lax.fori_loop(0, half * panels // TILE, clear, 0)
        words.wait()

        def units_of(c):
            c = jnp.minimum(c, chunks - 1)
            wide = jnp.transpose(jnp.broadcast_to(unit_ref[pl.ds(c, 1), :], (LANES, LANES)))
            return jnp.where(wide == lane, 1, jnp.where(wide == lane + LANES, 65536, 0))

        unit_a[...] = units_of(0)

        def chunk(c, units, later):
            places = row_ref.at[c]
            head = places[0]

            def load(s):
                words = odd if s % 2 else even
                at = [places[s + STRIDE * t] for t in range(GROUP)]
                new = [
                    words[pl.ds(a, 1), :] + units[pl.ds(s + STRIDE * t, 1), :]
                    for t, a in enumerate(at)
                ]
                return words, at, new

            def store(words, at, new):
                for a, n in zip(at, new):
                    words[pl.ds(a, 1), :] = n

            @pl.when(head < CLASH)
            def _():
                coming = units_of(c + 1)
                held = load(0)
                for s in range(1, STRIDE):
                    following = load(s)
                    store(*held)
                    held = following
                store(*held)
                later[...] = coming

            @pl.when(head >= CLASH)
            def _():
                later[...] = units_of(c + 1)
                for j in range(LANES):
                    words = odd if j % 2 else even
                    a = places[j]
                    if j == 0:
                        a = a - CLASH
                    words[pl.ds(a, 1), :] = words[pl.ds(a, 1), :] + units[pl.ds(j, 1), :]

        def two(i, carry):
            chunk(2 * i, unit_a, unit_b)
            chunk(2 * i + 1, unit_b, unit_a)
            return carry

        lax.fori_loop(0, chunks // 2, two, 0)

    first = step * TILE
    total = jnp.zeros((TILE, LANES), jnp.int32)
    for p in range(panels):
        part = pl.ds(pl.multiple_of(p * half + first, TILE), TILE)
        word = even[part, :] + odd[part, :]
        total = total + word
        cols = slice(p * LANES, (p + 1) * LANES)
        for h, count in enumerate((jnp.bitwise_and(word, 0xFFFF), jnp.right_shift(word, 16))):
            adj_ref[h, :, cols] = count.astype(jnp.float32).astype(jnp.bfloat16)
    for h, count in enumerate((jnp.bitwise_and(total, 0xFFFF), jnp.right_shift(total, 16))):
        degree = jnp.sum(count.astype(jnp.float32), axis=1, keepdims=True)
        wide = jnp.broadcast_to(jnp.maximum(degree, 1.0), (TILE, LANES))
        degt_ref[h] = jnp.transpose(wide)[:8]


def adjacency(edge_src, edge_dst, edge_count, node_rows, table_rows):
    half = node_rows // 2
    panels = table_rows // LANES
    chunks = edge_src.shape[0] // LANES
    grid_shape = (chunks, LANES)
    adj, degt = pl.pallas_call(
        lambda *refs: counts_kernel(half, panels, *refs),
        grid=(half // TILE,),
        out_shape=(
            jax.ShapeDtypeStruct((2, half, table_rows), jnp.bfloat16),
            jax.ShapeDtypeStruct((2, 8, half), jnp.float32),
        ),
        in_specs=[SMEM] + [pl.BlockSpec(grid_shape, lambda i: (0, 0))] * 2,
        out_specs=(
            pl.BlockSpec((2, TILE, table_rows), lambda i: (0, i, 0)),
            pl.BlockSpec((2, 8, TILE), lambda i: (0, 0, i)),
        ),
        scratch_shapes=[
            pltpu.VMEM((half * panels + GROUP, LANES), jnp.int32),
            pltpu.VMEM((half * panels + GROUP, LANES), jnp.int32),
            pltpu.VMEM((LANES, LANES), jnp.int32),
            pltpu.VMEM((LANES, LANES), jnp.int32),
            pltpu.VMEM(grid_shape, jnp.int32),
            pltpu.SMEM(grid_shape, jnp.int32),
            pltpu.VMEM(grid_shape, jnp.int32),
            pltpu.SemaphoreType.DMA,
        ],
        compiler_params=params(60),
        cost_estimate=cost(60_000_000, 16 * 2**20),
        name="counts",
    )(edge_count, edge_src.reshape(grid_shape), edge_dst.reshape(grid_shape))
    return adj.reshape(node_rows, table_rows), degt


def step_kernel(
    adj_ref,
    feat_in,
    degt_ref,
    ask_ref,
    halo_ref,
    ends_ref,
    weight_ref,
    label_ref,
    ws_in,
    wn_in,
    wh_in,
    bias_ref,
    wo_ref,
    logit_ref,
    gfeat_ref,
    gself_ref,
    gneigh_ref,
    ghid_ref,
    gbias_ref,
    gout_ref,
    adj_s,
    feat_ref,
    ws_ref,
    wn_ref,
    wh_ref,
    gfeat_s,
    pair_s,
    deg_s,
    hcol_s,
    hrow_s,
    wcol_s,
    wfull_s,
    feat_t,
    agg_t,
    wrow_s,
    ask_s,
    arecv_s,
    first_s,
    frecv_s,
    arr_s,
    emb_s,
    agg_s,
    served_s,
    recv_s,
    left_s,
    right_s,
    delta_s,
    pgl_s,
    pgr_s,
    rgrad_s,
    back_s,
    gradb_s,
    gt_s,
    gw_s,
    small_s,
    cols_s,
    part_s,
    precv_s,
    hpart_s,
    hprecv_s,
    halo_s,
    hrecv_s,
    hrows_s,
    share_s,
    srecv_s,
    in_sem,
    adj_sem,
    send_sem,
    recv_sem,
):
    node_rows, width = feat_ref.shape
    block, peers = ask_ref.shape
    half = halo_ref.shape[0]
    recv_rows = peers * block
    pairs = ends_ref.shape[1]
    grp = lax.axis_size("grp")
    me = lax.axis_index("dom") * grp + lax.axis_index("grp")
    burst = WIDE // block
    bursts = peers // burst
    hburst = burst // 2
    tiles = node_rows // TILE
    barrier = pltpu.get_barrier_semaphore()

    def load_adj(i):
        return pltpu.make_async_copy(
            adj_ref.at[tile_of(i), :], adj_s.at[tile_of(i), :], adj_sem.at[i]
        )

    loads = [
        pltpu.make_async_copy(a, b, in_sem.at[n])
        for n, (a, b) in enumerate(
            ((feat_in, feat_ref), (ws_in, ws_ref), (wn_in, wn_ref), (wh_in, wh_ref))
        )
    ]
    for load in loads:
        load.start()

    def fetch(i, carry):
        load_adj(i).start()
        return carry


    def greet(i, carry):
        for u in range(7):
            pl.semaphore_signal(
                barrier,
                inc=1,
                device_id=jnp.bitwise_and(me + (i * 7 + u + 1), peers - 1),
                device_id_type=LOGICAL,
            )
        return carry

    pl.semaphore_signal(
        barrier,
        inc=1,
        device_id=jnp.bitwise_and(me + (peers - 1), peers - 1),
        device_id_type=LOGICAL,
    )
    lax.fori_loop(0, (peers - 2) // 7, greet, 0)
    lax.fori_loop(0, tiles, fetch, 0)
    for load in loads:
        load.wait()

    def rows_of(p):
        return pl.ds(pl.multiple_of(p * block, block), block)

    def burst_at(k):
        return lax.rem(me // burst + k, bursts)

    def ship(k, source, target, which):
        low = jnp.bitwise_and(me, burst - 1)
        first = burst_at(k) * burst

        def one(i):
            p = first + jnp.bitwise_and(low + i, burst - 1)
            pltpu.make_async_remote_copy(
                src_ref=source(p),
                dst_ref=target,
                send_sem=send_sem.at[which],
                recv_sem=recv_sem.at[which, k],
                device_id=p,
                device_id_type=LOGICAL,
            ).start()

        @pl.when(k > 0)
        def _():
            one(0)

        for i in range(1, burst):
            one(i)

    def arrived(k, ref, unit, which):
        first = pl.ds(unit, (burst - 1) * unit) if unit else pl.ds(1, burst - 1)
        rest = pl.ds(0, burst * unit) if unit else pl.ds(0, burst)
        if isinstance(k, int) and k == 0:
            part = ref.at[first]
        else:
            part = ref.at[rest]
        pltpu.make_async_copy(part, part, recv_sem.at[which, k]).wait()

    def sent(part, which):
        pltpu.make_async_copy(part, part, send_sem.at[which]).wait()

    def source_at(k):
        return lax.rem(me // burst - k + bursts, bursts)

    def produce(fill, source, target, which):
        fill(0)

        def middle(k, carry):
            fill(k)
            ship(k - 1, source, target, which)
            return carry

        lax.fori_loop(1, bursts, middle, 0)

    def halves(rows):
        wide = rows.reshape(burst, half, width)
        return jnp.concatenate([wide[:, :, :LANES], wide[:, :, LANES:]], axis=1)

    def whole(blocks):
        wide = blocks.astype(jnp.float32)
        return jnp.concatenate([wide[:, :half], wide[:, half : 2 * half]], axis=2)

    def spread(table, depth):
        shape = (table.shape[0], depth, table.shape[1])
        keep = lax.broadcasted_iota(jnp.int32, shape, 1) == lax.broadcasted_iota(
            jnp.int32, shape, 2
        )
        wide = jnp.broadcast_to(table[:, None, :], shape)
        one = jnp.sum(jnp.where(keep, wide, 0.0), axis=2, keepdims=True)
        return one.reshape(shape[0] * depth, 1)

    def as_row(col):
        return jnp.transpose(jnp.broadcast_to(col, (col.shape[0], LANES)))[:8]

    deg_s[...] = jnp.concatenate([degt_ref[0], degt_ref[1]], axis=1)
    hcol_s[...] = spread(jnp.transpose(halo_ref[...].astype(jnp.float32)), half)
    ask_table = jnp.transpose(
        jnp.concatenate(
            [ask_ref[...].astype(jnp.float32), jnp.zeros((LANES - block, peers), jnp.float32)],
            axis=0,
        )
    )
    ask_s[...] = ask_table.astype(jnp.int32).reshape(peers, 1, LANES)

    def outgoing(t, carry):
        hot = pick(hcol_s[tile_of(t), :].astype(jnp.int32), 0, node_rows, 1)
        part = pl.ds(pl.multiple_of(t * burst, burst), burst)
        first_s[part] = halves(dot32(hot, feat_ref[...])).astype(jnp.bfloat16)
        return carry

    lax.fori_loop(0, bursts, outgoing, 0)

    def local_sums(i, carry):
        load_adj(i).wait()
        at = tile_of(i)
        gfeat_s[at, :] = dot32(adj_s[at, :node_rows], feat_ref[...])
        return carry

    lax.fori_loop(0, tiles, local_sums, 0)
    pl.semaphore_wait(barrier, peers - 1)
    first_of = lambda p: first_s.at[p]
    for k in range(bursts):
        ship(k, first_of, frecv_s.at[me], 0)
    ask_of = lambda p: ask_s.at[p]
    for k in range(bursts):
        ship(k, ask_of, arecv_s.at[me], 8)
    frecv_s[me] = first_s[me]
    arecv_s[me] = ask_s[me]
    pair_s[...] = jnp.concatenate(
        [
            ends_ref[...].astype(jnp.float32),
            weight_ref[...],
            label_ref[...].astype(jnp.float32),
            jnp.zeros((4, pairs), jnp.float32),
        ],
        axis=0,
    )

    def columns(i, carry):
        at = pl.ds(pl.multiple_of(i * WIDE, WIDE), WIDE)
        cols_s[at, :] = jnp.transpose(pair_s[:, at])
        return carry

    lax.fori_loop(0, pairs // WIDE, columns, 0)
    hrow_s[...] = as_row(hcol_s[...])
    for k in range(bursts):
        arrived(k, frecv_s, 0, 0)
        arrived(k, arecv_s, 0, 8)
    arr_s[...] = whole(frecv_s[...]).reshape(peers * half, width).astype(jnp.bfloat16)
    wcol_s[0:peers, :] = jnp.max(arecv_s[...], axis=1).astype(jnp.float32)

    def ship_half(n, source, target, which):
        k = n // 2
        low = jnp.bitwise_and(me, hburst - 1)
        first = half_at(n)

        def one(i):
            p = first + jnp.bitwise_and(low + i, hburst - 1)
            pltpu.make_async_remote_copy(
                src_ref=source(p),
                dst_ref=target,
                send_sem=send_sem.at[which],
                recv_sem=recv_sem.at[which, k],
                device_id=p,
                device_id_type=LOGICAL,
            ).start()

        @pl.when(n > 0)
        def _():
            one(0)

        for i in range(1, hburst):
            one(i)

    def produce_halves(fill, source, target, which):
        fill(0)

        def middle(n, carry):
            fill(n)
            ship_half(n - 1, source, target, which)
            return carry

        lax.fori_loop(1, 2 * bursts, middle, 0)

    def encode(i, carry):
        at = pl.ds(pl.multiple_of(i * TALL, TALL), TALL)
        sums = gfeat_s[at, :] + dot32(adj_s[at, node_rows:], arr_s[...])
        degree = jnp.transpose(deg_s[:, at])[:, :1]
        mean = (sums / degree).astype(jnp.bfloat16)
        agg_s[at, :] = mean
        emb_s[at, :] = (dot32(feat_ref[at, :], ws_ref[...]) + dot32(mean, wn_ref[...])).astype(
            jnp.bfloat16
        )
        return carry

    lax.fori_loop(0, node_rows // TALL, encode, 0)

    def half_at(n):
        k, sub = n // 2, lax.rem(n, 2)
        low = jnp.bitwise_and(me, burst - 1) // hburst
        return burst_at(k) * burst + jnp.bitwise_and(low + sub, 1) * hburst

    def serve(n):
        p = half_at(n)
        at = pl.ds(pl.multiple_of(p * block, TILE), TILE)
        asked = spread(wcol_s[pl.ds(pl.multiple_of(p, hburst), hburst), :], block)
        wfull_s[at, :] = asked
        hot = pick(asked.astype(jnp.int32), 0, node_rows, 1)
        served_s[at, :] = dot32(hot, emb_s[...]).astype(jnp.bfloat16)

    served_of = lambda p: served_s.at[rows_of(p), :]
    produce_halves(serve, served_of, recv_s.at[rows_of(me), :], 1)
    recv_s[rows_of(me), :] = served_s[rows_of(me), :]
    small_s[...] = jnp.zeros(small_s.shape, jnp.float32)
    ship_half(2 * bursts - 1, served_of, recv_s.at[rows_of(me), :], 1)
    feat_t[...] = jnp.transpose(feat_ref[...])
    agg_t[...] = jnp.transpose(agg_s[...])

    def ask_rows(i, carry):
        at = pl.ds(pl.multiple_of(i * WIDE, WIDE), WIDE)
        wrow_s[:, at] = as_row(wfull_s[at, :])
        return carry

    lax.fori_loop(0, recv_rows // WIDE, ask_rows, 0)

    for k in range(bursts):
        arrived(k, recv_s, block, 1)
        b = source_at(k)
        here = pl.ds(pl.multiple_of(b * WIDE, WIDE), WIDE)

        def gather(i, carry):
            at = pl.ds(pl.multiple_of(i * TALL, TALL), TALL)
            for side, rows in ((0, left_s), (1, right_s)):
                ends = cols_s[at, side : side + 1].astype(jnp.int32)
                found = dot32(pick(ends, b * WIDE, WIDE, 1), recv_s[here, :]).astype(
                    jnp.bfloat16
                )
                rows[at, :] = found if k == 0 else rows[at, :] + found
            return carry

        lax.fori_loop(0, pairs // TALL, gather, 0)

    def forward(i, carry):
        at = pl.ds(pl.multiple_of(i * TALL, TALL), TALL)
        cols = cols_s[at, :]
        left = left_s[at, :]
        right = right_s[at, :]
        pre = dot32(left, wh_ref[:width, :]) + dot32(right, wh_ref[width:, :]) + bias_ref[...]
        hidden = jnp.maximum(pre, 0.0)
        logit = jnp.sum(hidden * wo_ref[...], axis=1, keepdims=True)
        logit_ref[:, at] = jnp.transpose(jnp.broadcast_to(logit, (TALL, LANES)))[:1]
        slope = cols[:, 2:3] * (jax.nn.sigmoid(logit) - cols[:, 3:4])
        delta = jnp.where(pre > 0, slope * wo_ref[...], 0.0)
        small_s[0:1, :] += jnp.sum(delta, axis=0, keepdims=True)
        small_s[1:2, :] += jnp.sum(slope * hidden, axis=0, keepdims=True)
        delta_b = delta.astype(jnp.bfloat16)
        delta_s[at, :] = delta_b
        pgl_s[at, :] = dot_nt(delta_b, wh_ref[:width, :]).astype(jnp.bfloat16)
        pgr_s[at, :] = dot_nt(delta_b, wh_ref[width:, :]).astype(jnp.bfloat16)
        return carry

    lax.fori_loop(0, pairs // TALL, forward, 0)
    ends_row = ends_ref[...]

    def collect(n):
        first = half_at(n) * block
        total = dot32(pick(ends_row[0:1, :], first, TILE, 0), pgl_s[...]) + dot32(
            pick(ends_row[1:2, :], first, TILE, 0), pgr_s[...]
        )
        rgrad_s[pl.ds(pl.multiple_of(first, TILE), TILE), :] = total.astype(jnp.bfloat16)

    rgrad_of = lambda p: rgrad_s.at[rows_of(p), :]
    produce_halves(collect, rgrad_of, back_s.at[rows_of(me), :], 2)
    back_s[rows_of(me), :] = rgrad_s[rows_of(me), :]
    ship_half(2 * bursts - 1, rgrad_of, back_s.at[rows_of(me), :], 2)
    gw_s[2 * width : 3 * width, :] = dot_tn(left_s[...], delta_s[...])
    gw_s[3 * width :, :] = dot_tn(right_s[...], delta_s[...])

    def eighths(rows):
        wide = rows.reshape(burst // 2, 8, width)
        both = jnp.concatenate([wide[:, None, :, :LANES], wide[:, None, :, LANES:]], axis=1)
        return both.reshape(burst, 8, LANES).astype(jnp.bfloat16)

    def joined(blocks):
        wide = blocks.reshape(peers // 2, 2, 8, LANES)
        return jnp.concatenate([wide[:, 0], wide[:, 1]], axis=2).reshape(2 * width, width)

    def eighth_of(t):
        return pl.ds(pl.multiple_of(t * LANES, LANES), LANES)

    for k in range(bursts):
        t = burst_at(k)
        hpart_s[pl.ds(t * burst, burst)] = eighths(gw_s[eighth_of(t + bursts), :])
    hpart_of = lambda p: hpart_s.at[p]
    hprecv_s[me] = hpart_s[me]
    for k in range(bursts):
        ship(k, hpart_of, hprecv_s.at[me], 7)
    for k in range(bursts):
        arrived(k, back_s, block, 2)
        b = source_at(k)
        here = pl.ds(pl.multiple_of(b * WIDE, WIDE), WIDE)

        def put(i, carry):
            at = pl.ds(pl.multiple_of(i * TALL, TALL), TALL)
            found = dot32(pick(wrow_s[0:1, here].astype(jnp.int32), i * TALL, TALL, 0), back_s[here, :])
            gfeat_s[at, :] = found if k == 0 else gfeat_s[at, :] + found
            return carry

        lax.fori_loop(0, node_rows // TALL, put, 0)
    gradb_s[...] = gfeat_s[...].astype(jnp.bfloat16)
    gw_s[:width, :] = dot32(feat_t[...], gradb_s[...])
    gw_s[width : 2 * width, :] = dot32(agg_t[...], gradb_s[...])
    def weight_terms(k):
        t = burst_at(k)
        part_s[pl.ds(t * burst, burst)] = eighths(gw_s[eighth_of(t), :])

    part_of = lambda p: part_s.at[p]
    produce(weight_terms, part_of, precv_s.at[me], 3)
    precv_s[me] = part_s[me]
    gt_s[...] = (dot_nt(wn_ref[...], gradb_s[...]) / deg_s[0:1, :]).astype(jnp.bfloat16)
    ship(bursts - 1, part_of, precv_s.at[me], 3)

    def table_grad(first):
        cols = pl.ds(pl.multiple_of(first, TILE), TILE)
        return jnp.transpose(dot32(gt_s[...], adj_s[:, cols]))

    def return_halo(k):
        t = burst_at(k)
        halo_s[pl.ds(t * burst, burst)] = halves(
            table_grad(node_rows + t * TILE)
        ).astype(jnp.bfloat16)

    halo_of = lambda p: halo_s.at[p]
    produce(return_halo, halo_of, hrecv_s.at[me], 4)
    hrecv_s[me] = halo_s[me]

    def direct(i, carry):
        at = tile_of(i)
        gfeat_s[at, :] = dot_nt(gradb_s[at, :], ws_ref[...]) + table_grad(i * TILE)
        return carry

    direct(0, 0)
    ship(bursts - 1, halo_of, hrecv_s.at[me], 4)
    for k in range(bursts):
        arrived(k, precv_s, 0, 3)
        arrived(k, hprecv_s, 0, 7)
    own = jnp.concatenate(
        [
            jnp.sum(precv_s[...].astype(jnp.float32), axis=0),
            jnp.sum(hprecv_s[...].astype(jnp.float32), axis=0),
        ],
        axis=0,
    )
    small = small_s[...]
    small_hi = small.astype(jnp.bfloat16).astype(jnp.float32)
    small_lo = small - small_hi
    lines = [
        part[r : r + 1, c : c + LANES]
        for part in (small_hi, small_lo)
        for r in range(2)
        for c in (0, LANES)
    ]
    share_s[...] = jnp.concatenate([own] + lines, axis=0).astype(jnp.bfloat16)
    direct(1, 0)

    core = lax.rem(me // grp, 2)
    partner = me + (1 - 2 * core) * grp
    groups = peers // (2 * grp)

    def share(i, carry):
        own_q = (me // (2 * grp)) * grp + lax.rem(me, grp)
        for u in range(7):
            q = jnp.bitwise_and(own_q + (i * 7 + u + 1) * 27, peers // 2 - 1)
            pltpu.make_async_remote_copy(
                src_ref=share_s,
                dst_ref=srecv_s.at[me],
                send_sem=send_sem.at[5],
                recv_sem=recv_sem.at[5, 0],
                device_id=q + (q // grp) * grp + core * grp,
                device_id_type=LOGICAL,
            ).start()
        return carry

    lax.fori_loop(0, (peers // 2 - 1) // 7, share, 0)
    srecv_s[me] = share_s[...]
    lax.fori_loop(2, tiles, direct, 0)
    for k in range(bursts):
        arrived(k, hrecv_s, 0, 4)
    hrows_s[...] = whole(hrecv_s[...]).reshape(peers * half, width).astype(jnp.bfloat16)

    def place(i, carry):
        at = pl.ds(pl.multiple_of(i * TALL, TALL), TALL)
        hot = pick(hrow_s[0:1, :].astype(jnp.int32), i * TALL, TALL, 0)
        gfeat_s[at, :] += dot32(hot, hrows_s[...])
        return carry

    lax.fori_loop(0, node_rows // TALL, place, 0)
    result = pltpu.make_async_copy(gfeat_s, gfeat_ref, adj_sem.at[0])
    result.start()
    others = srecv_s.at[pl.ds(1, peers // 2 - 1)]
    pltpu.make_async_copy(others, others, recv_sem.at[5, 0]).wait()

    def across(i, carry):
        part = srecv_s.at[pl.ds(i * (2 * grp) + core * grp, grp)]
        pltpu.make_async_remote_copy(
            src_ref=part,
            dst_ref=part,
            send_sem=send_sem.at[6],
            recv_sem=recv_sem.at[5, 1],
            device_id=partner,
            device_id_type=LOGICAL,
        ).start()
        return carry

    lax.fori_loop(0, groups, across, 0)
    sent(others, 5)
    sent(srecv_s.at[pl.ds(0, peers // 2)], 6)
    for which, ref in ((1, served_s), (2, rgrad_s)):
        sent(ref.at[pl.ds(block, recv_rows - block), :], which)
    for which, ref in ((0, frecv_s), (3, part_s), (4, halo_s), (7, hpart_s), (8, arecv_s)):
        sent(ref.at[pl.ds(1, peers - 1)], which)
    mates = srecv_s.at[pl.ds(0, peers // 2)]
    pltpu.make_async_copy(mates, mates, recv_sem.at[5, 1]).wait()
    everyone = srecv_s[...].astype(jnp.float32)
    node_terms = joined(everyone[:, :8])
    gself_ref[...] = node_terms[:width]
    gneigh_ref[...] = node_terms[width:]
    ghid_ref[...] = joined(everyone[:, 8:16])
    total = jnp.sum(everyone[:, block:], axis=0)
    total = total[:4] + total[4:]
    gbias_ref[...] = jnp.concatenate([total[0:1], total[1:2]], axis=1)
    gout_ref[...] = jnp.concatenate([total[2:3], total[3:4]], axis=1)
    result.wait()


def finish_kernel(count, *refs):
    taken, given, held = refs[:count], refs[count : 2 * count], refs[2 * count : 3 * count]
    in_sem, out_sem = refs[3 * count :]
    parts = []
    for a, h, b in zip(taken, held, given):
        rows = a.shape[0]
        step = TILE if rows > TILE else rows
        parts += [(a, h, b, pl.ds(r, step)) for r in range(0, rows, step)]
    moves = [
        (
            pltpu.make_async_copy(a.at[at, :], h.at[at, :], in_sem.at[n]),
            pltpu.make_async_copy(h.at[at, :], b.at[at, :], out_sem.at[n]),
        )
        for n, (a, h, b, at) in enumerate(parts)
    ]
    for fetch, _ in moves:
        fetch.start()
    for fetch, put in moves:
        fetch.wait()
        put.start()
    for _, put in moves:
        put.wait()


def finish(arrays):
    count = len(arrays)
    moves = sum(max(a.shape[0] // TILE, 1) for a in arrays)
    return pl.pallas_call(
        lambda *refs: finish_kernel(count, *refs),
        out_shape=tuple(jax.ShapeDtypeStruct(a.shape, a.dtype) for a in arrays),
        in_specs=[ANY] * count,
        out_specs=(ANY,) * count,
        scratch_shapes=[pltpu.VMEM(a.shape, a.dtype) for a in arrays]
        + [pltpu.SemaphoreType.DMA((moves,)), pltpu.SemaphoreType.DMA((moves,))],
        compiler_params=params(60),
        name="finish",
    )(*arrays)


def train_step(
    adj, features, degt, ask, halo, ends, pair_weight, labels, w_self, w_neigh, w_hidden,
    bias, w_out
):
    node_rows, width = features.shape
    table_rows = adj.shape[1]
    block, peers = ask.shape
    half = halo.shape[0]
    recv_rows = peers * block
    pairs = ends.shape[1]
    lines = 2 * half + 8
    bf16 = lambda *shape: pltpu.VMEM(shape, jnp.bfloat16)
    return pl.pallas_call(
        step_kernel,
        out_shape=(
            jax.ShapeDtypeStruct((1, pairs), jnp.float32),
            jax.ShapeDtypeStruct((node_rows, width), jnp.float32),
            jax.ShapeDtypeStruct((width, width), jnp.float32),
            jax.ShapeDtypeStruct((width, width), jnp.float32),
            jax.ShapeDtypeStruct((2 * width, width), jnp.float32),
            jax.ShapeDtypeStruct((1, width), jnp.float32),
            jax.ShapeDtypeStruct((1, width), jnp.float32),
        ),
        in_specs=[ANY, ANY] + [VMEM] * 6 + [ANY] * 3 + [VMEM] * 2,
        out_specs=(VMEM, ANY) + (VMEM,) * 5,
        scratch_shapes=[
            bf16(node_rows, table_rows),
            bf16(node_rows, width),
            bf16(width, width),
            bf16(width, width),
            bf16(2 * width, width),
            pltpu.VMEM((node_rows, width), jnp.float32),
            pltpu.VMEM((8, pairs), jnp.float32),
            pltpu.VMEM((8, node_rows), jnp.float32),
            pltpu.VMEM((peers * half, 1), jnp.float32),
            pltpu.VMEM((8, peers * half), jnp.float32),
            pltpu.VMEM((peers, LANES), jnp.float32),
            pltpu.VMEM((recv_rows, 1), jnp.float32),
            bf16(width, node_rows),
            bf16(width, node_rows),
            pltpu.VMEM((8, recv_rows), jnp.float32),
            pltpu.VMEM((peers, 1, LANES), jnp.int32),
            pltpu.VMEM((peers, 1, LANES), jnp.int32),
            bf16(peers, block, LANES),
            bf16(peers, block, LANES),
            bf16(peers * half, width),
            bf16(node_rows, width),
            bf16(node_rows, width),
            bf16(recv_rows, width),
            bf16(recv_rows, width),
            bf16(pairs, width),
            bf16(pairs, width),
            bf16(pairs, width),
            bf16(pairs, width),
            bf16(pairs, width),
            bf16(recv_rows, width),
            bf16(recv_rows, width),
            bf16(node_rows, width),
            bf16(width, node_rows),
            pltpu.VMEM((4 * width, width), jnp.float32),
            pltpu.VMEM((8, width), jnp.float32),
            pltpu.VMEM((pairs, 8), jnp.float32),
            bf16(peers, half, LANES),
            bf16(peers, half, LANES),
            bf16(peers, half, LANES),
            bf16(peers, half, LANES),
            bf16(peers, block, LANES),
            bf16(peers, block, LANES),
            bf16(peers * half, width),
            bf16(lines, LANES),
            bf16(peers, lines, LANES),
            pltpu.SemaphoreType.DMA((4,)),
            pltpu.SemaphoreType.DMA((node_rows // TILE,)),
            pltpu.SemaphoreType.DMA((9,)),
            pltpu.SemaphoreType.DMA((9, recv_rows // WIDE)),
        ],
        compiler_params=pltpu.CompilerParams(
            vmem_limit_bytes=62 * 2**20, collective_id=0, has_side_effects=True
        ),
        cost_estimate=cost(30_000_000_000, 24 * 2**20),
        name="train_step",
    )(
        adj, features, degt, ask, halo, ends, pair_weight, labels, w_self, w_neigh,
        w_hidden, bias, w_out,
    )


def per_device(
    features,
    edge_src,
    edge_dst,
    edge_count,
    halo_index,
    request_rows,
    pair_ends,
    labels,
    pair_weight,
    w_self,
    w_neigh,
    w_hidden,
    b_hidden,
    w_out,
):
    node_rows = features.shape[0]
    halo = halo_index[0].T
    adj, degt = adjacency(edge_src, edge_dst, edge_count, node_rows, node_rows + halo.size)
    logits, grad_features, grad_self, grad_neigh, grad_hidden, grad_bias, grad_out = train_step(
        adj, features, degt, request_rows[0].T, halo, pair_ends.T, pair_weight[None],
        labels[None], w_self, w_neigh, w_hidden, b_hidden[None], w_out[None]
    )
    grad_features, grad_self, grad_neigh, grad_hidden, grad_bias, grad_out, logits = finish(
        (grad_features, grad_self, grad_neigh, grad_hidden, grad_bias, grad_out, logits)
    )
    return (
        logits[0],
        grad_features,
        grad_self,
        grad_neigh,
        grad_hidden,
        grad_bias[0],
        grad_out[0],
    )


def solution(mesh):
    split = P(AXES)
    in_specs = (
        P(AXES, None),
        split,
        split,
        split,
        P(AXES, None, None),
        P(AXES, None, None),
        P(AXES, None),
        split,
        split,
        P(),
        P(),
        P(),
        P(),
        P(),
    )
    out_specs = (split, P(AXES, None), P(), P(), P(), P(), P())
    return jax.shard_map(
        per_device, mesh=mesh, in_specs=in_specs, out_specs=out_specs, check_vma=False
    )
```

```python
import jax
import jax.numpy as jnp
from jax import lax
from jax.experimental import pallas as pl
from jax.experimental.pallas import tpu as pltpu
from jax.sharding import PartitionSpec as P

AXES = ("dom", "grp")
LANES = 128
GROUP = 4
STRIDE = LANES // GROUP
TILE = 256
STRIP = 128
WIDE = 512
TALL = 1024
LOGICAL = pl.DeviceIdType.LOGICAL
CLASH = 1 << 20
VMEM = pl.BlockSpec(memory_space=pltpu.VMEM)
SMEM = pl.BlockSpec(memory_space=pltpu.SMEM)
ANY = pl.BlockSpec(memory_space=pl.ANY)


def dot32(a, b):
    return jnp.dot(a, b, preferred_element_type=jnp.float32)


def dot_nt(a, b):
    return lax.dot_general(a, b, (((1,), (1,)), ((), ())), preferred_element_type=jnp.float32)


def dot_tn(a, b):
    return lax.dot_general(a, b, (((0,), (0,)), ((), ())), preferred_element_type=jnp.float32)


def params(mib):
    return pltpu.CompilerParams(vmem_limit_bytes=mib * 2**20)


def cost(flops, size):
    return pl.CostEstimate(flops=flops, bytes_accessed=size, transcendentals=0)


def tile_of(i):
    return pl.ds(pl.multiple_of(i * TILE, TILE), TILE)


def pick(index, first, count, axis):
    shape = (index.shape[0], count) if axis == 1 else (count, index.shape[1])
    ids = lax.broadcasted_iota(jnp.int32, shape, axis) + first
    return jnp.where(index == ids, 1.0, 0.0).astype(jnp.bfloat16)


def edge_words(half, panels, count, src, dst):
    shape = src.shape
    lane = lax.broadcasted_iota(jnp.int32, shape, 1)
    live = lax.broadcasted_iota(jnp.int32, shape, 0) * LANES + lane < count
    upper = jnp.where(dst >= half, 1, 0)
    row = jnp.right_shift(src, 7) * half + dst - upper * half
    row = jnp.where(live, row, half * panels + lane // STRIDE)
    unit = jnp.where(live, jnp.bitwise_and(src, LANES - 1) + upper * LANES, 2 * LANES)
    clash = jnp.zeros(shape, jnp.int32)
    for k in range(1, GROUP // 2 + 1):
        clash = clash + jnp.where(row == pltpu.roll(row, k * STRIDE, 1), 1, 0)
    any_clash = jnp.max(clash.astype(jnp.float32), axis=1, keepdims=True) > 0.0
    return row + jnp.where(any_clash & (lane == 0), CLASH, 0), unit


def counts_kernel(
    half, panels, count_ref, src_ref, dst_ref, adj_ref, degt_ref, even, odd, unit_a, unit_b,
    row_v, row_ref, unit_ref, row_sem
):
    step = pl.program_id(0)
    chunks = unit_ref.shape[0]

    @pl.when(step == 0)
    def _():
        row_v[...], unit_ref[...] = edge_words(
            half, panels, count_ref[0], src_ref[...], dst_ref[...]
        )
        words = pltpu.make_async_copy(row_v, row_ref, row_sem)
        words.start()
        lane = lax.broadcasted_iota(jnp.int32, (LANES, LANES), 1)

        def clear(i, carry):
            even[tile_of(i), :] = jnp.zeros((TILE, LANES), jnp.int32)
            odd[tile_of(i), :] = jnp.zeros((TILE, LANES), jnp.int32)
            return carry

        lax.fori_loop(0, half * panels // TILE, clear, 0)
        words.wait()

        def units_of(c):
            c = jnp.minimum(c, chunks - 1)
            wide = jnp.transpose(jnp.broadcast_to(unit_ref[pl.ds(c, 1), :], (LANES, LANES)))
            return jnp.where(wide == lane, 1, jnp.where(wide == lane + LANES, 65536, 0))

        unit_a[...] = units_of(0)

        def chunk(c, units, later):
            places = row_ref.at[c]
            head = places[0]

            def load(s):
                words = odd if s % 2 else even
                at = [places[s + STRIDE * t] for t in range(GROUP)]
                new = [
                    words[pl.ds(a, 1), :] + units[pl.ds(s + STRIDE * t, 1), :]
                    for t, a in enumerate(at)
                ]
                return words, at, new

            def store(words, at, new):
                for a, n in zip(at, new):
                    words[pl.ds(a, 1), :] = n

            @pl.when(head < CLASH)
            def _():
                coming = units_of(c + 1)
                held = load(0)
                for s in range(1, STRIDE):
                    following = load(s)
                    store(*held)
                    held = following
                store(*held)
                later[...] = coming

            @pl.when(head >= CLASH)
            def _():
                later[...] = units_of(c + 1)
                for j in range(LANES):
                    words = odd if j % 2 else even
                    a = places[j]
                    if j == 0:
                        a = a - CLASH
                    words[pl.ds(a, 1), :] = words[pl.ds(a, 1), :] + units[pl.ds(j, 1), :]

        def two(i, carry):
            chunk(2 * i, unit_a, unit_b)
            chunk(2 * i + 1, unit_b, unit_a)
            return carry

        lax.fori_loop(0, chunks // 2, two, 0)

    first = step * STRIP
    total = jnp.zeros((STRIP, LANES), jnp.int32)
    for p in range(panels):
        part = pl.ds(pl.multiple_of(p * half + first, STRIP), STRIP)
        word = even[part, :] + odd[part, :]
        total = total + word
        cols = slice(p * LANES, (p + 1) * LANES)
        for h, count in enumerate((jnp.bitwise_and(word, 0xFFFF), jnp.right_shift(word, 16))):
            adj_ref[h, :, cols] = count.astype(jnp.float32).astype(jnp.bfloat16)
    for h, count in enumerate((jnp.bitwise_and(total, 0xFFFF), jnp.right_shift(total, 16))):
        degree = jnp.sum(count.astype(jnp.float32), axis=1, keepdims=True)
        wide = jnp.broadcast_to(jnp.maximum(degree, 1.0), (STRIP, LANES))
        degt_ref[h] = jnp.transpose(wide)[:8]


def adjacency(edge_src, edge_dst, edge_count, node_rows, table_rows):
    half = node_rows // 2
    panels = table_rows // LANES
    chunks = edge_src.shape[0] // LANES
    grid_shape = (chunks, LANES)
    adj, degt = pl.pallas_call(
        lambda *refs: counts_kernel(half, panels, *refs),
        grid=(half // STRIP,),
        out_shape=(
            jax.ShapeDtypeStruct((2, half, table_rows), jnp.bfloat16),
            jax.ShapeDtypeStruct((2, 8, half), jnp.float32),
        ),
        in_specs=[SMEM] + [pl.BlockSpec(grid_shape, lambda i: (0, 0))] * 2,
        out_specs=(
            pl.BlockSpec((2, STRIP, table_rows), lambda i: (0, i, 0)),
            pl.BlockSpec((2, 8, STRIP), lambda i: (0, 0, i)),
        ),
        scratch_shapes=[
            pltpu.VMEM((half * panels + GROUP, LANES), jnp.int32),
            pltpu.VMEM((half * panels + GROUP, LANES), jnp.int32),
            pltpu.VMEM((LANES, LANES), jnp.int32),
            pltpu.VMEM((LANES, LANES), jnp.int32),
            pltpu.VMEM(grid_shape, jnp.int32),
            pltpu.SMEM(grid_shape, jnp.int32),
            pltpu.VMEM(grid_shape, jnp.int32),
            pltpu.SemaphoreType.DMA,
        ],
        compiler_params=params(60),
        cost_estimate=cost(60_000_000, 16 * 2**20),
        name="counts",
    )(edge_count, edge_src.reshape(grid_shape), edge_dst.reshape(grid_shape))
    return adj.reshape(node_rows, table_rows), degt


def step_kernel(
    adj_ref,
    feat_in,
    degt_ref,
    ask_ref,
    halo_ref,
    ends_ref,
    weight_ref,
    label_ref,
    ws_in,
    wn_in,
    wh_in,
    bias_ref,
    wo_ref,
    logit_ref,
    gfeat_ref,
    gself_ref,
    gneigh_ref,
    ghid_ref,
    gbias_ref,
    gout_ref,
    adj_s,
    feat_ref,
    ws_ref,
    wn_ref,
    wh_ref,
    gfeat_s,
    pair_s,
    deg_s,
    hcol_s,
    hrow_s,
    wcol_s,
    wfull_s,
    feat_t,
    agg_t,
    wrow_s,
    ask_s,
    arecv_s,
    first_s,
    frecv_s,
    arr_s,
    emb_s,
    agg_s,
    served_s,
    recv_s,
    left_s,
    right_s,
    delta_s,
    pgl_s,
    pgr_s,
    rgrad_s,
    back_s,
    gradb_s,
    gt_s,
    gw_s,
    small_s,
    cols_s,
    part_s,
    precv_s,
    hpart_s,
    hprecv_s,
    halo_s,
    hrecv_s,
    hrows_s,
    share_s,
    srecv_s,
    in_sem,
    adj_sem,
    send_sem,
    recv_sem,
):
    node_rows, width = feat_ref.shape
    block, peers = ask_ref.shape
    half = halo_ref.shape[0]
    recv_rows = peers * block
    pairs = ends_ref.shape[1]
    grp = lax.axis_size("grp")
    me = lax.axis_index("dom") * grp + lax.axis_index("grp")
    burst = WIDE // block
    bursts = peers // burst
    hburst = burst // 2
    tiles = node_rows // TILE
    barrier = pltpu.get_barrier_semaphore()

    def load_adj(i):
        return pltpu.make_async_copy(
            adj_ref.at[tile_of(i), :], adj_s.at[tile_of(i), :], adj_sem.at[i]
        )

    loads = [
        pltpu.make_async_copy(a, b, in_sem.at[n])
        for n, (a, b) in enumerate(
            ((feat_in, feat_ref), (ws_in, ws_ref), (wn_in, wn_ref), (wh_in, wh_ref))
        )
    ]
    for load in loads:
        load.start()

    def fetch(i, carry):
        load_adj(i).start()
        return carry


    def greet(i, carry):
        for u in range(7):
            pl.semaphore_signal(
                barrier,
                inc=1,
                device_id=jnp.bitwise_and(me + (i * 7 + u + 1), peers - 1),
                device_id_type=LOGICAL,
            )
        return carry

    pl.semaphore_signal(
        barrier,
        inc=1,
        device_id=jnp.bitwise_and(me + (peers - 1), peers - 1),
        device_id_type=LOGICAL,
    )
    lax.fori_loop(0, (peers - 2) // 7, greet, 0)
    lax.fori_loop(0, tiles, fetch, 0)
    for load in loads:
        load.wait()

    def rows_of(p):
        return pl.ds(pl.multiple_of(p * block, block), block)

    def burst_at(k):
        return lax.rem(me // burst + k, bursts)

    def ship(k, source, target, which):
        low = jnp.bitwise_and(me, burst - 1)
        first = burst_at(k) * burst

        def one(i):
            p = first + jnp.bitwise_and(low + i, burst - 1)
            pltpu.make_async_remote_copy(
                src_ref=source(p),
                dst_ref=target,
                send_sem=send_sem.at[which],
                recv_sem=recv_sem.at[which, k],
                device_id=p,
                device_id_type=LOGICAL,
            ).start()

        @pl.when(k > 0)
        def _():
            one(0)

        for i in range(1, burst):
            one(i)

    def arrived(k, ref, unit, which):
        first = pl.ds(unit, (burst - 1) * unit) if unit else pl.ds(1, burst - 1)
        rest = pl.ds(0, burst * unit) if unit else pl.ds(0, burst)
        if isinstance(k, int) and k == 0:
            part = ref.at[first]
        else:
            part = ref.at[rest]
        pltpu.make_async_copy(part, part, recv_sem.at[which, k]).wait()

    def sent(part, which):
        pltpu.make_async_copy(part, part, send_sem.at[which]).wait()

    def source_at(k):
        return lax.rem(me // burst - k + bursts, bursts)

    def produce(fill, source, target, which):
        fill(0)

        def middle(k, carry):
            fill(k)
            ship(k - 1, source, target, which)
            return carry

        lax.fori_loop(1, bursts, middle, 0)

    def halves(rows):
        wide = rows.reshape(burst, half, width)
        return jnp.concatenate([wide[:, :, :LANES], wide[:, :, LANES:]], axis=1)

    def whole(blocks):
        wide = blocks.astype(jnp.float32)
        return jnp.concatenate([wide[:, :half], wide[:, half : 2 * half]], axis=2)

    def spread(table, depth):
        shape = (table.shape[0], depth, table.shape[1])
        keep = lax.broadcasted_iota(jnp.int32, shape, 1) == lax.broadcasted_iota(
            jnp.int32, shape, 2
        )
        wide = jnp.broadcast_to(table[:, None, :], shape)
        one = jnp.sum(jnp.where(keep, wide, 0.0), axis=2, keepdims=True)
        return one.reshape(shape[0] * depth, 1)

    def as_row(col):
        return jnp.transpose(jnp.broadcast_to(col, (col.shape[0], LANES)))[:8]

    deg_s[...] = jnp.concatenate([degt_ref[0], degt_ref[1]], axis=1)
    hcol_s[...] = spread(jnp.transpose(halo_ref[...].astype(jnp.float32)), half)
    ask_table = jnp.transpose(
        jnp.concatenate(
            [ask_ref[...].astype(jnp.float32), jnp.zeros((LANES - block, peers), jnp.float32)],
            axis=0,
        )
    )
    ask_s[...] = ask_table.astype(jnp.int32).reshape(peers, 1, LANES)

    def outgoing(t, carry):
        hot = pick(hcol_s[tile_of(t), :].astype(jnp.int32), 0, node_rows, 1)
        part = pl.ds(pl.multiple_of(t * burst, burst), burst)
        first_s[part] = halves(dot32(hot, feat_ref[...])).astype(jnp.bfloat16)
        return carry

    lax.fori_loop(0, bursts, outgoing, 0)

    def local_sums(i, carry):
        load_adj(i).wait()
        at = tile_of(i)
        gfeat_s[at, :] = dot32(adj_s[at, :node_rows], feat_ref[...])
        return carry

    lax.fori_loop(0, tiles, local_sums, 0)
    pl.semaphore_wait(barrier, peers - 1)
    first_of = lambda p: first_s.at[p]
    for k in range(bursts):
        ship(k, first_of, frecv_s.at[me], 0)
    ask_of = lambda p: ask_s.at[p]
    for k in range(bursts):
        ship(k, ask_of, arecv_s.at[me], 8)
    frecv_s[me] = first_s[me]
    arecv_s[me] = ask_s[me]
    pair_s[...] = jnp.concatenate(
        [
            ends_ref[...].astype(jnp.float32),
            weight_ref[...],
            label_ref[...].astype(jnp.float32),
            jnp.zeros((4, pairs), jnp.float32),
        ],
        axis=0,
    )

    def columns(i, carry):
        at = pl.ds(pl.multiple_of(i * WIDE, WIDE), WIDE)
        cols_s[at, :] = jnp.transpose(pair_s[:, at])
        return carry

    lax.fori_loop(0, pairs // WIDE, columns, 0)
    hrow_s[...] = as_row(hcol_s[...])
    for k in range(bursts):
        arrived(k, frecv_s, 0, 0)
        arrived(k, arecv_s, 0, 8)
    arr_s[...] = whole(frecv_s[...]).reshape(peers * half, width).astype(jnp.bfloat16)
    wcol_s[0:peers, :] = jnp.max(arecv_s[...], axis=1).astype(jnp.float32)

    def ship_half(n, source, target, which):
        k = n // 2
        low = jnp.bitwise_and(me, hburst - 1)
        first = half_at(n)

        def one(i):
            p = first + jnp.bitwise_and(low + i, hburst - 1)
            pltpu.make_async_remote_copy(
                src_ref=source(p),
                dst_ref=target,
                send_sem=send_sem.at[which],
                recv_sem=recv_sem.at[which, k],
                device_id=p,
                device_id_type=LOGICAL,
            ).start()

        @pl.when(n > 0)
        def _():
            one(0)

        for i in range(1, hburst):
            one(i)

    def produce_halves(fill, source, target, which):
        fill(0)

        def middle(n, carry):
            fill(n)
            ship_half(n - 1, source, target, which)
            return carry

        lax.fori_loop(1, 2 * bursts, middle, 0)

    def encode(i, carry):
        at = pl.ds(pl.multiple_of(i * TALL, TALL), TALL)
        sums = gfeat_s[at, :] + dot32(adj_s[at, node_rows:], arr_s[...])
        degree = jnp.transpose(deg_s[:, at])[:, :1]
        mean = (sums / degree).astype(jnp.bfloat16)
        agg_s[at, :] = mean
        emb_s[at, :] = (dot32(feat_ref[at, :], ws_ref[...]) + dot32(mean, wn_ref[...])).astype(
            jnp.bfloat16
        )
        return carry

    lax.fori_loop(0, node_rows // TALL, encode, 0)

    def half_at(n):
        k, sub = n // 2, lax.rem(n, 2)
        low = jnp.bitwise_and(me, burst - 1) // hburst
        return burst_at(k) * burst + jnp.bitwise_and(low + sub, 1) * hburst

    def serve(n):
        p = half_at(n)
        at = pl.ds(pl.multiple_of(p * block, TILE), TILE)
        asked = spread(wcol_s[pl.ds(pl.multiple_of(p, hburst), hburst), :], block)
        wfull_s[at, :] = asked
        hot = pick(asked.astype(jnp.int32), 0, node_rows, 1)
        served_s[at, :] = dot32(hot, emb_s[...]).astype(jnp.bfloat16)

    served_of = lambda p: served_s.at[rows_of(p), :]
    produce_halves(serve, served_of, recv_s.at[rows_of(me), :], 1)
    recv_s[rows_of(me), :] = served_s[rows_of(me), :]
    small_s[...] = jnp.zeros(small_s.shape, jnp.float32)
    ship_half(2 * bursts - 1, served_of, recv_s.at[rows_of(me), :], 1)
    feat_t[...] = jnp.transpose(feat_ref[...])
    agg_t[...] = jnp.transpose(agg_s[...])

    def ask_rows(i, carry):
        at = pl.ds(pl.multiple_of(i * WIDE, WIDE), WIDE)
        wrow_s[:, at] = as_row(wfull_s[at, :])
        return carry

    lax.fori_loop(0, recv_rows // WIDE, ask_rows, 0)

    for k in range(bursts):
        arrived(k, recv_s, block, 1)
        b = source_at(k)
        here = pl.ds(pl.multiple_of(b * WIDE, WIDE), WIDE)

        def gather(i, carry):
            at = pl.ds(pl.multiple_of(i * TALL, TALL), TALL)
            for side, rows in ((0, left_s), (1, right_s)):
                ends = cols_s[at, side : side + 1].astype(jnp.int32)
                found = dot32(pick(ends, b * WIDE, WIDE, 1), recv_s[here, :]).astype(
                    jnp.bfloat16
                )
                rows[at, :] = found if k == 0 else rows[at, :] + found
            return carry

        lax.fori_loop(0, pairs // TALL, gather, 0)

    def forward(i, carry):
        at = pl.ds(pl.multiple_of(i * TALL, TALL), TALL)
        cols = cols_s[at, :]
        left = left_s[at, :]
        right = right_s[at, :]
        pre = dot32(left, wh_ref[:width, :]) + dot32(right, wh_ref[width:, :]) + bias_ref[...]
        hidden = jnp.maximum(pre, 0.0)
        logit = jnp.sum(hidden * wo_ref[...], axis=1, keepdims=True)
        logit_ref[:, at] = jnp.transpose(jnp.broadcast_to(logit, (TALL, LANES)))[:1]
        slope = cols[:, 2:3] * (jax.nn.sigmoid(logit) - cols[:, 3:4])
        delta = jnp.where(pre > 0, slope * wo_ref[...], 0.0)
        small_s[0:1, :] += jnp.sum(delta, axis=0, keepdims=True)
        small_s[1:2, :] += jnp.sum(slope * hidden, axis=0, keepdims=True)
        delta_b = delta.astype(jnp.bfloat16)
        delta_s[at, :] = delta_b
        pgl_s[at, :] = dot_nt(delta_b, wh_ref[:width, :]).astype(jnp.bfloat16)
        pgr_s[at, :] = dot_nt(delta_b, wh_ref[width:, :]).astype(jnp.bfloat16)
        return carry

    lax.fori_loop(0, pairs // TALL, forward, 0)
    ends_row = ends_ref[...]

    def collect(n):
        first = half_at(n) * block
        total = dot32(pick(ends_row[0:1, :], first, TILE, 0), pgl_s[...]) + dot32(
            pick(ends_row[1:2, :], first, TILE, 0), pgr_s[...]
        )
        rgrad_s[pl.ds(pl.multiple_of(first, TILE), TILE), :] = total.astype(jnp.bfloat16)

    rgrad_of = lambda p: rgrad_s.at[rows_of(p), :]
    produce_halves(collect, rgrad_of, back_s.at[rows_of(me), :], 2)
    back_s[rows_of(me), :] = rgrad_s[rows_of(me), :]
    ship_half(2 * bursts - 1, rgrad_of, back_s.at[rows_of(me), :], 2)
    gw_s[2 * width : 3 * width, :] = dot_tn(left_s[...], delta_s[...])
    gw_s[3 * width :, :] = dot_tn(right_s[...], delta_s[...])

    def eighths(rows):
        wide = rows.reshape(burst // 2, 8, width)
        both = jnp.concatenate([wide[:, None, :, :LANES], wide[:, None, :, LANES:]], axis=1)
        return both.reshape(burst, 8, LANES).astype(jnp.bfloat16)

    def joined(blocks):
        wide = blocks.reshape(peers // 2, 2, 8, LANES)
        return jnp.concatenate([wide[:, 0], wide[:, 1]], axis=2).reshape(2 * width, width)

    def eighth_of(t):
        return pl.ds(pl.multiple_of(t * LANES, LANES), LANES)

    for k in range(bursts):
        t = burst_at(k)
        hpart_s[pl.ds(t * burst, burst)] = eighths(gw_s[eighth_of(t + bursts), :])
    hpart_of = lambda p: hpart_s.at[p]
    hprecv_s[me] = hpart_s[me]
    for k in range(bursts):
        ship(k, hpart_of, hprecv_s.at[me], 7)
    for k in range(bursts):
        arrived(k, back_s, block, 2)
        b = source_at(k)
        here = pl.ds(pl.multiple_of(b * WIDE, WIDE), WIDE)

        def put(i, carry):
            at = pl.ds(pl.multiple_of(i * TALL, TALL), TALL)
            found = dot32(pick(wrow_s[0:1, here].astype(jnp.int32), i * TALL, TALL, 0), back_s[here, :])
            gfeat_s[at, :] = found if k == 0 else gfeat_s[at, :] + found
            return carry

        lax.fori_loop(0, node_rows // TALL, put, 0)
    gradb_s[...] = gfeat_s[...].astype(jnp.bfloat16)
    gw_s[:width, :] = dot32(feat_t[...], gradb_s[...])
    gw_s[width : 2 * width, :] = dot32(agg_t[...], gradb_s[...])
    def weight_terms(k):
        t = burst_at(k)
        part_s[pl.ds(t * burst, burst)] = eighths(gw_s[eighth_of(t), :])

    part_of = lambda p: part_s.at[p]
    produce(weight_terms, part_of, precv_s.at[me], 3)
    precv_s[me] = part_s[me]
    gt_s[...] = (dot_nt(wn_ref[...], gradb_s[...]) / deg_s[0:1, :]).astype(jnp.bfloat16)
    ship(bursts - 1, part_of, precv_s.at[me], 3)

    def table_grad(first):
        cols = pl.ds(pl.multiple_of(first, TILE), TILE)
        return jnp.transpose(dot32(gt_s[...], adj_s[:, cols]))

    def return_halo(k):
        t = burst_at(k)
        halo_s[pl.ds(t * burst, burst)] = halves(
            table_grad(node_rows + t * TILE)
        ).astype(jnp.bfloat16)

    halo_of = lambda p: halo_s.at[p]
    produce(return_halo, halo_of, hrecv_s.at[me], 4)
    hrecv_s[me] = halo_s[me]

    def direct(i, carry):
        at = tile_of(i)
        gfeat_s[at, :] = dot_nt(gradb_s[at, :], ws_ref[...]) + table_grad(i * TILE)
        return carry

    direct(0, 0)
    ship(bursts - 1, halo_of, hrecv_s.at[me], 4)
    for k in range(bursts):
        arrived(k, precv_s, 0, 3)
        arrived(k, hprecv_s, 0, 7)
    own = jnp.concatenate(
        [
            jnp.sum(precv_s[...].astype(jnp.float32), axis=0),
            jnp.sum(hprecv_s[...].astype(jnp.float32), axis=0),
        ],
        axis=0,
    )
    small = small_s[...]
    small_hi = small.astype(jnp.bfloat16).astype(jnp.float32)
    small_lo = small - small_hi
    lines = [
        part[r : r + 1, c : c + LANES]
        for part in (small_hi, small_lo)
        for r in range(2)
        for c in (0, LANES)
    ]
    share_s[...] = jnp.concatenate([own] + lines, axis=0).astype(jnp.bfloat16)
    direct(1, 0)

    core = lax.rem(me // grp, 2)
    partner = me + (1 - 2 * core) * grp
    groups = peers // (2 * grp)

    def share(i, carry):
        own_q = (me // (2 * grp)) * grp + lax.rem(me, grp)
        for u in range(7):
            q = jnp.bitwise_and(own_q + (i * 7 + u + 1) * 27, peers // 2 - 1)
            pltpu.make_async_remote_copy(
                src_ref=share_s,
                dst_ref=srecv_s.at[me],
                send_sem=send_sem.at[5],
                recv_sem=recv_sem.at[5, 0],
                device_id=q + (q // grp) * grp + core * grp,
                device_id_type=LOGICAL,
            ).start()
        return carry

    lax.fori_loop(0, (peers // 2 - 1) // 7, share, 0)
    srecv_s[me] = share_s[...]
    lax.fori_loop(2, tiles, direct, 0)
    for k in range(bursts):
        arrived(k, hrecv_s, 0, 4)
    hrows_s[...] = whole(hrecv_s[...]).reshape(peers * half, width).astype(jnp.bfloat16)

    def place(i, carry):
        at = pl.ds(pl.multiple_of(i * TALL, TALL), TALL)
        hot = pick(hrow_s[0:1, :].astype(jnp.int32), i * TALL, TALL, 0)
        gfeat_s[at, :] += dot32(hot, hrows_s[...])
        return carry

    lax.fori_loop(0, node_rows // TALL, place, 0)
    result = pltpu.make_async_copy(gfeat_s, gfeat_ref, adj_sem.at[0])
    result.start()
    others = srecv_s.at[pl.ds(1, peers // 2 - 1)]
    pltpu.make_async_copy(others, others, recv_sem.at[5, 0]).wait()

    def across(i, carry):
        part = srecv_s.at[pl.ds(i * (2 * grp) + core * grp, grp)]
        pltpu.make_async_remote_copy(
            src_ref=part,
            dst_ref=part,
            send_sem=send_sem.at[6],
            recv_sem=recv_sem.at[5, 1],
            device_id=partner,
            device_id_type=LOGICAL,
        ).start()
        return carry

    lax.fori_loop(0, groups, across, 0)
    sent(others, 5)
    sent(srecv_s.at[pl.ds(0, peers // 2)], 6)
    for which, ref in ((1, served_s), (2, rgrad_s)):
        sent(ref.at[pl.ds(block, recv_rows - block), :], which)
    for which, ref in ((0, frecv_s), (3, part_s), (4, halo_s), (7, hpart_s), (8, arecv_s)):
        sent(ref.at[pl.ds(1, peers - 1)], which)
    mates = srecv_s.at[pl.ds(0, peers // 2)]
    pltpu.make_async_copy(mates, mates, recv_sem.at[5, 1]).wait()
    everyone = srecv_s[...].astype(jnp.float32)
    node_terms = joined(everyone[:, :8])
    gself_ref[...] = node_terms[:width]
    gneigh_ref[...] = node_terms[width:]
    ghid_ref[...] = joined(everyone[:, 8:16])
    total = jnp.sum(everyone[:, block:], axis=0)
    total = total[:4] + total[4:]
    gbias_ref[...] = jnp.concatenate([total[0:1], total[1:2]], axis=1)
    gout_ref[...] = jnp.concatenate([total[2:3], total[3:4]], axis=1)
    result.wait()


def finish_kernel(count, *refs):
    taken, given, held = refs[:count], refs[count : 2 * count], refs[2 * count : 3 * count]
    in_sem, out_sem = refs[3 * count :]
    parts = []
    for a, h, b in zip(taken, held, given):
        rows = a.shape[0]
        step = TILE if rows > TILE else rows
        parts += [(a, h, b, pl.ds(r, step)) for r in range(0, rows, step)]
    moves = [
        (
            pltpu.make_async_copy(a.at[at, :], h.at[at, :], in_sem.at[n]),
            pltpu.make_async_copy(h.at[at, :], b.at[at, :], out_sem.at[n]),
        )
        for n, (a, h, b, at) in enumerate(parts)
    ]
    for fetch, _ in moves:
        fetch.start()
    for fetch, put in moves:
        fetch.wait()
        put.start()
    for _, put in moves:
        put.wait()


def finish(arrays):
    count = len(arrays)
    moves = sum(max(a.shape[0] // TILE, 1) for a in arrays)
    return pl.pallas_call(
        lambda *refs: finish_kernel(count, *refs),
        out_shape=tuple(jax.ShapeDtypeStruct(a.shape, a.dtype) for a in arrays),
        in_specs=[ANY] * count,
        out_specs=(ANY,) * count,
        scratch_shapes=[pltpu.VMEM(a.shape, a.dtype) for a in arrays]
        + [pltpu.SemaphoreType.DMA((moves,)), pltpu.SemaphoreType.DMA((moves,))],
        compiler_params=params(60),
        name="finish",
    )(*arrays)


def train_step(
    adj, features, degt, ask, halo, ends, pair_weight, labels, w_self, w_neigh, w_hidden,
    bias, w_out
):
    node_rows, width = features.shape
    table_rows = adj.shape[1]
    block, peers = ask.shape
    half = halo.shape[0]
    recv_rows = peers * block
    pairs = ends.shape[1]
    lines = 2 * half + 8
    bf16 = lambda *shape: pltpu.VMEM(shape, jnp.bfloat16)
    return pl.pallas_call(
        step_kernel,
        out_shape=(
            jax.ShapeDtypeStruct((1, pairs), jnp.float32),
            jax.ShapeDtypeStruct((node_rows, width), jnp.float32),
            jax.ShapeDtypeStruct((width, width), jnp.float32),
            jax.ShapeDtypeStruct((width, width), jnp.float32),
            jax.ShapeDtypeStruct((2 * width, width), jnp.float32),
            jax.ShapeDtypeStruct((1, width), jnp.float32),
            jax.ShapeDtypeStruct((1, width), jnp.float32),
        ),
        in_specs=[ANY, ANY] + [VMEM] * 6 + [ANY] * 3 + [VMEM] * 2,
        out_specs=(VMEM, ANY) + (VMEM,) * 5,
        scratch_shapes=[
            bf16(node_rows, table_rows),
            bf16(node_rows, width),
            bf16(width, width),
            bf16(width, width),
            bf16(2 * width, width),
            pltpu.VMEM((node_rows, width), jnp.float32),
            pltpu.VMEM((8, pairs), jnp.float32),
            pltpu.VMEM((8, node_rows), jnp.float32),
            pltpu.VMEM((peers * half, 1), jnp.float32),
            pltpu.VMEM((8, peers * half), jnp.float32),
            pltpu.VMEM((peers, LANES), jnp.float32),
            pltpu.VMEM((recv_rows, 1), jnp.float32),
            bf16(width, node_rows),
            bf16(width, node_rows),
            pltpu.VMEM((8, recv_rows), jnp.float32),
            pltpu.VMEM((peers, 1, LANES), jnp.int32),
            pltpu.VMEM((peers, 1, LANES), jnp.int32),
            bf16(peers, block, LANES),
            bf16(peers, block, LANES),
            bf16(peers * half, width),
            bf16(node_rows, width),
            bf16(node_rows, width),
            bf16(recv_rows, width),
            bf16(recv_rows, width),
            bf16(pairs, width),
            bf16(pairs, width),
            bf16(pairs, width),
            bf16(pairs, width),
            bf16(pairs, width),
            bf16(recv_rows, width),
            bf16(recv_rows, width),
            bf16(node_rows, width),
            bf16(width, node_rows),
            pltpu.VMEM((4 * width, width), jnp.float32),
            pltpu.VMEM((8, width), jnp.float32),
            pltpu.VMEM((pairs, 8), jnp.float32),
            bf16(peers, half, LANES),
            bf16(peers, half, LANES),
            bf16(peers, half, LANES),
            bf16(peers, half, LANES),
            bf16(peers, block, LANES),
            bf16(peers, block, LANES),
            bf16(peers * half, width),
            bf16(lines, LANES),
            bf16(peers, lines, LANES),
            pltpu.SemaphoreType.DMA((4,)),
            pltpu.SemaphoreType.DMA((node_rows // TILE,)),
            pltpu.SemaphoreType.DMA((9,)),
            pltpu.SemaphoreType.DMA((9, recv_rows // WIDE)),
        ],
        compiler_params=pltpu.CompilerParams(
            vmem_limit_bytes=62 * 2**20, collective_id=0, has_side_effects=True
        ),
        cost_estimate=cost(30_000_000_000, 24 * 2**20),
        name="train_step",
    )(
        adj, features, degt, ask, halo, ends, pair_weight, labels, w_self, w_neigh,
        w_hidden, bias, w_out,
    )


def per_device(
    features,
    edge_src,
    edge_dst,
    edge_count,
    halo_index,
    request_rows,
    pair_ends,
    labels,
    pair_weight,
    w_self,
    w_neigh,
    w_hidden,
    b_hidden,
    w_out,
):
    node_rows = features.shape[0]
    halo = halo_index[0].T
    adj, degt = adjacency(edge_src, edge_dst, edge_count, node_rows, node_rows + halo.size)
    logits, grad_features, grad_self, grad_neigh, grad_hidden, grad_bias, grad_out = train_step(
        adj, features, degt, request_rows[0].T, halo, pair_ends.T, pair_weight[None],
        labels[None], w_self, w_neigh, w_hidden, b_hidden[None], w_out[None]
    )
    grad_features, grad_self, grad_neigh, grad_hidden, grad_bias, grad_out, logits = finish(
        (grad_features, grad_self, grad_neigh, grad_hidden, grad_bias, grad_out, logits)
    )
    return (
        logits[0],
        grad_features,
        grad_self,
        grad_neigh,
        grad_hidden,
        grad_bias[0],
        grad_out[0],
    )


def solution(mesh):
    split = P(AXES)
    in_specs = (
        P(AXES, None),
        split,
        split,
        split,
        P(AXES, None, None),
        P(AXES, None, None),
        P(AXES, None),
        split,
        split,
        P(),
        P(),
        P(),
        P(),
        P(),
    )
    out_specs = (split, P(AXES, None), P(), P(), P(), P(), P())
    return jax.shard_map(
        per_device, mesh=mesh, in_specs=in_specs, out_specs=out_specs, check_vma=False
    )
```

```python
import jax
import jax.numpy as jnp
from jax import lax
from jax.experimental import pallas as pl
from jax.experimental.pallas import tpu as pltpu
from jax.sharding import PartitionSpec as P

AXES = ("dom", "grp")
LANES = 128
GROUP = 4
STRIDE = LANES // GROUP
TILE = 256
WIDE = 512
TALL = 1024
LOGICAL = pl.DeviceIdType.LOGICAL
CLASH = 1 << 20
VMEM = pl.BlockSpec(memory_space=pltpu.VMEM)
SMEM = pl.BlockSpec(memory_space=pltpu.SMEM)
ANY = pl.BlockSpec(memory_space=pl.ANY)


def dot32(a, b):
    return jnp.dot(a, b, preferred_element_type=jnp.float32)


def dot_nt(a, b):
    return lax.dot_general(a, b, (((1,), (1,)), ((), ())), preferred_element_type=jnp.float32)


def dot_tn(a, b):
    return lax.dot_general(a, b, (((0,), (0,)), ((), ())), preferred_element_type=jnp.float32)


def params(mib):
    return pltpu.CompilerParams(vmem_limit_bytes=mib * 2**20)


def cost(flops, size):
    return pl.CostEstimate(flops=flops, bytes_accessed=size, transcendentals=0)


def tile_of(i):
    return pl.ds(pl.multiple_of(i * TILE, TILE), TILE)


def pick(index, first, count, axis):
    shape = (index.shape[0], count) if axis == 1 else (count, index.shape[1])
    ids = lax.broadcasted_iota(jnp.int32, shape, axis) + first
    return jnp.where(index == ids, 1.0, 0.0).astype(jnp.bfloat16)


def edge_words(half, panels, count, src, dst):
    shape = src.shape
    lane = lax.broadcasted_iota(jnp.int32, shape, 1)
    live = lax.broadcasted_iota(jnp.int32, shape, 0) * LANES + lane < count
    upper = jnp.where(dst >= half, 1, 0)
    row = jnp.right_shift(src, 7) * half + dst - upper * half
    row = jnp.where(live, row, half * panels + lane // STRIDE)
    unit = jnp.where(live, jnp.bitwise_and(src, LANES - 1) + upper * LANES, 2 * LANES)
    clash = jnp.zeros(shape, jnp.int32)
    for k in range(1, GROUP // 2 + 1):
        clash = clash + jnp.where(row == pltpu.roll(row, k * STRIDE, 1), 1, 0)
    any_clash = jnp.max(clash.astype(jnp.float32), axis=1, keepdims=True) > 0.0
    return row + jnp.where(any_clash & (lane == 0), CLASH, 0), unit


def counts_kernel(
    half, panels, count_ref, src_ref, dst_ref, adj_ref, degt_ref, even, odd, unit_a, unit_b,
    row_v, row_ref, unit_ref, row_sem
):
    step = pl.program_id(0)
    chunks = unit_ref.shape[0]

    @pl.when(step == 0)
    def _():
        row_v[...], unit_ref[...] = edge_words(
            half, panels, count_ref[0], src_ref[...], dst_ref[...]
        )
        words = pltpu.make_async_copy(row_v, row_ref, row_sem)
        words.start()
        lane = lax.broadcasted_iota(jnp.int32, (LANES, LANES), 1)

        def clear(i, carry):
            even[tile_of(i), :] = jnp.zeros((TILE, LANES), jnp.int32)
            odd[tile_of(i), :] = jnp.zeros((TILE, LANES), jnp.int32)
            return carry

        lax.fori_loop(0, half * panels // TILE, clear, 0)
        words.wait()

        def units_of(c):
            c = jnp.minimum(c, chunks - 1)
            wide = jnp.transpose(jnp.broadcast_to(unit_ref[pl.ds(c, 1), :], (LANES, LANES)))
            return jnp.where(wide == lane, 1, jnp.where(wide == lane + LANES, 65536, 0))

        unit_a[...] = units_of(0)

        def chunk(c, units, later):
            places = row_ref.at[c]
            head = places[0]

            def load(s):
                words = odd if s % 2 else even
                at = [places[s + STRIDE * t] for t in range(GROUP)]
                new = [
                    words[pl.ds(a, 1), :] + units[pl.ds(s + STRIDE * t, 1), :]
                    for t, a in enumerate(at)
                ]
                return words, at, new

            def store(words, at, new):
                for a, n in zip(at, new):
                    words[pl.ds(a, 1), :] = n

            @pl.when(head < CLASH)
            def _():
                coming = units_of(c + 1)
                held = load(0)
                for s in range(1, STRIDE):
                    following = load(s)
                    store(*held)
                    held = following
                store(*held)
                later[...] = coming

            @pl.when(head >= CLASH)
            def _():
                later[...] = units_of(c + 1)
                for j in range(LANES):
                    words = odd if j % 2 else even
                    a = places[j]
                    if j == 0:
                        a = a - CLASH
                    words[pl.ds(a, 1), :] = words[pl.ds(a, 1), :] + units[pl.ds(j, 1), :]

        def two(i, carry):
            chunk(2 * i, unit_a, unit_b)
            chunk(2 * i + 1, unit_b, unit_a)
            return carry

        lax.fori_loop(0, chunks // 2, two, 0)

    first = step * TILE
    total = jnp.zeros((TILE, LANES), jnp.int32)
    for p in range(panels):
        part = pl.ds(pl.multiple_of(p * half + first, TILE), TILE)
        word = even[part, :] + odd[part, :]
        total = total + word
        cols = slice(p * LANES, (p + 1) * LANES)
        for h, count in enumerate((jnp.bitwise_and(word, 0xFFFF), jnp.right_shift(word, 16))):
            adj_ref[h, :, cols] = count.astype(jnp.float32).astype(jnp.bfloat16)
    for h, count in enumerate((jnp.bitwise_and(total, 0xFFFF), jnp.right_shift(total, 16))):
        degree = jnp.sum(count.astype(jnp.float32), axis=1, keepdims=True)
        wide = jnp.broadcast_to(jnp.maximum(degree, 1.0), (TILE, LANES))
        degt_ref[h] = jnp.transpose(wide)[:8]


def adjacency(edge_src, edge_dst, edge_count, node_rows, table_rows):
    half = node_rows // 2
    panels = table_rows // LANES
    chunks = edge_src.shape[0] // LANES
    grid_shape = (chunks, LANES)
    adj, degt = pl.pallas_call(
        lambda *refs: counts_kernel(half, panels, *refs),
        grid=(half // TILE,),
        out_shape=(
            jax.ShapeDtypeStruct((2, half, table_rows), jnp.bfloat16),
            jax.ShapeDtypeStruct((2, 8, half), jnp.float32),
        ),
        in_specs=[SMEM] + [pl.BlockSpec(grid_shape, lambda i: (0, 0))] * 2,
        out_specs=(
            pl.BlockSpec((2, TILE, table_rows), lambda i: (0, i, 0)),
            pl.BlockSpec((2, 8, TILE), lambda i: (0, 0, i)),
        ),
        scratch_shapes=[
            pltpu.VMEM((half * panels + GROUP, LANES), jnp.int32),
            pltpu.VMEM((half * panels + GROUP, LANES), jnp.int32),
            pltpu.VMEM((LANES, LANES), jnp.int32),
            pltpu.VMEM((LANES, LANES), jnp.int32),
            pltpu.VMEM(grid_shape, jnp.int32),
            pltpu.SMEM(grid_shape, jnp.int32),
            pltpu.VMEM(grid_shape, jnp.int32),
            pltpu.SemaphoreType.DMA,
        ],
        compiler_params=params(60),
        cost_estimate=cost(60_000_000, 16 * 2**20),
        name="counts",
    )(edge_count, edge_src.reshape(grid_shape), edge_dst.reshape(grid_shape))
    return adj.reshape(node_rows, table_rows), degt


def step_kernel(
    adj_ref,
    feat_in,
    degt_ref,
    ask_ref,
    halo_ref,
    ends_ref,
    weight_ref,
    label_ref,
    ws_in,
    wn_in,
    wh_in,
    bias_ref,
    wo_ref,
    logit_ref,
    gfeat_ref,
    gself_ref,
    gneigh_ref,
    ghid_ref,
    gbias_ref,
    gout_ref,
    adj_s,
    feat_ref,
    ws_ref,
    wn_ref,
    wh_ref,
    gfeat_s,
    pair_s,
    deg_s,
    hcol_s,
    hrow_s,
    wcol_s,
    wfull_s,
    feat_t,
    agg_t,
    wrow_s,
    ask_s,
    arecv_s,
    first_s,
    frecv_s,
    arr_s,
    emb_s,
    agg_s,
    served_s,
    recv_s,
    left_s,
    right_s,
    delta_s,
    pgl_s,
    pgr_s,
    rgrad_s,
    back_s,
    gradb_s,
    gt_s,
    gw_s,
    small_s,
    cols_s,
    part_s,
    precv_s,
    hpart_s,
    hprecv_s,
    halo_s,
    hrecv_s,
    hrows_s,
    share_s,
    srecv_s,
    in_sem,
    adj_sem,
    send_sem,
    recv_sem,
):
    node_rows, width = feat_ref.shape
    block, peers = ask_ref.shape
    half = halo_ref.shape[0]
    recv_rows = peers * block
    pairs = ends_ref.shape[1]
    grp = lax.axis_size("grp")
    me = lax.axis_index("dom") * grp + lax.axis_index("grp")
    burst = WIDE // block
    bursts = peers // burst
    hburst = burst // 2
    tiles = node_rows // TILE
    barrier = pltpu.get_barrier_semaphore()

    def load_adj(i):
        return pltpu.make_async_copy(
            adj_ref.at[tile_of(i), :], adj_s.at[tile_of(i), :], adj_sem.at[i]
        )

    loads = [
        pltpu.make_async_copy(a, b, in_sem.at[n])
        for n, (a, b) in enumerate(
            ((feat_in, feat_ref), (ws_in, ws_ref), (wn_in, wn_ref), (wh_in, wh_ref))
        )
    ]
    for load in loads:
        load.start()

    def fetch(i, carry):
        load_adj(i).start()
        return carry


    def greet(i, carry):
        for u in range(7):
            pl.semaphore_signal(
                barrier,
                inc=1,
                device_id=jnp.bitwise_and(me + (i * 7 + u + 1), peers - 1),
                device_id_type=LOGICAL,
            )
        return carry

    pl.semaphore_signal(
        barrier,
        inc=1,
        device_id=jnp.bitwise_and(me + (peers - 1), peers - 1),
        device_id_type=LOGICAL,
    )
    lax.fori_loop(0, (peers - 2) // 7, greet, 0)
    lax.fori_loop(0, tiles, fetch, 0)
    for load in loads:
        load.wait()

    def rows_of(p):
        return pl.ds(pl.multiple_of(p * block, block), block)

    def burst_at(k):
        return lax.rem(me // burst + k, bursts)

    def ship(k, source, target, which):
        low = jnp.bitwise_and(me, burst - 1)
        first = burst_at(k) * burst

        def one(i):
            p = first + jnp.bitwise_and(low + i, burst - 1)
            pltpu.make_async_remote_copy(
                src_ref=source(p),
                dst_ref=target,
                send_sem=send_sem.at[which],
                recv_sem=recv_sem.at[which, k],
                device_id=p,
                device_id_type=LOGICAL,
            ).start()

        @pl.when(k > 0)
        def _():
            one(0)

        for i in range(1, burst):
            one(i)

    def arrived(k, ref, unit, which):
        first = pl.ds(unit, (burst - 1) * unit) if unit else pl.ds(1, burst - 1)
        rest = pl.ds(0, burst * unit) if unit else pl.ds(0, burst)
        if isinstance(k, int) and k == 0:
            part = ref.at[first]
        else:
            part = ref.at[rest]
        pltpu.make_async_copy(part, part, recv_sem.at[which, k]).wait()

    def sent(part, which):
        pltpu.make_async_copy(part, part, send_sem.at[which]).wait()

    def source_at(k):
        return lax.rem(me // burst - k + bursts, bursts)

    def produce(fill, source, target, which):
        fill(0)

        def middle(k, carry):
            fill(k)
            ship(k - 1, source, target, which)
            return carry

        lax.fori_loop(1, bursts, middle, 0)

    def halves(rows):
        wide = rows.reshape(burst, half, width)
        return jnp.concatenate([wide[:, :, :LANES], wide[:, :, LANES:]], axis=1)

    def whole(blocks):
        wide = blocks.astype(jnp.float32)
        return jnp.concatenate([wide[:, :half], wide[:, half : 2 * half]], axis=2)

    def spread(table, depth):
        shape = (table.shape[0], depth, table.shape[1])
        keep = lax.broadcasted_iota(jnp.int32, shape, 1) == lax.broadcasted_iota(
            jnp.int32, shape, 2
        )
        wide = jnp.broadcast_to(table[:, None, :], shape)
        one = jnp.sum(jnp.where(keep, wide, 0.0), axis=2, keepdims=True)
        return one.reshape(shape[0] * depth, 1)

    def as_row(col):
        return jnp.transpose(jnp.broadcast_to(col, (col.shape[0], LANES)))[:8]

    deg_s[...] = jnp.concatenate([degt_ref[0], degt_ref[1]], axis=1)
    hcol_s[...] = spread(jnp.transpose(halo_ref[...].astype(jnp.float32)), half)
    ask_table = jnp.transpose(
        jnp.concatenate(
            [ask_ref[...].astype(jnp.float32), jnp.zeros((LANES - block, peers), jnp.float32)],
            axis=0,
        )
    )
    ask_s[...] = ask_table.astype(jnp.int32).reshape(peers, 1, LANES)

    def outgoing(t, carry):
        hot = pick(hcol_s[tile_of(t), :].astype(jnp.int32), 0, node_rows, 1)
        part = pl.ds(pl.multiple_of(t * burst, burst), burst)
        first_s[part] = halves(dot32(hot, feat_ref[...])).astype(jnp.bfloat16)
        return carry

    lax.fori_loop(0, bursts, outgoing, 0)

    def local_sums(i, carry):
        load_adj(i).wait()
        at = tile_of(i)
        gfeat_s[at, :] = dot32(adj_s[at, :node_rows], feat_ref[...])
        return carry

    lax.fori_loop(0, tiles, local_sums, 0)
    pl.semaphore_wait(barrier, peers - 1)
    first_of = lambda p: first_s.at[p]
    for k in range(bursts):
        ship(k, first_of, frecv_s.at[me], 0)
    ask_of = lambda p: ask_s.at[p]
    for k in range(bursts):
        ship(k, ask_of, arecv_s.at[me], 8)
    frecv_s[me] = first_s[me]
    arecv_s[me] = ask_s[me]
    pair_s[...] = jnp.concatenate(
        [
            ends_ref[...].astype(jnp.float32),
            weight_ref[...],
            label_ref[...].astype(jnp.float32),
            jnp.zeros((4, pairs), jnp.float32),
        ],
        axis=0,
    )

    def columns(i, carry):
        at = pl.ds(pl.multiple_of(i * WIDE, WIDE), WIDE)
        cols_s[at, :] = jnp.transpose(pair_s[:, at])
        return carry

    lax.fori_loop(0, pairs // WIDE, columns, 0)
    hrow_s[...] = as_row(hcol_s[...])
    for k in range(bursts):
        arrived(k, frecv_s, 0, 0)
        arrived(k, arecv_s, 0, 8)
    arr_s[...] = whole(frecv_s[...]).reshape(peers * half, width).astype(jnp.bfloat16)
    wcol_s[0:peers, :] = jnp.max(arecv_s[...], axis=1).astype(jnp.float32)

    def ship_half(n, source, target, which):
        k = n // 2
        low = jnp.bitwise_and(me, hburst - 1)
        first = half_at(n)

        def one(i):
            p = first + jnp.bitwise_and(low + i, hburst - 1)
            pltpu.make_async_remote_copy(
                src_ref=source(p),
                dst_ref=target,
                send_sem=send_sem.at[which],
                recv_sem=recv_sem.at[which, k],
                device_id=p,
                device_id_type=LOGICAL,
            ).start()

        @pl.when(n > 0)
        def _():
            one(0)

        for i in range(1, hburst):
            one(i)

    def produce_halves(fill, source, target, which):
        fill(0)

        def middle(n, carry):
            fill(n)
            ship_half(n - 1, source, target, which)
            return carry

        lax.fori_loop(1, 2 * bursts, middle, 0)

    def encode(i, carry):
        at = pl.ds(pl.multiple_of(i * TALL, TALL), TALL)
        sums = gfeat_s[at, :] + dot32(adj_s[at, node_rows:], arr_s[...])
        degree = jnp.transpose(deg_s[:, at])[:, :1]
        mean = (sums / degree).astype(jnp.bfloat16)
        agg_s[at, :] = mean
        emb_s[at, :] = (dot32(feat_ref[at, :], ws_ref[...]) + dot32(mean, wn_ref[...])).astype(
            jnp.bfloat16
        )
        return carry

    lax.fori_loop(0, node_rows // TALL, encode, 0, unroll=2)

    def half_at(n):
        k, sub = n // 2, lax.rem(n, 2)
        low = jnp.bitwise_and(me, burst - 1) // hburst
        return burst_at(k) * burst + jnp.bitwise_and(low + sub, 1) * hburst

    def serve(n):
        p = half_at(n)
        at = pl.ds(pl.multiple_of(p * block, TILE), TILE)
        asked = spread(wcol_s[pl.ds(pl.multiple_of(p, hburst), hburst), :], block)
        wfull_s[at, :] = asked
        hot = pick(asked.astype(jnp.int32), 0, node_rows, 1)
        served_s[at, :] = dot32(hot, emb_s[...]).astype(jnp.bfloat16)

    served_of = lambda p: served_s.at[rows_of(p), :]
    produce_halves(serve, served_of, recv_s.at[rows_of(me), :], 1)
    recv_s[rows_of(me), :] = served_s[rows_of(me), :]
    small_s[...] = jnp.zeros(small_s.shape, jnp.float32)
    ship_half(2 * bursts - 1, served_of, recv_s.at[rows_of(me), :], 1)
    feat_t[...] = jnp.transpose(feat_ref[...])
    agg_t[...] = jnp.transpose(agg_s[...])

    def ask_rows(i, carry):
        at = pl.ds(pl.multiple_of(i * WIDE, WIDE), WIDE)
        wrow_s[:, at] = as_row(wfull_s[at, :])
        return carry

    lax.fori_loop(0, recv_rows // WIDE, ask_rows, 0)

    for k in range(bursts):
        arrived(k, recv_s, block, 1)
        b = source_at(k)
        here = pl.ds(pl.multiple_of(b * WIDE, WIDE), WIDE)

        def gather(i, carry):
            at = pl.ds(pl.multiple_of(i * TALL, TALL), TALL)
            for side, rows in ((0, left_s), (1, right_s)):
                ends = cols_s[at, side : side + 1].astype(jnp.int32)
                found = dot32(pick(ends, b * WIDE, WIDE, 1), recv_s[here, :]).astype(
                    jnp.bfloat16
                )
                rows[at, :] = found if k == 0 else rows[at, :] + found
            return carry

        lax.fori_loop(0, pairs // TALL, gather, 0)

    def forward(i, carry):
        at = pl.ds(pl.multiple_of(i * TALL, TALL), TALL)
        cols = cols_s[at, :]
        left = left_s[at, :]
        right = right_s[at, :]
        pre = dot32(left, wh_ref[:width, :]) + dot32(right, wh_ref[width:, :]) + bias_ref[...]
        hidden = jnp.maximum(pre, 0.0)
        logit = jnp.sum(hidden * wo_ref[...], axis=1, keepdims=True)
        logit_ref[:, at] = jnp.transpose(jnp.broadcast_to(logit, (TALL, LANES)))[:1]
        slope = cols[:, 2:3] * (jax.nn.sigmoid(logit) - cols[:, 3:4])
        delta = jnp.where(pre > 0, slope * wo_ref[...], 0.0)
        small_s[0:1, :] += jnp.sum(delta, axis=0, keepdims=True)
        small_s[1:2, :] += jnp.sum(slope * hidden, axis=0, keepdims=True)
        delta_b = delta.astype(jnp.bfloat16)
        delta_s[at, :] = delta_b
        pgl_s[at, :] = dot_nt(delta_b, wh_ref[:width, :]).astype(jnp.bfloat16)
        pgr_s[at, :] = dot_nt(delta_b, wh_ref[width:, :]).astype(jnp.bfloat16)
        return carry

    lax.fori_loop(0, pairs // TALL, forward, 0, unroll=2)
    ends_row = ends_ref[...]

    def collect(n):
        first = half_at(n) * block
        total = dot32(pick(ends_row[0:1, :], first, TILE, 0), pgl_s[...]) + dot32(
            pick(ends_row[1:2, :], first, TILE, 0), pgr_s[...]
        )
        rgrad_s[pl.ds(pl.multiple_of(first, TILE), TILE), :] = total.astype(jnp.bfloat16)

    rgrad_of = lambda p: rgrad_s.at[rows_of(p), :]
    produce_halves(collect, rgrad_of, back_s.at[rows_of(me), :], 2)
    back_s[rows_of(me), :] = rgrad_s[rows_of(me), :]
    ship_half(2 * bursts - 1, rgrad_of, back_s.at[rows_of(me), :], 2)
    gw_s[2 * width : 3 * width, :] = dot_tn(left_s[...], delta_s[...])
    gw_s[3 * width :, :] = dot_tn(right_s[...], delta_s[...])

    def eighths(rows):
        wide = rows.reshape(burst // 2, 8, width)
        both = jnp.concatenate([wide[:, None, :, :LANES], wide[:, None, :, LANES:]], axis=1)
        return both.reshape(burst, 8, LANES).astype(jnp.bfloat16)

    def joined(blocks):
        wide = blocks.reshape(peers // 2, 2, 8, LANES)
        return jnp.concatenate([wide[:, 0], wide[:, 1]], axis=2).reshape(2 * width, width)

    def eighth_of(t):
        return pl.ds(pl.multiple_of(t * LANES, LANES), LANES)

    for k in range(bursts):
        t = burst_at(k)
        hpart_s[pl.ds(t * burst, burst)] = eighths(gw_s[eighth_of(t + bursts), :])
    hpart_of = lambda p: hpart_s.at[p]
    hprecv_s[me] = hpart_s[me]
    for k in range(bursts):
        ship(k, hpart_of, hprecv_s.at[me], 7)
    for k in range(bursts):
        arrived(k, back_s, block, 2)
        b = source_at(k)
        here = pl.ds(pl.multiple_of(b * WIDE, WIDE), WIDE)

        def put(i, carry):
            at = pl.ds(pl.multiple_of(i * TALL, TALL), TALL)
            found = dot32(pick(wrow_s[0:1, here].astype(jnp.int32), i * TALL, TALL, 0), back_s[here, :])
            gfeat_s[at, :] = found if k == 0 else gfeat_s[at, :] + found
            return carry

        lax.fori_loop(0, node_rows // TALL, put, 0)
    gradb_s[...] = gfeat_s[...].astype(jnp.bfloat16)
    gw_s[:width, :] = dot32(feat_t[...], gradb_s[...])
    gw_s[width : 2 * width, :] = dot32(agg_t[...], gradb_s[...])
    def weight_terms(k):
        t = burst_at(k)
        part_s[pl.ds(t * burst, burst)] = eighths(gw_s[eighth_of(t), :])

    part_of = lambda p: part_s.at[p]
    produce(weight_terms, part_of, precv_s.at[me], 3)
    precv_s[me] = part_s[me]
    gt_s[...] = (dot_nt(wn_ref[...], gradb_s[...]) / deg_s[0:1, :]).astype(jnp.bfloat16)
    ship(bursts - 1, part_of, precv_s.at[me], 3)

    def table_grad(first):
        cols = pl.ds(pl.multiple_of(first, TILE), TILE)
        return jnp.transpose(dot32(gt_s[...], adj_s[:, cols]))

    def return_halo(k):
        t = burst_at(k)
        halo_s[pl.ds(t * burst, burst)] = halves(
            table_grad(node_rows + t * TILE)
        ).astype(jnp.bfloat16)

    halo_of = lambda p: halo_s.at[p]
    produce(return_halo, halo_of, hrecv_s.at[me], 4)
    hrecv_s[me] = halo_s[me]

    def direct(i, carry):
        at = tile_of(i)
        gfeat_s[at, :] = dot_nt(gradb_s[at, :], ws_ref[...]) + table_grad(i * TILE)
        return carry

    direct(0, 0)
    ship(bursts - 1, halo_of, hrecv_s.at[me], 4)
    for k in range(bursts):
        arrived(k, precv_s, 0, 3)
        arrived(k, hprecv_s, 0, 7)
    own = jnp.concatenate(
        [
            jnp.sum(precv_s[...].astype(jnp.float32), axis=0),
            jnp.sum(hprecv_s[...].astype(jnp.float32), axis=0),
        ],
        axis=0,
    )
    small = small_s[...]
    small_hi = small.astype(jnp.bfloat16).astype(jnp.float32)
    small_lo = small - small_hi
    lines = [
        part[r : r + 1, c : c + LANES]
        for part in (small_hi, small_lo)
        for r in range(2)
        for c in (0, LANES)
    ]
    share_s[...] = jnp.concatenate([own] + lines, axis=0).astype(jnp.bfloat16)
    direct(1, 0)

    core = lax.rem(me // grp, 2)
    partner = me + (1 - 2 * core) * grp
    groups = peers // (2 * grp)

    def share(i, carry):
        own_q = (me // (2 * grp)) * grp + lax.rem(me, grp)
        for u in range(7):
            q = jnp.bitwise_and(own_q + (i * 7 + u + 1) * 27, peers // 2 - 1)
            pltpu.make_async_remote_copy(
                src_ref=share_s,
                dst_ref=srecv_s.at[me],
                send_sem=send_sem.at[5],
                recv_sem=recv_sem.at[5, 0],
                device_id=q + (q // grp) * grp + core * grp,
                device_id_type=LOGICAL,
            ).start()
        return carry

    lax.fori_loop(0, (peers // 2 - 1) // 7, share, 0)
    srecv_s[me] = share_s[...]
    lax.fori_loop(2, tiles, direct, 0)
    for k in range(bursts):
        arrived(k, hrecv_s, 0, 4)
    hrows_s[...] = whole(hrecv_s[...]).reshape(peers * half, width).astype(jnp.bfloat16)

    def place(i, carry):
        at = pl.ds(pl.multiple_of(i * TALL, TALL), TALL)
        hot = pick(hrow_s[0:1, :].astype(jnp.int32), i * TALL, TALL, 0)
        gfeat_s[at, :] += dot32(hot, hrows_s[...])
        return carry

    lax.fori_loop(0, node_rows // TALL, place, 0)
    result = pltpu.make_async_copy(gfeat_s, gfeat_ref, adj_sem.at[0])
    result.start()
    others = srecv_s.at[pl.ds(1, peers // 2 - 1)]
    pltpu.make_async_copy(others, others, recv_sem.at[5, 0]).wait()

    def across(i, carry):
        part = srecv_s.at[pl.ds(i * (2 * grp) + core * grp, grp)]
        pltpu.make_async_remote_copy(
            src_ref=part,
            dst_ref=part,
            send_sem=send_sem.at[6],
            recv_sem=recv_sem.at[5, 1],
            device_id=partner,
            device_id_type=LOGICAL,
        ).start()
        return carry

    lax.fori_loop(0, groups, across, 0)
    sent(others, 5)
    sent(srecv_s.at[pl.ds(0, peers // 2)], 6)
    for which, ref in ((1, served_s), (2, rgrad_s)):
        sent(ref.at[pl.ds(block, recv_rows - block), :], which)
    for which, ref in ((0, frecv_s), (3, part_s), (4, halo_s), (7, hpart_s), (8, arecv_s)):
        sent(ref.at[pl.ds(1, peers - 1)], which)
    mates = srecv_s.at[pl.ds(0, peers // 2)]
    pltpu.make_async_copy(mates, mates, recv_sem.at[5, 1]).wait()
    everyone = srecv_s[...].astype(jnp.float32)
    node_terms = joined(everyone[:, :8])
    gself_ref[...] = node_terms[:width]
    gneigh_ref[...] = node_terms[width:]
    ghid_ref[...] = joined(everyone[:, 8:16])
    total = jnp.sum(everyone[:, block:], axis=0)
    total = total[:4] + total[4:]
    gbias_ref[...] = jnp.concatenate([total[0:1], total[1:2]], axis=1)
    gout_ref[...] = jnp.concatenate([total[2:3], total[3:4]], axis=1)
    result.wait()


def finish_kernel(count, *refs):
    taken, given, held = refs[:count], refs[count : 2 * count], refs[2 * count : 3 * count]
    in_sem, out_sem = refs[3 * count :]
    parts = []
    for a, h, b in zip(taken, held, given):
        rows = a.shape[0]
        step = TILE if rows > TILE else rows
        parts += [(a, h, b, pl.ds(r, step)) for r in range(0, rows, step)]
    moves = [
        (
            pltpu.make_async_copy(a.at[at, :], h.at[at, :], in_sem.at[n]),
            pltpu.make_async_copy(h.at[at, :], b.at[at, :], out_sem.at[n]),
        )
        for n, (a, h, b, at) in enumerate(parts)
    ]
    for fetch, _ in moves:
        fetch.start()
    for fetch, put in moves:
        fetch.wait()
        put.start()
    for _, put in moves:
        put.wait()


def finish(arrays):
    count = len(arrays)
    moves = sum(max(a.shape[0] // TILE, 1) for a in arrays)
    return pl.pallas_call(
        lambda *refs: finish_kernel(count, *refs),
        out_shape=tuple(jax.ShapeDtypeStruct(a.shape, a.dtype) for a in arrays),
        in_specs=[ANY] * count,
        out_specs=(ANY,) * count,
        scratch_shapes=[pltpu.VMEM(a.shape, a.dtype) for a in arrays]
        + [pltpu.SemaphoreType.DMA((moves,)), pltpu.SemaphoreType.DMA((moves,))],
        compiler_params=params(60),
        name="finish",
    )(*arrays)


def train_step(
    adj, features, degt, ask, halo, ends, pair_weight, labels, w_self, w_neigh, w_hidden,
    bias, w_out
):
    node_rows, width = features.shape
    table_rows = adj.shape[1]
    block, peers = ask.shape
    half = halo.shape[0]
    recv_rows = peers * block
    pairs = ends.shape[1]
    lines = 2 * half + 8
    bf16 = lambda *shape: pltpu.VMEM(shape, jnp.bfloat16)
    return pl.pallas_call(
        step_kernel,
        out_shape=(
            jax.ShapeDtypeStruct((1, pairs), jnp.float32),
            jax.ShapeDtypeStruct((node_rows, width), jnp.float32),
            jax.ShapeDtypeStruct((width, width), jnp.float32),
            jax.ShapeDtypeStruct((width, width), jnp.float32),
            jax.ShapeDtypeStruct((2 * width, width), jnp.float32),
            jax.ShapeDtypeStruct((1, width), jnp.float32),
            jax.ShapeDtypeStruct((1, width), jnp.float32),
        ),
        in_specs=[ANY, ANY] + [VMEM] * 6 + [ANY] * 3 + [VMEM] * 2,
        out_specs=(VMEM, ANY) + (VMEM,) * 5,
        scratch_shapes=[
            bf16(node_rows, table_rows),
            bf16(node_rows, width),
            bf16(width, width),
            bf16(width, width),
            bf16(2 * width, width),
            pltpu.VMEM((node_rows, width), jnp.float32),
            pltpu.VMEM((8, pairs), jnp.float32),
            pltpu.VMEM((8, node_rows), jnp.float32),
            pltpu.VMEM((peers * half, 1), jnp.float32),
            pltpu.VMEM((8, peers * half), jnp.float32),
            pltpu.VMEM((peers, LANES), jnp.float32),
            pltpu.VMEM((recv_rows, 1), jnp.float32),
            bf16(width, node_rows),
            bf16(width, node_rows),
            pltpu.VMEM((8, recv_rows), jnp.float32),
            pltpu.VMEM((peers, 1, LANES), jnp.int32),
            pltpu.VMEM((peers, 1, LANES), jnp.int32),
            bf16(peers, block, LANES),
            bf16(peers, block, LANES),
            bf16(peers * half, width),
            bf16(node_rows, width),
            bf16(node_rows, width),
            bf16(recv_rows, width),
            bf16(recv_rows, width),
            bf16(pairs, width),
            bf16(pairs, width),
            bf16(pairs, width),
            bf16(pairs, width),
            bf16(pairs, width),
            bf16(recv_rows, width),
            bf16(recv_rows, width),
            bf16(node_rows, width),
            bf16(width, node_rows),
            pltpu.VMEM((4 * width, width), jnp.float32),
            pltpu.VMEM((8, width), jnp.float32),
            pltpu.VMEM((pairs, 8), jnp.float32),
            bf16(peers, half, LANES),
            bf16(peers, half, LANES),
            bf16(peers, half, LANES),
            bf16(peers, half, LANES),
            bf16(peers, block, LANES),
            bf16(peers, block, LANES),
            bf16(peers * half, width),
            bf16(lines, LANES),
            bf16(peers, lines, LANES),
            pltpu.SemaphoreType.DMA((4,)),
            pltpu.SemaphoreType.DMA((node_rows // TILE,)),
            pltpu.SemaphoreType.DMA((9,)),
            pltpu.SemaphoreType.DMA((9, recv_rows // WIDE)),
        ],
        compiler_params=pltpu.CompilerParams(
            vmem_limit_bytes=62 * 2**20, collective_id=0, has_side_effects=True
        ),
        cost_estimate=cost(30_000_000_000, 24 * 2**20),
        name="train_step",
    )(
        adj, features, degt, ask, halo, ends, pair_weight, labels, w_self, w_neigh,
        w_hidden, bias, w_out,
    )


def per_device(
    features,
    edge_src,
    edge_dst,
    edge_count,
    halo_index,
    request_rows,
    pair_ends,
    labels,
    pair_weight,
    w_self,
    w_neigh,
    w_hidden,
    b_hidden,
    w_out,
):
    node_rows = features.shape[0]
    halo = halo_index[0].T
    adj, degt = adjacency(edge_src, edge_dst, edge_count, node_rows, node_rows + halo.size)
    logits, grad_features, grad_self, grad_neigh, grad_hidden, grad_bias, grad_out = train_step(
        adj, features, degt, request_rows[0].T, halo, pair_ends.T, pair_weight[None],
        labels[None], w_self, w_neigh, w_hidden, b_hidden[None], w_out[None]
    )
    grad_features, grad_self, grad_neigh, grad_hidden, grad_bias, grad_out, logits = finish(
        (grad_features, grad_self, grad_neigh, grad_hidden, grad_bias, grad_out, logits)
    )
    return (
        logits[0],
        grad_features,
        grad_self,
        grad_neigh,
        grad_hidden,
        grad_bias[0],
        grad_out[0],
    )


def solution(mesh):
    split = P(AXES)
    in_specs = (
        P(AXES, None),
        split,
        split,
        split,
        P(AXES, None, None),
        P(AXES, None, None),
        P(AXES, None),
        split,
        split,
        P(),
        P(),
        P(),
        P(),
        P(),
    )
    out_specs = (split, P(AXES, None), P(), P(), P(), P(), P())
    return jax.shard_map(
        per_device, mesh=mesh, in_specs=in_specs, out_specs=out_specs, check_vma=False
    )
```
